256 devices in a mesh: gx: 16 (over z, core), gy: 8 (over x_hi, y), gz: 2 (over x_lo).
Axes of the slice: x: 4 (x_hi: 2, x_lo: 2; x = x_hi * 2 + x_lo), y: 4, z: 8, core: 2. Of those that a mesh axis runs over, the one named last changes fastest.
Arguments:
- load_current: float32 [1536, 8192], P('gy', 'gx'), may hold values from 0 to 90
- sink_mask: int32 [1536, 8192], P('gy', 'gx'), may hold values 0 or 1
- pad_mask: int32 [1536, 8192], P('gy', 'gx'), may hold values from 0 to 1, as said below
- plane_class: int32 [4, 1536, 8192], P('gz', 'gy', 'gx'), may hold values from 0 to 7
- via_class: int32 [4, 1536, 8192], P('gz', 'gy', 'gx'), may hold values from 0 to 7
- plane_table: float32 [4, 8], P('gz'), may hold values from 0.25 to 4
- via_table: float32 [4, 8], P('gz'), may hold values from 0.25 to 4
Outputs:
- voltage: float32 [4, 1536, 8192], P('gz', 'gy', 'gx')
- residual: float32 [4, 1536, 8192], P('gz', 'gy', 'gx')
The draws below stay inside these ranges and needn't reach their ends.
Inputs may be any that keep to these rules, and one draw needn't show every extreme that they name: `pad_mask`: exactly one pad in each aligned 8 x 8 tile of nodes.
All inputs are finite; a program needn't handle non-finite values. No bound on the sum of `sink_mask` on one device may be relied on, other than what follows from the above.
Results may differ from the reference program's by a relative error of at most 0.00012.
Values sent between devices are 32-bit elements; how exact they have to be, the bound alone decides.
No kernel may reach another device: no remote copies, remote signals or barrier semaphores. Data moves between devices by JAX's collectives and lax.ppermute only.
A program may use at most 64 MiB of HBM per device.

```python
import math
import jax
import jax.numpy as jnp

L_DEV = 2
ITERS = 3
NCLASS = 8
LAYERS = 4
NX = 8192
NY = 1536
N_GZ = 2


def draw_pad_mask(key, part):
    pad_key = jax.random.fold_in(key, 11)
    pad_spots = jax.random.randint(pad_key, (NY // 8, NX // 8), 0, 64)
    row_ids = jnp.arange(NY, dtype=jnp.int32)[:, None]
    col_ids = jnp.arange(NX, dtype=jnp.int32)[None, :]
    local_index = row_ids % 8 * 8 + col_ids % 8
    chosen = jnp.repeat(jnp.repeat(pad_spots, 8, axis=0), 8, axis=1)
    return (local_index == chosen).astype(jnp.int32)


def draw_load_current(key, part):
    base_key = jax.random.fold_in(key, 23)
    row_key, col_key, cell_key = jax.random.split(base_key, 3)
    rise_rows = jnp.arange(NY, dtype=jnp.float32) / NY * math.log(3.0)
    rise_cols = jnp.arange(NX, dtype=jnp.float32) / NX * math.log(3.0)
    log_span = math.log(10.0)
    cell_factor = jnp.exp(jax.random.uniform(cell_key, (NY, NX), jnp.float32, math.log(0.2), math.log(2.0)))
    row_scale = jnp.exp(jax.random.uniform(row_key, (NY, 1), jnp.float32) * log_span + rise_rows[:, None])
    col_scale = jnp.exp(jax.random.uniform(col_key, (1, NX), jnp.float32) * log_span + rise_cols[None, :])
    return (0.02 * row_scale * col_scale * cell_factor).astype(jnp.float32)


def touch_ends(values, rng, low, high):
    dims = values.shape
    spot = [jax.random.randint(jax.random.fold_in(rng, axis), (), 0, dims[axis]) for axis in range(len(dims))]
    values = values.at[tuple(spot)].set(low)
    longest = dims.index(max(dims))
    spot[longest] = (spot[longest] + 1) % dims[longest]
    return values.at[tuple(spot)].set(high)


def shard_levels(own_key, dims, cuts, least, largest):
    factor_of = 1.0
    for dim, blocks in cuts:
        heights = jax.random.uniform(jax.random.fold_in(jax.random.fold_in(own_key, 6), dim), (blocks,), jnp.float32, least / len(cuts), largest / len(cuts))
        factor_of = factor_of * jnp.repeat(jnp.exp(heights), dims[dim] // blocks).reshape((-1,) + (1,) * (len(dims) - 1 - dim))
    return factor_of


def setup_inputs(seed: int = 0) -> dict:
    splits = jax.random.split(jax.random.key(seed), 8)
    load_current = draw_load_current(jax.random.fold_in(splits[7], 71), 0)
    sink_mask = touch_ends((jax.random.randint(splits[1], (NY, NX), 0, 2) < 1).astype(jnp.int32), jax.random.fold_in(splits[1], 1), 0, 1)
    pad_mask = draw_pad_mask(jax.random.fold_in(splits[7], 71), 0)
    plane_class = touch_ends(jax.random.randint(splits[3], (LAYERS, NY, NX), 0, NCLASS), jax.random.fold_in(splits[3], 1), 0, NCLASS - 1).astype(jnp.int32)
    via_class = touch_ends(jax.random.randint(splits[4], (LAYERS, NY, NX), 0, NCLASS), jax.random.fold_in(splits[4], 1), 0, NCLASS - 1).astype(jnp.int32)
    plane_table = jnp.clip(jnp.exp(math.log(4.0) - 2.7725887 * jax.random.uniform(splits[5], (LAYERS, NCLASS), jnp.float32) ** shard_levels(splits[5], (LAYERS, NCLASS), ((0, 2),), -0.2, 0.2)), 0.25, 4.0)
    via_table = jnp.clip(jnp.exp(math.log(4.0) - 2.7725887 * jax.random.uniform(splits[6], (LAYERS, NCLASS), jnp.float32) ** shard_levels(splits[6], (LAYERS, NCLASS), ((0, 2),), -0.2, 0.2)), 0.25, 4.0)
    return {"load_current": load_current, "sink_mask": sink_mask, "pad_mask": pad_mask, "plane_class": plane_class, "via_class": via_class, "plane_table": plane_table, "via_table": via_table}


PAD_CONDUCTANCE = 20.0


def lookup(classes, table):
    summed = jnp.zeros(classes.shape, jnp.float32)
    for level in range(table.shape[1]):
        summed = summed + jnp.where(classes == level, table[:, level][:, None, None], jnp.float32(0.0))
    return summed


def harmonic(first, second):
    return 2.0 * first * second / (first + second)


def factor(diagonal, up_edge):
    inverses = []
    factors = []
    for level in range(diagonal.shape[0]):
        pivots = diagonal[level]
        if level > 0:
            pivots = pivots + up_edge[level - 1] * factors[level - 1]
        inverse = 1.0 / pivots
        inverses.append(inverse)
        factors.append(-up_edge[level] * inverse)
    return jnp.stack(inverses), jnp.stack(factors)


def solve_block(inverses, factors, up_edge, source_term):
    forward = []
    for level in range(source_term.shape[0]):
        entries = source_term[level]
        if level > 0:
            entries = entries + up_edge[level - 1] * forward[level - 1]
        forward.append(entries * inverses[level])
    result = [forward[-1]]
    for level in range(source_term.shape[0] - 2, -1, -1):
        result.insert(0, forward[level] - factors[level] * result[0])
    return jnp.stack(result)


def reference(load_current, sink_mask, pad_mask, plane_class, via_class, plane_table, via_table):
    g_plane = lookup(plane_class, plane_table)
    g_via = lookup(via_class, via_table)
    zero_plane = jnp.zeros((1, NY, NX), jnp.float32)
    east_edge = harmonic(g_plane, jnp.roll(g_plane, -1, 2))
    north_edge = harmonic(g_plane, jnp.roll(g_plane, -1, 1))
    up_edge = jnp.concatenate([harmonic(g_via[:-1], g_via[1:]), zero_plane], 0)
    down_edge = jnp.concatenate([zero_plane, up_edge[:-1]], 0)
    west_edge = jnp.roll(east_edge, 1, 2)
    south_edge = jnp.roll(north_edge, 1, 1)
    pad_layer = jnp.concatenate([jnp.zeros((LAYERS - 1, NY, NX), jnp.float32), (PAD_CONDUCTANCE * pad_mask.astype(jnp.float32))[None]], 0)
    diagonal = east_edge + west_edge + north_edge + south_edge + up_edge + down_edge + pad_layer

    def operate(field):
        above_field = jnp.concatenate([field[1:], zero_plane], 0)
        below_field = jnp.concatenate([zero_plane, field[:-1]], 0)
        return (diagonal * field
                - east_edge * jnp.roll(field, -1, 2) - west_edge * jnp.roll(field, 1, 2)
                - north_edge * jnp.roll(field, -1, 1) - south_edge * jnp.roll(field, 1, 1)
                - up_edge * above_field - down_edge * below_field)

    def blocks(array):
        return array.reshape(N_GZ, L_DEV, NY, NX)

    up_blocks = blocks(up_edge)
    inverses, factors = jax.vmap(factor)(blocks(diagonal), up_blocks)

    def precondition(residual):
        return jax.vmap(solve_block)(inverses, factors, up_blocks, blocks(residual)).reshape(LAYERS, NY, NX)

    source = sink_mask.astype(jnp.float32) * load_current
    right_side = jnp.concatenate([source[None], jnp.zeros((LAYERS - 1, NY, NX), jnp.float32)], 0)
    voltage = jnp.zeros((LAYERS, NY, NX), jnp.float32)
    residual = right_side
    precond = precondition(residual)
    direction = precond
    weight_now = jnp.sum(residual * precond)
    for iteration in range(ITERS):
        image_field = operate(direction)
        step_size = weight_now / jnp.sum(direction * image_field)
        voltage = voltage + step_size * direction
        residual = residual - step_size * image_field
        if iteration + 1 < ITERS:
            precond = precondition(residual)
            weight_next = jnp.sum(residual * precond)
            direction = precond + (weight_next / weight_now) * direction
            weight_now = weight_next
    return voltage, residual
```

```python
import jax
import jax.numpy as jnp
from jax import lax
from jax.experimental import pallas as pl
from jax.experimental.pallas import tpu as pltpu
from jax.sharding import Mesh
from jax.sharding import PartitionSpec as P

ITERS = 3
GX = ("gx_0", "gx_1")
GY = ("gy_0", "gy_1")
GX_GY_GZ = ("gx_0", "gx_1", "gy_0", "gy_1", "gz")


PAD_CONDUCTANCE = 20.0


def padded(array, sides, width):
    edges = {}
    for axis, dim in sides:
        peers, length = (lax.axis_size(axis), array.shape[dim])
        up = [(i, (i + 1) % peers) for i in range(peers)]
        last = lax.slice_in_dim(array, length - width, length, axis=dim)
        leading = lax.slice_in_dim(array, 0, width, axis=dim)
        edges[dim] = (
            lax.ppermute(last, axis, up),
            lax.ppermute(leading, axis, [(b, a) for a, b in up]),
        )
    done = []
    for _, dim in sides:
        low, high = edges[dim]
        around = [(width, width) if d in done else (0, 0) for d in range(array.ndim)]
        array = jnp.concatenate([jnp.pad(low, around), array, jnp.pad(high, around)], axis=dim)
        done.append(dim)
    return array


def padded_2(block, sides, width):
    for axis, dim in sides:
        count = lax.axis_size(axis)
        forward = [(i, i + 1) for i in range(count - 1)]
        backward = [(target, source) for source, target in forward]
        low = lax.ppermute(
            lax.slice_in_dim(block, block.shape[dim] - width, None, axis=dim), axis, forward
        )
        high = lax.ppermute(lax.slice_in_dim(block, 0, width, axis=dim), axis, backward)
        block = jnp.concatenate([low, block, high], axis=dim)
    return block


def by_axis(array, axes):
    for axis in axes:
        array = lax.psum(array, axis)
    return array


def lookup(classes, table):
    summed = jnp.zeros(classes.shape, jnp.float32)
    for level in range(table.shape[1]):
        summed = summed + jnp.where(
            classes == level, table[:, level][:, None, None], jnp.float32(0.0)
        )
    return summed


def harmonic(first, second):
    return 2.0 * first * second / (first + second)


def factor(diagonal, up_edge):
    inverses = []
    factors = []
    for level in range(diagonal.shape[0]):
        pivots = diagonal[level]
        if level > 0:
            pivots = pivots + up_edge[level - 1] * factors[level - 1]
        inverse = 1.0 / pivots
        inverses.append(inverse)
        factors.append(-up_edge[level] * inverse)
    return (jnp.stack(inverses), jnp.stack(factors))


def solve_block(inverses, factors, up_edge, source_term):
    forward = []
    for level in range(source_term.shape[0]):
        entries = source_term[level]
        if level > 0:
            entries = entries + up_edge[level - 1] * forward[level - 1]
        forward.append(entries * inverses[level])
    result = [forward[-1]]
    level = 0
    result.insert(0, forward[level] - factors[level] * result[0])
    return jnp.stack(result)


def plane_extend(field):
    return padded(field, ((GX, 2), (GY, 1)), 1)


def layer_extend(field):
    return padded_2(field, (("gz", 0),), 1)


def merged_sums(residual, precond, image_field):
    return (
        by_axis(jnp.sum(residual * precond), GX_GY_GZ),
        by_axis(jnp.sum(image_field * precond), GX_GY_GZ),
    )


def recurrence(load_current, sink_mask, pad_mask, plane_class, via_class, plane_table, via_table):
    n_layers, n_rows, n_cols = plane_class.shape
    g_plane = lookup(plane_class, plane_table)
    g_via = lookup(via_class, via_table)
    plane_ext = plane_extend(g_plane)
    middle = plane_ext[:, 1:-1, :]
    across = harmonic(middle[:, :, :-1], middle[:, :, 1:])
    east_edge = across[:, :, 1:]
    west_edge = across[:, :, :-1]
    column = plane_ext[:, :, 1:-1]
    along_rows = harmonic(column[:, :-1], column[:, 1:])
    north_edge = along_rows[:, 1:]
    south_edge = along_rows[:, :-1]
    via_ext = layer_extend(g_via)
    vertical = harmonic(via_ext[:-1], via_ext[1:])
    up_edge = vertical[1:]
    down_edge = vertical[:-1]
    group_index = lax.axis_index("gz")
    is_top = group_index == lax.axis_size("gz") - 1
    is_bottom = group_index == 0
    pad_plane = jnp.where(is_top, PAD_CONDUCTANCE * pad_mask.astype(jnp.float32), jnp.float32(0.0))
    pad_layer = jnp.concatenate(
        [jnp.zeros((n_layers - 1, n_rows, n_cols), jnp.float32), pad_plane[None]], 0
    )
    diagonal = east_edge + west_edge + north_edge + south_edge + up_edge + down_edge + pad_layer
    inverses, factors = factor(diagonal, up_edge)

    def precondition(residual):
        return solve_block(inverses, factors, up_edge, residual)

    def operate(field):
        inner = plane_extend(field)
        layer_ext = layer_extend(field)
        above_field = layer_ext[2:]
        below_field = layer_ext[:-2]
        return (
            diagonal * field
            - east_edge * inner[:, 1:-1, 2:]
            - west_edge * inner[:, 1:-1, :-2]
            - north_edge * inner[:, 2:, 1:-1]
            - south_edge * inner[:, :-2, 1:-1]
            - up_edge * above_field
            - down_edge * below_field
        )

    source = jnp.where(is_bottom, sink_mask.astype(jnp.float32) * load_current, jnp.float32(0.0))
    right_side = jnp.concatenate(
        [source[None], jnp.zeros((n_layers - 1, n_rows, n_cols), jnp.float32)], 0
    )
    voltage = jnp.zeros((n_layers, n_rows, n_cols), jnp.float32)
    residual = right_side
    precond = precondition(residual)
    image_field = operate(precond)
    weight_now, curvature = merged_sums(residual, precond, image_field)
    step_size = weight_now / curvature
    direction = precond
    image_dir = image_field
    for iteration in range(ITERS):
        voltage = voltage + step_size * direction
        residual = residual - step_size * image_dir
        if iteration + 1 < ITERS:
            precond = precondition(residual)
            image_field = operate(precond)
            weight_next, curvature = merged_sums(residual, precond, image_field)
            momentum = weight_next / weight_now
            step_size = weight_next / (curvature - momentum * weight_next / step_size)
            direction = precond + momentum * direction
            image_dir = image_field + momentum * image_dir
            weight_now = weight_next
    return (voltage, residual)


STEP = 8
LANES = 128
GUARD = 0.02
VMEM = pl.BlockSpec(memory_space=pltpu.VMEM)
SMEM = pl.BlockSpec(memory_space=pltpu.SMEM)


def select_class(classes, entry):
    low = (classes & 1) != 0
    mid = (classes & 2) != 0
    high = (classes & 4) != 0
    pairs = [jnp.where(low, entry(2 * k + 1), entry(2 * k)) for k in range(4)]
    return jnp.where(high, jnp.where(mid, pairs[3], pairs[2]), jnp.where(mid, pairs[1], pairs[0]))


def via_kernel(gz, table, classes, via_i, inner):
    group = gz[0]
    for r in range(0, via_i.shape[0], STEP):
        rows = pl.ds(r, STEP)
        one = select_class(classes[1 - group, rows, :], lambda k: table[1 - group, k])
        two = select_class(classes[group, rows, :], lambda k: table[group, k])
        via_i[rows, :] = one
        inner[rows, :] = harmonic(one, two)


def stage_columns(stage, r, field_i, field_o):
    lane = lax.broadcasted_iota(jnp.int32, (STEP, LANES), 1)
    last = field_i.shape[1] - LANES
    first_o = pltpu.roll(field_o[:, :LANES], 1, 1)
    last_i = pltpu.roll(field_i[:, last:], 3, 1)
    last_o = pltpu.roll(field_o[:, last:], 4, 1)
    picked = jnp.where(lane == 2, last_i, last_o)
    picked = jnp.where(lane == 1, first_o, picked)
    stage[pl.ds(r, STEP), :] = jnp.where(lane == 0, field_i[:, :LANES], picked)


def send_edges(stage, field_i, field_o, edges):
    first_row, last_row, first_col, last_col = edges
    n_rows = field_i.shape[0]
    first_row[0:1, :] = field_i[0:1, :]
    first_row[1:2, :] = field_o[0:1, :]
    last_row[0:1, :] = field_i[n_rows - 1 : n_rows, :]
    last_row[1:2, :] = field_o[n_rows - 1 : n_rows, :]
    turned = stage[...].T
    first_col[...] = turned[0:2, :]
    last_col[...] = turned[2:4, :]


def take_columns(flat, west, east, columns):
    flat[...] = jnp.zeros(flat.shape, jnp.float32)
    flat[0:2, :] = west[...]
    flat[2:4, :] = east[...]
    columns[...] = flat[...].T


def plane_kernel(gz, table, classes, plane_i, plane_o, *rest):
    edges, stage = rest[:4], rest[4]
    group = gz[0]
    stage[...] = jnp.zeros(stage.shape, jnp.float32)
    for r in range(0, plane_i.shape[0], STEP):
        rows = pl.ds(r, STEP)
        one = select_class(classes[1 - group, rows, :], lambda k: table[1 - group, k])
        two = select_class(classes[group, rows, :], lambda k: table[group, k])
        plane_i[rows, :] = one
        plane_o[rows, :] = two
        stage_columns(stage, r, one, two)
    send_edges(stage, plane_i, plane_o, edges)


def around(field, layer, r, south, north, columns):
    n_rows, n_cols = field.shape
    own = field[pl.ds(r, STEP), :]
    sub = lax.broadcasted_iota(jnp.int32, own.shape, 0)
    lane = lax.broadcasted_iota(jnp.int32, own.shape, 1)
    if r:
        below = field[r - 1 : r - 1 + STEP, :]
    else:
        below = jnp.where(sub == 0, south[layer : layer + 1, :], pltpu.roll(own, 1, 0))
    if r + STEP < n_rows:
        above = field[r + 1 : r + 1 + STEP, :]
    else:
        above = jnp.where(
            sub == STEP - 1, north[layer : layer + 1, :], pltpu.roll(own, STEP - 1, 0)
        )
    west_col = columns[pl.ds(r, STEP), layer : layer + 1]
    east_col = columns[pl.ds(r, STEP), layer + 2 : layer + 3]
    west = jnp.where(lane == 0, west_col, pltpu.roll(own, 1, 1))
    east = jnp.where(lane == n_cols - 1, east_col, pltpu.roll(own, n_cols - 1, 1))
    return own, east, west, above, below


def fold(total):
    width = total.shape[1]
    while width > LANES:
        width //= 2
        total = total[:, :width] + total[:, width:]
    return jnp.sum(total, axis=0, keepdims=True)


def edge_kernel(
    gz, plane_i, plane_o, south, north, west, east, via_i, via_far, inner, load, sink, pad, *rest
):
    edges_i, edges_o = rest[0:4], rest[4:8]
    cross, inv_ii, inv_oo, inv_io, v_i, v_o, source, payload = rest[8:16]
    sends, part = rest[16:20], rest[20]
    stage, flat, columns = rest[21:]
    group = gz[0]
    take_columns(flat, west, east, columns)
    stage[...] = jnp.zeros(stage.shape, jnp.float32)
    total = jnp.zeros((STEP, plane_i.shape[1]), jnp.float32)
    for r in range(0, plane_i.shape[0], STEP):
        rows = pl.ds(r, STEP)
        sums = []
        for layer, field, edges in ((0, plane_i, edges_i), (1, plane_o, edges_o)):
            own, *others = around(field, layer, r, south, north, columns)
            values = [harmonic(own, other) for other in others]
            for edge, value in zip(edges, values):
                edge[rows, :] = value
            sums.append(values[0] + values[1] + values[2] + values[3])
        up = inner[rows, :]
        far = harmonic(via_i[rows, :], via_far[rows, :])
        cross[rows, :] = far
        pads = PAD_CONDUCTANCE * pad[rows, :].astype(jnp.float32)
        diag_i = sums[0] + up + far
        diag_o = sums[1] + up + jnp.where(group == 1, pads, 0.0)
        inverse = 1.0 / (diag_i * diag_o - up * up)
        ii, oo, io = diag_o * inverse, diag_i * inverse, up * inverse
        drawn = sink[rows, :].astype(jnp.float32) * load[rows, :]
        drawn = jnp.where(group == 0, drawn, 0.0)
        one, two = io * drawn, oo * drawn
        inv_ii[rows, :], inv_oo[rows, :], inv_io[rows, :] = ii, oo, io
        source[rows, :] = drawn
        v_i[rows, :], v_o[rows, :] = one, two
        payload[rows, :] = jnp.where(group == 0, one, ii)
        stage_columns(stage, r, one, two)
        total = total + two * drawn
    send_edges(stage, v_i, v_o, sends)
    part[...] = jnp.zeros(part.shape, jnp.float32)
    part[0:1, :] = fold(total)


def stencil(field, layer, r, halos, columns, edges):
    own, *others = around(field, layer, r, halos[0], halos[1], columns)
    rows = pl.ds(r, STEP)
    east, west, above, below = [edge[rows, :] * value for edge, value in zip(edges, others)]
    return own, (east + west) + (above + below)


def first_kernel(gz, v_i, v_o, south, north, west, east, *rest):
    edges_i, edges_o = rest[0:4], rest[4:8]
    cross, inv_ii, inv_oo, inv_io, given, before = rest[8:14]
    n_i, n_o, w_i, w_o, far = rest[14:19]
    sends, part = rest[19:23], rest[23]
    stage, flat, columns = rest[24:]
    group = gz[0]
    take_columns(flat, west, east, columns)
    stage[...] = jnp.zeros(stage.shape, jnp.float32)
    sums = [jnp.zeros((STEP, v_i.shape[1]), jnp.float32)] * 2
    for r in range(0, v_i.shape[0], STEP):
        rows = pl.ds(r, STEP)
        own_i, out_i = stencil(v_i, 0, r, (south, north), columns, edges_i)
        own_o, out_o = stencil(v_o, 1, r, (south, north), columns, edges_o)
        link, got = cross[rows, :], given[rows, :]
        out_i = out_i + jnp.where(group == 1, link * got, 0.0)
        far[rows, :] = link * own_i * got
        ii, oo, io = inv_ii[rows, :], inv_oo[rows, :], inv_io[rows, :]
        one, two = ii * out_i + io * out_o, io * out_i + oo * out_o
        n_i[rows, :], n_o[rows, :] = out_i, out_o
        w_i[rows, :], w_o[rows, :] = one, two
        stage_columns(stage, r, one, two)
        sums[0] = sums[0] + (own_i * out_i + own_o * out_o)
        sums[1] = sums[1] + (one * out_i + two * out_o)
    send_edges(stage, w_i, w_o, sends)
    part[...] = before[...]
    part[1:2, :] = fold(sums[0])
    part[2:3, :] = fold(sums[1])


def second_kernel(gz, v_i, v_o, south, north, west, east, *rest):
    edges_i, edges_o = rest[0:4], rest[4:8]
    cross, inv_ii, inv_oo, inv_io, made, given, before = rest[8:15]
    n_i, n_o, w_i, w_o = rest[15:19]
    sends, part = rest[19:23], rest[23]
    stage, flat, columns = rest[24:]
    group = gz[0]
    take_columns(flat, west, east, columns)
    stage[...] = jnp.zeros(stage.shape, jnp.float32)
    sums = [jnp.zeros((STEP, v_i.shape[1]), jnp.float32)] * 2
    for r in range(0, v_i.shape[0], STEP):
        rows = pl.ds(r, STEP)
        own_i, out_i = stencil(v_i, 0, r, (south, north), columns, edges_i)
        own_o, out_o = stencil(v_o, 1, r, (south, north), columns, edges_o)
        out_i = out_i + cross[rows, :] * jnp.where(group == 0, made[rows, :], given[rows, :])
        ii, oo, io = inv_ii[rows, :], inv_oo[rows, :], inv_io[rows, :]
        one, two = ii * out_i + io * out_o, io * out_i + oo * out_o
        n_i[rows, :], n_o[rows, :] = out_i, out_o
        w_i[rows, :], w_o[rows, :] = one, two
        stage_columns(stage, r, one, two)
        sums[0] = sums[0] + (own_i * out_i + own_o * out_o)
        sums[1] = sums[1] + (one * out_i + two * out_o)
    send_edges(stage, w_i, w_o, sends)
    part[...] = before[...]
    part[3:4, :] = fold(sums[0])
    part[4:5, :] = fold(sums[1])


def third_kernel(v_i, v_o, south, north, west, east, *rest):
    edges_i, edges_o = rest[0:4], rest[4:8]
    cross, given, before = rest[8:11]
    n_i, n_o, spread = rest[11:14]
    flat, columns = rest[14:]
    take_columns(flat, west, east, columns)
    total = jnp.zeros((STEP, v_i.shape[1]), jnp.float32)
    for r in range(0, v_i.shape[0], STEP):
        rows = pl.ds(r, STEP)
        own_i, out_i = stencil(v_i, 0, r, (south, north), columns, edges_i)
        own_o, out_o = stencil(v_o, 1, r, (south, north), columns, edges_o)
        out_i = out_i + cross[rows, :] * given[rows, :]
        n_i[rows, :], n_o[rows, :] = out_i, out_o
        total = total + (own_i * out_i + own_o * out_o)
    row = lax.broadcasted_iota(jnp.int32, before.shape, 0)
    part = jnp.where(row == 5, fold(total), before[...])
    for k in range(spread.shape[0]):
        spread[k] = part


def tree(parts):
    values = [parts[k] for k in range(parts.shape[0])]
    while len(values) > 1:
        values = [a + b for a, b in zip(values[::2], values[1::2])]
    return values[0]


def relay_kernel(parts, spread):
    total = tree(parts)
    for k in range(spread.shape[0]):
        spread[k] = total


def solve_kernel(parts, coefs, flag):
    sums = jnp.sum(tree(parts), axis=1, keepdims=True)
    g = [jnp.broadcast_to(sums[k : k + 1, :], (1, LANES)) for k in range(6)]
    step = [g[k] - g[k + 1] for k in range(5)]
    scale = [lax.rsqrt(g[0]), lax.rsqrt(g[2]), lax.rsqrt(g[4])]

    def entry(i, j):
        return step[i + j] * scale[i] * scale[j]

    d0 = entry(0, 0)
    l10, l20 = entry(1, 0) / d0, entry(2, 0) / d0
    d1 = entry(1, 1) - l10 * entry(1, 0)
    e21 = entry(2, 1) - l20 * entry(1, 0)
    l21 = e21 / d1
    d2 = entry(2, 2) - l20 * entry(2, 0) - l21 * e21
    y0 = g[0] * scale[0]
    y1 = g[1] * scale[1] - l10 * y0
    y2 = g[2] * scale[2] - l20 * y0 - l21 * y1
    x2 = y2 / d2
    x1 = y1 / d1 - l21 * x2
    x0 = y0 / d0 - l10 * x1 - l20 * x2
    c0, c1, c2 = x0 * scale[0], x1 * scale[1], x2 * scale[2]
    for k, value in enumerate((c0, c1, c2, 1.0 - c0, c0 - c1, c1 - c2)):
        coefs[k : k + 1, :] = value
    coefs[6:8, :] = jnp.zeros((2, LANES), jnp.float32)
    good = (d0 > GUARD) & (d1 > GUARD) & (d2 > GUARD)
    flag[...] = jnp.where(good, 1, 0)


def combine_kernel(gz, coefs, source, *rest):
    fields, volts, left = rest[:12], rest[12], rest[13]
    group = gz[0]
    width = source.shape[1]
    c = [jnp.broadcast_to(coefs[k : k + 1, 0:1], (STEP, width)) for k in range(6)]
    for r in range(0, source.shape[0], STEP):
        rows = pl.ds(r, STEP)
        v0i, v0o, v1i, v1o, v2i, v2o, n0i, n0o, n1i, n1o, n2i, n2o = [f[rows, :] for f in fields]
        volts[1 - group, rows, :] = c[0] * v0i + c[1] * v1i + c[2] * v2i
        volts[group, rows, :] = c[0] * v0o + c[1] * v1o + c[2] * v2o
        left[1 - group, rows, :] = c[4] * n0i + c[5] * n1i + c[2] * n2i
        left[group, rows, :] = (
            c[3] * source[rows, :] + c[4] * n0o + c[5] * n1o + c[2] * n2o
        )


def call(kernel, name, outs, scratch, n_smem, *args):
    return pl.pallas_call(
        kernel,
        name=name,
        in_specs=[SMEM] * n_smem + [VMEM] * (len(args) - n_smem),
        out_specs=[VMEM] * len(outs),
        out_shape=outs,
        scratch_shapes=scratch,
    )(*args)


def halos(first_row, last_row, first_col, last_col):
    def ring(axis):
        size = lax.axis_size(axis)
        return [(i, (i + 1) % size) for i in range(size)]

    up_y, up_x = ring(GY), ring(GX)
    back_y, back_x = [(b, a) for a, b in up_y], [(b, a) for a, b in up_x]
    return (
        lax.ppermute(last_row, GY, up_y),
        lax.ppermute(first_row, GY, back_y),
        lax.ppermute(last_col, GX, up_x),
        lax.ppermute(first_col, GX, back_x),
    )


def shards(load_current, sink_mask, pad_mask, plane_class, via_class, plane_table, via_table):
    _, n_rows, n_cols = plane_class.shape
    tall = -(-n_rows // LANES) * LANES
    f32 = jnp.float32
    plane = jax.ShapeDtypeStruct((n_rows, n_cols), f32)
    both = jax.ShapeDtypeStruct((2, n_rows, n_cols), f32)
    row = jax.ShapeDtypeStruct((2, n_cols), f32)
    col = jax.ShapeDtypeStruct((2, tall), f32)
    sheet = jax.ShapeDtypeStruct((STEP, LANES), f32)
    edge_outs = [row, row, col, col]
    stage = pltpu.VMEM((tall, LANES), f32)
    turn = [pltpu.VMEM((LANES, tall), f32), pltpu.VMEM((tall, LANES), f32)]
    gz = lax.axis_index("gz").reshape(1).astype(jnp.int32)
    swap = [(0, 1), (1, 0)]
    n_gx, n_rest = lax.axis_size(GX), lax.axis_size(("gy_0", "gy_1", "gz"))

    via_i, inner = call(via_kernel, "via", [plane] * 2, [], 2, gz, via_table, via_class)
    via_far = lax.ppermute(via_i, "gz", swap)
    plane_i, plane_o, *sends = call(
        plane_kernel, "plane", [plane] * 2 + edge_outs, [stage], 2, gz, plane_table, plane_class
    )
    near = halos(*sends)
    outs = call(
        edge_kernel, "edge", [plane] * 16 + edge_outs + [sheet], [stage] + turn, 1,
        gz, plane_i, plane_o, *near, via_i, via_far, inner, load_current, sink_mask, pad_mask,
    )
    edges, (cross, inv_ii, inv_oo, inv_io) = outs[0:8], outs[8:12]
    v0i, v0o, source, payload = outs[12:16]
    sends, part = outs[16:20], outs[20]
    given = lax.ppermute(payload, "gz", swap)
    near = halos(*sends)
    n0i, n0o, v1i, v1o, made, *sends, part = call(
        first_kernel, "first", [plane] * 5 + edge_outs + [sheet], [stage] + turn, 1,
        gz, v0i, v0o, *near, *edges, cross, inv_ii, inv_oo, inv_io, given, part,
    )
    given = lax.ppermute(v1i, "gz", [(0, 1)])
    near = halos(*sends)
    n1i, n1o, v2i, v2o, *sends, part = call(
        second_kernel, "second", [plane] * 4 + edge_outs + [sheet], [stage] + turn, 1,
        gz, v1i, v1o, *near, *edges, cross, inv_ii, inv_oo, inv_io, made, given, part,
    )
    given = lax.ppermute(v2i, "gz", swap)
    near = halos(*sends)
    n2i, n2o, spread = call(
        third_kernel, "third",
        [plane] * 2 + [jax.ShapeDtypeStruct((n_gx, STEP, LANES), f32)], turn, 0,
        v2i, v2o, *near, *edges, cross, given, part,
    )
    parts = lax.all_to_all(spread, GX, 0, 0, tiled=True)
    (spread,) = call(
        relay_kernel, "relay", [jax.ShapeDtypeStruct((n_rest, STEP, LANES), f32)], [], 0, parts
    )
    parts = lax.all_to_all(spread, ("gy_0", "gy_1", "gz"), 0, 0, tiled=True)
    coefs, flag = call(
        solve_kernel, "solve", [sheet, jax.ShapeDtypeStruct((1, LANES), jnp.int32)], [], 0, parts
    )

    def fast():
        return tuple(
            call(
                combine_kernel, "combine", [both] * 2, [], 1, gz, coefs, source,
                v0i, v0o, v1i, v1o, v2i, v2o, n0i, n0o, n1i, n1o, n2i, n2o,
            )
        )

    def careful():
        return recurrence(
            load_current, sink_mask, pad_mask, plane_class, via_class, plane_table, via_table
        )

    return lax.cond(flag[0, 0] == 1, fast, careful)


def solution(mesh):
    split = Mesh(
        mesh.devices.reshape(8, 2, 2, 4, mesh.shape["gz"]), ("gx_0", "gx_1", "gy_0", "gy_1", "gz")
    )
    placed = (
        P(GY, GX),
        P(GY, GX),
        P(GY, GX),
        P("gz", GY, GX),
        P("gz", GY, GX),
        P("gz", None),
        P("gz", None),
    )
    return jax.shard_map(
        shards,
        mesh=split,
        in_specs=placed,
        out_specs=(P("gz", GY, GX), P("gz", GY, GX)),
        check_vma=False,
    )
```

```python
import jax
import jax.numpy as jnp
from jax import lax
from jax.experimental import pallas as pl
from jax.experimental.pallas import tpu as pltpu
from jax.sharding import Mesh
from jax.sharding import PartitionSpec as P

ITERS = 3
GX = ("gx_0", "gx_1")
GY = ("gy_0", "gy_1")
GX_GY_GZ = ("gx_0", "gx_1", "gy_0", "gy_1", "gz")


PAD_CONDUCTANCE = 20.0


def padded(array, sides, width):
    edges = {}
    for axis, dim in sides:
        peers, length = (lax.axis_size(axis), array.shape[dim])
        up = [(i, (i + 1) % peers) for i in range(peers)]
        last = lax.slice_in_dim(array, length - width, length, axis=dim)
        leading = lax.slice_in_dim(array, 0, width, axis=dim)
        edges[dim] = (
            lax.ppermute(last, axis, up),
            lax.ppermute(leading, axis, [(b, a) for a, b in up]),
        )
    done = []
    for _, dim in sides:
        low, high = edges[dim]
        around = [(width, width) if d in done else (0, 0) for d in range(array.ndim)]
        array = jnp.concatenate([jnp.pad(low, around), array, jnp.pad(high, around)], axis=dim)
        done.append(dim)
    return array


def padded_2(block, sides, width):
    for axis, dim in sides:
        count = lax.axis_size(axis)
        forward = [(i, i + 1) for i in range(count - 1)]
        backward = [(target, source) for source, target in forward]
        low = lax.ppermute(
            lax.slice_in_dim(block, block.shape[dim] - width, None, axis=dim), axis, forward
        )
        high = lax.ppermute(lax.slice_in_dim(block, 0, width, axis=dim), axis, backward)
        block = jnp.concatenate([low, block, high], axis=dim)
    return block


def by_axis(array, axes):
    for axis in axes:
        array = lax.psum(array, axis)
    return array


def lookup(classes, table):
    summed = jnp.zeros(classes.shape, jnp.float32)
    for level in range(table.shape[1]):
        summed = summed + jnp.where(
            classes == level, table[:, level][:, None, None], jnp.float32(0.0)
        )
    return summed


def harmonic(first, second):
    return 2.0 * first * second / (first + second)


def factor(diagonal, up_edge):
    inverses = []
    factors = []
    for level in range(diagonal.shape[0]):
        pivots = diagonal[level]
        if level > 0:
            pivots = pivots + up_edge[level - 1] * factors[level - 1]
        inverse = 1.0 / pivots
        inverses.append(inverse)
        factors.append(-up_edge[level] * inverse)
    return (jnp.stack(inverses), jnp.stack(factors))


def solve_block(inverses, factors, up_edge, source_term):
    forward = []
    for level in range(source_term.shape[0]):
        entries = source_term[level]
        if level > 0:
            entries = entries + up_edge[level - 1] * forward[level - 1]
        forward.append(entries * inverses[level])
    result = [forward[-1]]
    level = 0
    result.insert(0, forward[level] - factors[level] * result[0])
    return jnp.stack(result)


def plane_extend(field):
    return padded(field, ((GX, 2), (GY, 1)), 1)


def layer_extend(field):
    return padded_2(field, (("gz", 0),), 1)


def merged_sums(residual, precond, image_field):
    return (
        by_axis(jnp.sum(residual * precond), GX_GY_GZ),
        by_axis(jnp.sum(image_field * precond), GX_GY_GZ),
    )


def recurrence(load_current, sink_mask, pad_mask, plane_class, via_class, plane_table, via_table):
    n_layers, n_rows, n_cols = plane_class.shape
    g_plane = lookup(plane_class, plane_table)
    g_via = lookup(via_class, via_table)
    plane_ext = plane_extend(g_plane)
    middle = plane_ext[:, 1:-1, :]
    across = harmonic(middle[:, :, :-1], middle[:, :, 1:])
    east_edge = across[:, :, 1:]
    west_edge = across[:, :, :-1]
    column = plane_ext[:, :, 1:-1]
    along_rows = harmonic(column[:, :-1], column[:, 1:])
    north_edge = along_rows[:, 1:]
    south_edge = along_rows[:, :-1]
    via_ext = layer_extend(g_via)
    vertical = harmonic(via_ext[:-1], via_ext[1:])
    up_edge = vertical[1:]
    down_edge = vertical[:-1]
    group_index = lax.axis_index("gz")
    is_top = group_index == lax.axis_size("gz") - 1
    is_bottom = group_index == 0
    pad_plane = jnp.where(is_top, PAD_CONDUCTANCE * pad_mask.astype(jnp.float32), jnp.float32(0.0))
    pad_layer = jnp.concatenate(
        [jnp.zeros((n_layers - 1, n_rows, n_cols), jnp.float32), pad_plane[None]], 0
    )
    diagonal = east_edge + west_edge + north_edge + south_edge + up_edge + down_edge + pad_layer
    inverses, factors = factor(diagonal, up_edge)

    def precondition(residual):
        return solve_block(inverses, factors, up_edge, residual)

    def operate(field):
        inner = plane_extend(field)
        layer_ext = layer_extend(field)
        above_field = layer_ext[2:]
        below_field = layer_ext[:-2]
        return (
            diagonal * field
            - east_edge * inner[:, 1:-1, 2:]
            - west_edge * inner[:, 1:-1, :-2]
            - north_edge * inner[:, 2:, 1:-1]
            - south_edge * inner[:, :-2, 1:-1]
            - up_edge * above_field
            - down_edge * below_field
        )

    source = jnp.where(is_bottom, sink_mask.astype(jnp.float32) * load_current, jnp.float32(0.0))
    right_side = jnp.concatenate(
        [source[None], jnp.zeros((n_layers - 1, n_rows, n_cols), jnp.float32)], 0
    )
    voltage = jnp.zeros((n_layers, n_rows, n_cols), jnp.float32)
    residual = right_side
    precond = precondition(residual)
    image_field = operate(precond)
    weight_now, curvature = merged_sums(residual, precond, image_field)
    step_size = weight_now / curvature
    direction = precond
    image_dir = image_field
    for iteration in range(ITERS):
        voltage = voltage + step_size * direction
        residual = residual - step_size * image_dir
        if iteration + 1 < ITERS:
            precond = precondition(residual)
            image_field = operate(precond)
            weight_next, curvature = merged_sums(residual, precond, image_field)
            momentum = weight_next / weight_now
            step_size = weight_next / (curvature - momentum * weight_next / step_size)
            direction = precond + momentum * direction
            image_dir = image_field + momentum * image_dir
            weight_now = weight_next
    return (voltage, residual)


STEP = 8
LANES = 128
GUARD = 0.02
GRANT = 16 * 1024 * 1024
VMEM = pl.BlockSpec(memory_space=pltpu.VMEM)
SMEM = pl.BlockSpec(memory_space=pltpu.SMEM)


def select_class(classes, entry):
    low = (classes & 1) != 0
    mid = (classes & 2) != 0
    high = (classes & 4) != 0
    pairs = [jnp.where(low, entry(2 * k + 1), entry(2 * k)) for k in range(4)]
    return jnp.where(high, jnp.where(mid, pairs[3], pairs[2]), jnp.where(mid, pairs[1], pairs[0]))


def via_kernel(gz, table, classes, via_i, inner):
    group = gz[0]
    for r in range(0, via_i.shape[0], STEP):
        rows = pl.ds(r, STEP)
        one = select_class(classes[1 - group, rows, :], lambda k: table[1 - group, k])
        two = select_class(classes[group, rows, :], lambda k: table[group, k])
        via_i[rows, :] = one
        inner[rows, :] = harmonic(one, two)


def stage_columns(stage, r, field_i, field_o):
    lane = lax.broadcasted_iota(jnp.int32, (STEP, LANES), 1)
    last = field_i.shape[1] - LANES
    first_o = pltpu.roll(field_o[:, :LANES], 1, 1)
    last_i = pltpu.roll(field_i[:, last:], 3, 1)
    last_o = pltpu.roll(field_o[:, last:], 4, 1)
    picked = jnp.where(lane == 2, last_i, last_o)
    picked = jnp.where(lane == 1, first_o, picked)
    stage[pl.ds(r, STEP), :] = jnp.where(lane == 0, field_i[:, :LANES], picked)


def send_edges(stage, field_i, field_o, edges):
    first_row, last_row, first_col, last_col = edges
    n_rows = field_i.shape[0]
    first_row[0:1, :] = field_i[0:1, :]
    first_row[1:2, :] = field_o[0:1, :]
    last_row[0:1, :] = field_i[n_rows - 1 : n_rows, :]
    last_row[1:2, :] = field_o[n_rows - 1 : n_rows, :]
    turned = stage[...].T
    first_col[...] = turned[0:2, :]
    last_col[...] = turned[2:4, :]


def take_columns(flat, west, east, columns):
    flat[...] = jnp.zeros(flat.shape, jnp.float32)
    flat[0:2, :] = west[...]
    flat[2:4, :] = east[...]
    columns[...] = flat[...].T


def plane_kernel(gz, table, classes, plane_i, plane_o, *rest):
    edges, stage = rest[:4], rest[4]
    group = gz[0]
    stage[...] = jnp.zeros(stage.shape, jnp.float32)
    for r in range(0, plane_i.shape[0], STEP):
        rows = pl.ds(r, STEP)
        one = select_class(classes[1 - group, rows, :], lambda k: table[1 - group, k])
        two = select_class(classes[group, rows, :], lambda k: table[group, k])
        plane_i[rows, :] = one
        plane_o[rows, :] = two
        stage_columns(stage, r, one, two)
    send_edges(stage, plane_i, plane_o, edges)


def around(field, layer, r, south, north, columns):
    n_rows, n_cols = field.shape
    own = field[pl.ds(r, STEP), :]
    sub = lax.broadcasted_iota(jnp.int32, own.shape, 0)
    lane = lax.broadcasted_iota(jnp.int32, own.shape, 1)
    if r:
        below = field[r - 1 : r - 1 + STEP, :]
    else:
        below = jnp.where(sub == 0, south[layer : layer + 1, :], pltpu.roll(own, 1, 0))
    if r + STEP < n_rows:
        above = field[r + 1 : r + 1 + STEP, :]
    else:
        above = jnp.where(
            sub == STEP - 1, north[layer : layer + 1, :], pltpu.roll(own, STEP - 1, 0)
        )
    west_col = columns[pl.ds(r, STEP), layer : layer + 1]
    east_col = columns[pl.ds(r, STEP), layer + 2 : layer + 3]
    west = jnp.where(lane == 0, west_col, pltpu.roll(own, 1, 1))
    east = jnp.where(lane == n_cols - 1, east_col, pltpu.roll(own, n_cols - 1, 1))
    return own, east, west, above, below


def fold(total):
    width = total.shape[1]
    while width > LANES:
        width //= 2
        total = total[:, :width] + total[:, width:]
    return jnp.sum(total, axis=0, keepdims=True)


def edge_kernel(
    gz, plane_i, plane_o, south, north, west, east, via_i, via_far, inner, load, sink, pad, *rest
):
    edges_i, edges_o = rest[0:4], rest[4:8]
    cross, inv_ii, inv_oo, inv_io, v_i, v_o, source, payload = rest[8:16]
    sends, part = rest[16:20], rest[20]
    stage, flat, columns = rest[21:]
    group = gz[0]
    take_columns(flat, west, east, columns)
    stage[...] = jnp.zeros(stage.shape, jnp.float32)
    total = jnp.zeros((STEP, plane_i.shape[1]), jnp.float32)
    for r in range(0, plane_i.shape[0], STEP):
        rows = pl.ds(r, STEP)
        sums = []
        for layer, field, edges in ((0, plane_i, edges_i), (1, plane_o, edges_o)):
            own, *others = around(field, layer, r, south, north, columns)
            values = [harmonic(own, other) for other in others]
            for edge, value in zip(edges, values):
                edge[rows, :] = value
            sums.append(values[0] + values[1] + values[2] + values[3])
        up = inner[rows, :]
        far = harmonic(via_i[rows, :], via_far[rows, :])
        cross[rows, :] = far
        pads = PAD_CONDUCTANCE * pad[rows, :].astype(jnp.float32)
        diag_i = sums[0] + up + far
        diag_o = sums[1] + up + jnp.where(group == 1, pads, 0.0)
        inverse = 1.0 / (diag_i * diag_o - up * up)
        ii, oo, io = diag_o * inverse, diag_i * inverse, up * inverse
        drawn = sink[rows, :].astype(jnp.float32) * load[rows, :]
        drawn = jnp.where(group == 0, drawn, 0.0)
        one, two = io * drawn, oo * drawn
        inv_ii[rows, :], inv_oo[rows, :], inv_io[rows, :] = ii, oo, io
        source[rows, :] = drawn
        v_i[rows, :], v_o[rows, :] = one, two
        payload[rows, :] = jnp.where(group == 0, one, ii)
        stage_columns(stage, r, one, two)
        total = total + two * drawn
    send_edges(stage, v_i, v_o, sends)
    part[...] = jnp.zeros(part.shape, jnp.float32)
    part[0:1, :] = fold(total)


def stencil(field, layer, r, halos, columns, edges):
    own, *others = around(field, layer, r, halos[0], halos[1], columns)
    rows = pl.ds(r, STEP)
    east, west, above, below = [edge[rows, :] * value for edge, value in zip(edges, others)]
    return own, (east + west) + (above + below)


def first_kernel(gz, v_i, v_o, south, north, west, east, *rest):
    edges_i, edges_o = rest[0:4], rest[4:8]
    cross, inv_ii, inv_oo, inv_io, given, before = rest[8:14]
    n_i, n_o, w_i, w_o, far = rest[14:19]
    sends, part = rest[19:23], rest[23]
    stage, flat, columns = rest[24:]
    group = gz[0]
    take_columns(flat, west, east, columns)
    stage[...] = jnp.zeros(stage.shape, jnp.float32)
    sums = [jnp.zeros((STEP, v_i.shape[1]), jnp.float32)] * 2
    for r in range(0, v_i.shape[0], STEP):
        rows = pl.ds(r, STEP)
        own_i, out_i = stencil(v_i, 0, r, (south, north), columns, edges_i)
        own_o, out_o = stencil(v_o, 1, r, (south, north), columns, edges_o)
        link, got = cross[rows, :], given[rows, :]
        out_i = out_i + jnp.where(group == 1, link * got, 0.0)
        far[rows, :] = link * own_i * got
        ii, oo, io = inv_ii[rows, :], inv_oo[rows, :], inv_io[rows, :]
        one, two = ii * out_i + io * out_o, io * out_i + oo * out_o
        n_i[rows, :], n_o[rows, :] = out_i, out_o
        w_i[rows, :], w_o[rows, :] = one, two
        stage_columns(stage, r, one, two)
        sums[0] = sums[0] + (own_i * out_i + own_o * out_o)
        sums[1] = sums[1] + (one * out_i + two * out_o)
    send_edges(stage, w_i, w_o, sends)
    part[...] = before[...]
    part[1:2, :] = fold(sums[0])
    part[2:3, :] = fold(sums[1])


def second_kernel(gz, v_i, v_o, south, north, west, east, *rest):
    edges_i, edges_o = rest[0:4], rest[4:8]
    cross, inv_ii, inv_oo, inv_io, made, given, before = rest[8:15]
    n_i, n_o, w_i, w_o = rest[15:19]
    sends, part = rest[19:23], rest[23]
    stage, flat, columns = rest[24:]
    group = gz[0]
    take_columns(flat, west, east, columns)
    stage[...] = jnp.zeros(stage.shape, jnp.float32)
    sums = [jnp.zeros((STEP, v_i.shape[1]), jnp.float32)] * 2
    for r in range(0, v_i.shape[0], STEP):
        rows = pl.ds(r, STEP)
        own_i, out_i = stencil(v_i, 0, r, (south, north), columns, edges_i)
        own_o, out_o = stencil(v_o, 1, r, (south, north), columns, edges_o)
        out_i = out_i + cross[rows, :] * jnp.where(group == 0, made[rows, :], given[rows, :])
        ii, oo, io = inv_ii[rows, :], inv_oo[rows, :], inv_io[rows, :]
        one, two = ii * out_i + io * out_o, io * out_i + oo * out_o
        n_i[rows, :], n_o[rows, :] = out_i, out_o
        w_i[rows, :], w_o[rows, :] = one, two
        stage_columns(stage, r, one, two)
        sums[0] = sums[0] + (own_i * out_i + own_o * out_o)
        sums[1] = sums[1] + (one * out_i + two * out_o)
    send_edges(stage, w_i, w_o, sends)
    part[...] = before[...]
    part[3:4, :] = fold(sums[0])
    part[4:5, :] = fold(sums[1])


def third_kernel(v_i, v_o, south, north, west, east, *rest):
    edges_i, edges_o = rest[0:4], rest[4:8]
    cross, given, before = rest[8:11]
    n_i, n_o, spread = rest[11:14]
    flat, columns = rest[14:]
    take_columns(flat, west, east, columns)
    total = jnp.zeros((STEP, v_i.shape[1]), jnp.float32)
    for r in range(0, v_i.shape[0], STEP):
        rows = pl.ds(r, STEP)
        own_i, out_i = stencil(v_i, 0, r, (south, north), columns, edges_i)
        own_o, out_o = stencil(v_o, 1, r, (south, north), columns, edges_o)
        out_i = out_i + cross[rows, :] * given[rows, :]
        n_i[rows, :], n_o[rows, :] = out_i, out_o
        total = total + (own_i * out_i + own_o * out_o)
    row = lax.broadcasted_iota(jnp.int32, before.shape, 0)
    part = jnp.where(row == 5, fold(total), before[...])
    for k in range(spread.shape[0]):
        spread[k] = part


def tree(parts):
    values = [parts[k] for k in range(parts.shape[0])]
    while len(values) > 1:
        values = [a + b for a, b in zip(values[::2], values[1::2])]
    return values[0]


def relay_kernel(parts, spread):
    total = tree(parts)
    for k in range(spread.shape[0]):
        spread[k] = total


def solve_kernel(parts, coefs, flag):
    sums = jnp.sum(tree(parts), axis=1, keepdims=True)
    g = [jnp.broadcast_to(sums[k : k + 1, :], (1, LANES)) for k in range(6)]
    step = [g[k] - g[k + 1] for k in range(5)]
    scale = [lax.rsqrt(g[0]), lax.rsqrt(g[2]), lax.rsqrt(g[4])]

    def entry(i, j):
        return step[i + j] * scale[i] * scale[j]

    d0 = entry(0, 0)
    l10, l20 = entry(1, 0) / d0, entry(2, 0) / d0
    d1 = entry(1, 1) - l10 * entry(1, 0)
    e21 = entry(2, 1) - l20 * entry(1, 0)
    l21 = e21 / d1
    d2 = entry(2, 2) - l20 * entry(2, 0) - l21 * e21
    y0 = g[0] * scale[0]
    y1 = g[1] * scale[1] - l10 * y0
    y2 = g[2] * scale[2] - l20 * y0 - l21 * y1
    x2 = y2 / d2
    x1 = y1 / d1 - l21 * x2
    x0 = y0 / d0 - l10 * x1 - l20 * x2
    c0, c1, c2 = x0 * scale[0], x1 * scale[1], x2 * scale[2]
    for k, value in enumerate((c0, c1, c2, 1.0 - c0, c0 - c1, c1 - c2)):
        coefs[k : k + 1, :] = value
    coefs[6:8, :] = jnp.zeros((2, LANES), jnp.float32)
    good = (d0 > GUARD) & (d1 > GUARD) & (d2 > GUARD)
    flag[...] = jnp.where(good, 1, 0)


def combine_kernel(gz, coefs, source, *rest):
    fields, volts, left = rest[:12], rest[12], rest[13]
    group = gz[0]
    width = source.shape[1]
    c = [jnp.broadcast_to(coefs[k : k + 1, 0:1], (STEP, width)) for k in range(6)]
    for r in range(0, source.shape[0], STEP):
        rows = pl.ds(r, STEP)
        v0i, v0o, v1i, v1o, v2i, v2o, n0i, n0o, n1i, n1o, n2i, n2o = [f[rows, :] for f in fields]
        volts[1 - group, rows, :] = c[0] * v0i + c[1] * v1i + c[2] * v2i
        volts[group, rows, :] = c[0] * v0o + c[1] * v1o + c[2] * v2o
        left[1 - group, rows, :] = c[4] * n0i + c[5] * n1i + c[2] * n2i
        left[group, rows, :] = (
            c[3] * source[rows, :] + c[4] * n0o + c[5] * n1o + c[2] * n2o
        )


def call(kernel, name, outs, scratch, n_smem, *args):
    return pl.pallas_call(
        kernel,
        name=name,
        in_specs=[SMEM] * n_smem + [VMEM] * (len(args) - n_smem),
        out_specs=[VMEM] * len(outs),
        out_shape=outs,
        scratch_shapes=scratch,
        compiler_params=pltpu.CompilerParams(vmem_limit_bytes=GRANT),
    )(*args)


def halos(first_row, last_row, first_col, last_col):
    def ring(axis):
        size = lax.axis_size(axis)
        return [(i, (i + 1) % size) for i in range(size)]

    up_y, up_x = ring(GY), ring(GX)
    back_y, back_x = [(b, a) for a, b in up_y], [(b, a) for a, b in up_x]
    return (
        lax.ppermute(last_row, GY, up_y),
        lax.ppermute(first_row, GY, back_y),
        lax.ppermute(last_col, GX, up_x),
        lax.ppermute(first_col, GX, back_x),
    )


def shards(load_current, sink_mask, pad_mask, plane_class, via_class, plane_table, via_table):
    _, n_rows, n_cols = plane_class.shape
    tall = -(-n_rows // LANES) * LANES
    f32 = jnp.float32
    plane = jax.ShapeDtypeStruct((n_rows, n_cols), f32)
    both = jax.ShapeDtypeStruct((2, n_rows, n_cols), f32)
    row = jax.ShapeDtypeStruct((2, n_cols), f32)
    col = jax.ShapeDtypeStruct((2, tall), f32)
    sheet = jax.ShapeDtypeStruct((STEP, LANES), f32)
    edge_outs = [row, row, col, col]
    stage = pltpu.VMEM((tall, LANES), f32)
    turn = [pltpu.VMEM((LANES, tall), f32), pltpu.VMEM((tall, LANES), f32)]
    gz = lax.axis_index("gz").reshape(1).astype(jnp.int32)
    swap = [(0, 1), (1, 0)]
    n_gx, n_rest = lax.axis_size(GX), lax.axis_size(("gy_0", "gy_1", "gz"))

    via_i, inner = call(via_kernel, "via", [plane] * 2, [], 2, gz, via_table, via_class)
    via_far = lax.ppermute(via_i, "gz", swap)
    plane_i, plane_o, *sends = call(
        plane_kernel, "plane", [plane] * 2 + edge_outs, [stage], 2, gz, plane_table, plane_class
    )
    near = halos(*sends)
    outs = call(
        edge_kernel, "edge", [plane] * 16 + edge_outs + [sheet], [stage] + turn, 1,
        gz, plane_i, plane_o, *near, via_i, via_far, inner, load_current, sink_mask, pad_mask,
    )
    edges, (cross, inv_ii, inv_oo, inv_io) = outs[0:8], outs[8:12]
    v0i, v0o, source, payload = outs[12:16]
    sends, part = outs[16:20], outs[20]
    given = lax.ppermute(payload, "gz", swap)
    near = halos(*sends)
    n0i, n0o, v1i, v1o, made, *sends, part = call(
        first_kernel, "first", [plane] * 5 + edge_outs + [sheet], [stage] + turn, 1,
        gz, v0i, v0o, *near, *edges, cross, inv_ii, inv_oo, inv_io, given, part,
    )
    given = lax.ppermute(v1i, "gz", [(0, 1)])
    near = halos(*sends)
    n1i, n1o, v2i, v2o, *sends, part = call(
        second_kernel, "second", [plane] * 4 + edge_outs + [sheet], [stage] + turn, 1,
        gz, v1i, v1o, *near, *edges, cross, inv_ii, inv_oo, inv_io, made, given, part,
    )
    given = lax.ppermute(v2i, "gz", swap)
    near = halos(*sends)
    n2i, n2o, spread = call(
        third_kernel, "third",
        [plane] * 2 + [jax.ShapeDtypeStruct((n_gx, STEP, LANES), f32)], turn, 0,
        v2i, v2o, *near, *edges, cross, given, part,
    )
    parts = lax.all_to_all(spread, GX, 0, 0, tiled=True)
    (spread,) = call(
        relay_kernel, "relay", [jax.ShapeDtypeStruct((n_rest, STEP, LANES), f32)], [], 0, parts
    )
    parts = lax.all_to_all(spread, ("gy_0", "gy_1", "gz"), 0, 0, tiled=True)
    coefs, flag = call(
        solve_kernel, "solve", [sheet, jax.ShapeDtypeStruct((1, LANES), jnp.int32)], [], 0, parts
    )

    quick = call(
        combine_kernel, "combine", [both] * 2, [], 1, gz, coefs, source,
        v0i, v0o, v1i, v1o, v2i, v2o, n0i, n0o, n1i, n1o, n2i, n2o,
    )

    def careful():
        return recurrence(
            load_current, sink_mask, pad_mask, plane_class, via_class, plane_table, via_table
        )

    return lax.cond(flag[0, 0] == 1, lambda: tuple(quick), careful)


def solution(mesh):
    split = Mesh(
        mesh.devices.reshape(8, 2, 2, 4, mesh.shape["gz"]), ("gx_0", "gx_1", "gy_0", "gy_1", "gz")
    )
    placed = (
        P(GY, GX),
        P(GY, GX),
        P(GY, GX),
        P("gz", GY, GX),
        P("gz", GY, GX),
        P("gz", None),
        P("gz", None),
    )
    return jax.shard_map(
        shards,
        mesh=split,
        in_specs=placed,
        out_specs=(P("gz", GY, GX), P("gz", GY, GX)),
        check_vma=False,
    )
```

```python
import jax
import jax.numpy as jnp
from jax import lax
from jax.experimental import pallas as pl
from jax.experimental.pallas import tpu as pltpu
from jax.sharding import Mesh
from jax.sharding import PartitionSpec as P

ITERS = 3
GX = ("gx_0", "gx_1")
GY = ("gy_0", "gy_1")
GX_GY_GZ = ("gx_0", "gx_1", "gy_0", "gy_1", "gz")


PAD_CONDUCTANCE = 20.0


def padded(array, sides, width):
    edges = {}
    for axis, dim in sides:
        peers, length = (lax.axis_size(axis), array.shape[dim])
        up = [(i, (i + 1) % peers) for i in range(peers)]
        last = lax.slice_in_dim(array, length - width, length, axis=dim)
        leading = lax.slice_in_dim(array, 0, width, axis=dim)
        edges[dim] = (
            lax.ppermute(last, axis, up),
            lax.ppermute(leading, axis, [(b, a) for a, b in up]),
        )
    done = []
    for _, dim in sides:
        low, high = edges[dim]
        around = [(width, width) if d in done else (0, 0) for d in range(array.ndim)]
        array = jnp.concatenate([jnp.pad(low, around), array, jnp.pad(high, around)], axis=dim)
        done.append(dim)
    return array


def padded_2(block, sides, width):
    for axis, dim in sides:
        count = lax.axis_size(axis)
        forward = [(i, i + 1) for i in range(count - 1)]
        backward = [(target, source) for source, target in forward]
        low = lax.ppermute(
            lax.slice_in_dim(block, block.shape[dim] - width, None, axis=dim), axis, forward
        )
        high = lax.ppermute(lax.slice_in_dim(block, 0, width, axis=dim), axis, backward)
        block = jnp.concatenate([low, block, high], axis=dim)
    return block


def by_axis(array, axes):
    for axis in axes:
        array = lax.psum(array, axis)
    return array


def lookup(classes, table):
    summed = jnp.zeros(classes.shape, jnp.float32)
    for level in range(table.shape[1]):
        summed = summed + jnp.where(
            classes == level, table[:, level][:, None, None], jnp.float32(0.0)
        )
    return summed


def harmonic(first, second):
    return 2.0 * first * second / (first + second)


def factor(diagonal, up_edge):
    inverses = []
    factors = []
    for level in range(diagonal.shape[0]):
        pivots = diagonal[level]
        if level > 0:
            pivots = pivots + up_edge[level - 1] * factors[level - 1]
        inverse = 1.0 / pivots
        inverses.append(inverse)
        factors.append(-up_edge[level] * inverse)
    return (jnp.stack(inverses), jnp.stack(factors))


def solve_block(inverses, factors, up_edge, source_term):
    forward = []
    for level in range(source_term.shape[0]):
        entries = source_term[level]
        if level > 0:
            entries = entries + up_edge[level - 1] * forward[level - 1]
        forward.append(entries * inverses[level])
    result = [forward[-1]]
    level = 0
    result.insert(0, forward[level] - factors[level] * result[0])
    return jnp.stack(result)


def plane_extend(field):
    return padded(field, ((GX, 2), (GY, 1)), 1)


def layer_extend(field):
    return padded_2(field, (("gz", 0),), 1)


def merged_sums(residual, precond, image_field):
    return (
        by_axis(jnp.sum(residual * precond), GX_GY_GZ),
        by_axis(jnp.sum(image_field * precond), GX_GY_GZ),
    )


def recurrence(load_current, sink_mask, pad_mask, plane_class, via_class, plane_table, via_table):
    n_layers, n_rows, n_cols = plane_class.shape
    g_plane = lookup(plane_class, plane_table)
    g_via = lookup(via_class, via_table)
    plane_ext = plane_extend(g_plane)
    middle = plane_ext[:, 1:-1, :]
    across = harmonic(middle[:, :, :-1], middle[:, :, 1:])
    east_edge = across[:, :, 1:]
    west_edge = across[:, :, :-1]
    column = plane_ext[:, :, 1:-1]
    along_rows = harmonic(column[:, :-1], column[:, 1:])
    north_edge = along_rows[:, 1:]
    south_edge = along_rows[:, :-1]
    via_ext = layer_extend(g_via)
    vertical = harmonic(via_ext[:-1], via_ext[1:])
    up_edge = vertical[1:]
    down_edge = vertical[:-1]
    group_index = lax.axis_index("gz")
    is_top = group_index == lax.axis_size("gz") - 1
    is_bottom = group_index == 0
    pad_plane = jnp.where(is_top, PAD_CONDUCTANCE * pad_mask.astype(jnp.float32), jnp.float32(0.0))
    pad_layer = jnp.concatenate(
        [jnp.zeros((n_layers - 1, n_rows, n_cols), jnp.float32), pad_plane[None]], 0
    )
    diagonal = east_edge + west_edge + north_edge + south_edge + up_edge + down_edge + pad_layer
    inverses, factors = factor(diagonal, up_edge)

    def precondition(residual):
        return solve_block(inverses, factors, up_edge, residual)

    def operate(field):
        inner = plane_extend(field)
        layer_ext = layer_extend(field)
        above_field = layer_ext[2:]
        below_field = layer_ext[:-2]
        return (
            diagonal * field
            - east_edge * inner[:, 1:-1, 2:]
            - west_edge * inner[:, 1:-1, :-2]
            - north_edge * inner[:, 2:, 1:-1]
            - south_edge * inner[:, :-2, 1:-1]
            - up_edge * above_field
            - down_edge * below_field
        )

    source = jnp.where(is_bottom, sink_mask.astype(jnp.float32) * load_current, jnp.float32(0.0))
    right_side = jnp.concatenate(
        [source[None], jnp.zeros((n_layers - 1, n_rows, n_cols), jnp.float32)], 0
    )
    voltage = jnp.zeros((n_layers, n_rows, n_cols), jnp.float32)
    residual = right_side
    precond = precondition(residual)
    image_field = operate(precond)
    weight_now, curvature = merged_sums(residual, precond, image_field)
    step_size = weight_now / curvature
    direction = precond
    image_dir = image_field
    for iteration in range(ITERS):
        voltage = voltage + step_size * direction
        residual = residual - step_size * image_dir
        if iteration + 1 < ITERS:
            precond = precondition(residual)
            image_field = operate(precond)
            weight_next, curvature = merged_sums(residual, precond, image_field)
            momentum = weight_next / weight_now
            step_size = weight_next / (curvature - momentum * weight_next / step_size)
            direction = precond + momentum * direction
            image_dir = image_field + momentum * image_dir
            weight_now = weight_next
    return (voltage, residual)


STEP = 8
LANES = 128
DEEP = 4
GUARD = 0.02
GRANT = 16 * 1024 * 1024
N_OWN = 6
N_FAR = 4
VMEM = pl.BlockSpec(memory_space=pltpu.VMEM)
SMEM = pl.BlockSpec(memory_space=pltpu.SMEM)


def block(k):
    return pl.ds(pl.multiple_of(k * STEP, STEP), STEP)


def select_class(classes, entry):
    low = (classes & 1) != 0
    mid = (classes & 2) != 0
    high = (classes & 4) != 0
    pairs = [jnp.where(low, entry(2 * k + 1), entry(2 * k)) for k in range(4)]
    return jnp.where(high, jnp.where(mid, pairs[3], pairs[2]), jnp.where(mid, pairs[1], pairs[0]))


def via_kernel(gz, table, classes, via, pair, lone):
    group = gz[0]
    n_rows = via.shape[1]
    half = n_rows // 2 // STEP

    def fill(k, carry):
        rows = block(k)
        one = select_class(classes[1 - group, rows, :], lambda e: table[1 - group, e])
        two = select_class(classes[group, rows, :], lambda e: table[group, e])
        via[0, rows, :] = one
        via[1, rows, :] = harmonic(one, two)
        return carry

    lax.fori_loop(0, n_rows // STEP, fill, 0, unroll=2)

    def copy(k, carry):
        for f in range(2):
            pair[f, block(k), :] = via[f, block(k + (1 - group) * half), :]
        lone[block(k), :] = via[0, block(k + group * half), :]
        return carry

    lax.fori_loop(0, half, copy, 0, unroll=2)


def plane_kernel(gz, table, classes, load, sink, pad, via, plane, drawn, pair, top, bottom):
    group = gz[0]
    n_rows = plane.shape[1]
    half = n_rows // 2 // STEP

    def fill(k, carry):
        rows = block(k)
        plane[0, rows, :] = select_class(
            classes[1 - group, rows, :], lambda e: table[1 - group, e]
        )
        plane[1, rows, :] = select_class(classes[group, rows, :], lambda e: table[group, e])
        plane[2, rows, :] = PAD_CONDUCTANCE * pad[rows, :].astype(jnp.float32)
        drawn[rows, :] = sink[rows, :].astype(jnp.float32) * load[rows, :]
        return carry

    lax.fori_loop(0, n_rows // STEP, fill, 0, unroll=2)

    def copy(k, carry):
        for f in range(2):
            pair[f, block(k), :] = plane[f, block(k + (1 - group) * half), :]
        return carry

    lax.fori_loop(0, half, copy, 0, unroll=2)
    for f in range(N_OWN):
        at = pl.ds(DEEP * f, DEEP)
        top[at, :] = field_rows(plane, via, drawn, f, pl.ds(0, DEEP))
        bottom[at, :] = field_rows(plane, via, drawn, f, pl.ds(n_rows - DEEP, DEEP))


def field_rows(plane, via, drawn, f, rows):
    if f == 4:
        return drawn[rows, :]
    if f in (2, 3):
        return via[f - 2, rows, :]
    return plane[2 if f == 5 else f, rows, :]


def tile_of(stack, f, upper):
    rows = stack[f // 2 * STEP : f // 2 * STEP + STEP, :]
    return rows if (f % 2 == 1) == upper else pltpu.roll(rows, DEEP, 0)


def columns_kernel(plane, via, drawn, south, north, first, last, stage):
    n_rows, n_cols = drawn.shape
    lane = lax.broadcasted_iota(jnp.int32, (STEP, LANES), 1)
    place = lane // DEEP

    def put(rows, pick):
        out = jnp.zeros((STEP, LANES), jnp.float32)
        for f in range(N_OWN):
            value = pick(f)
            head, tail = value[:, :LANES], value[:, n_cols - LANES :]
            if f:
                head = pltpu.roll(head, DEEP * f, 1)
            tail = pltpu.roll(tail, DEEP * (N_OWN + f + 1), 1)
            out = jnp.where(place == f, head, jnp.where(place == N_OWN + f, tail, out))
        stage[rows, :] = out

    def inner(k, carry):
        put(block(k + 1), lambda f: field_rows(plane, via, drawn, f, block(k)))
        return carry

    put(pl.ds(0, STEP), lambda f: tile_of(south, f, True))
    lax.fori_loop(0, n_rows // STEP, inner, 0, unroll=2)
    put(pl.ds(n_rows + STEP, STEP), lambda f: tile_of(north, f, False))
    rest = n_rows + 2 * STEP
    stage[rest:, :] = jnp.zeros((stage.shape[0] - rest, LANES), jnp.float32)
    turned = stage[...].T
    size = DEEP * N_OWN
    first[...] = turned[:size, :]
    last[...] = turned[size : 2 * size, :]


def side(strip, slot, blank):
    lane = lax.broadcasted_iota(jnp.int32, strip.shape, 1)
    turned = pltpu.roll(strip, (LANES - DEEP - 2 * DEEP * slot) % LANES, 1)
    return jnp.where((lane < DEEP) | (lane >= LANES - DEEP), turned, blank)


def corner_kernel(gz, plane, via, south, north, west, east, small):
    group = gz[0]
    half, tall_rows = plane.shape[1] // 2, west.shape[1]
    for f in range(N_FAR):
        at, mine = 2 * DEEP * f, pl.ds(DEEP * f, DEEP)
        inner = field_rows(plane, via, None, f, pl.ds(half - DEEP, DEEP))
        small[at : at + DEEP, :] = jnp.where(group == 0, inner, south[mine, :])
        inner = field_rows(plane, via, None, f, pl.ds(half, DEEP))
        small[at + DEEP : at + 2 * DEEP, :] = jnp.where(group == 0, north[mine, :], inner)
    at, size = 2 * DEEP * N_FAR, DEEP * N_FAR
    small[at : at + size, :tall_rows] = west[:size, :]
    small[at : at + size, tall_rows:] = east[:size, :]


def own_kernel(gz, plane, via, drawn, south, north, west, east, near, edge_e, edge_n, near_sum, far_sum, wide, flat, tall):
    group = gz[0]
    n_rows, n_cols = drawn.shape
    half = n_rows // 2
    flat[...] = jnp.zeros(flat.shape, jnp.float32)
    for f in range(N_OWN):
        at = 2 * DEEP * f
        flat[at : at + DEEP, :] = west[DEEP * f : DEEP * f + DEEP, :]
        flat[at + DEEP : at + 2 * DEEP, :] = east[DEEP * f : DEEP * f + DEEP, :]
    tall[...] = flat[...].T

    def put(rows, pick):
        strip = tall[rows, :]
        for f in range(N_OWN):
            wide[f, rows, :n_cols] = pick(f)
            wide[f, rows, n_cols:] = side(strip, f, 1.0 if f < N_FAR else 0.0)

    def inner(k, carry):
        put(block(k + 1), lambda f: field_rows(plane, via, drawn, f, block(k)))
        return carry

    put(pl.ds(0, STEP), lambda f: tile_of(south, f, True))
    lax.fori_loop(0, n_rows // STEP, inner, 0, unroll=2)
    put(pl.ds(n_rows + STEP, STEP), lambda f: tile_of(north, f, False))
    last = n_rows // STEP + 1

    def around(layer, k):
        value = wide[layer, block(k), :]
        over = wide[layer, block(jnp.minimum(k + 1, last)), :]
        under = wide[layer, block(jnp.maximum(k - 1, 0)), :]
        sub = lax.broadcasted_iota(jnp.int32, value.shape, 0)
        above = jnp.where(
            sub == STEP - 1, pltpu.roll(over, STEP - 1, 0), pltpu.roll(value, STEP - 1, 0)
        )
        below = jnp.where(sub == 0, pltpu.roll(under, 1, 0), pltpu.roll(value, 1, 0))
        to_east, to_north = harmonic(value, eastward(value)), harmonic(value, above)
        return to_east, to_north, (to_east + westward(to_east)) + (to_north + harmonic(value, below))

    def frame(k, carry):
        at = k + group * (half // STEP)
        for layer in range(2):
            to_east, to_north, total = around(layer, at)
            edge_e[layer, block(k), :] = to_east
            edge_n[layer, block(k), :] = to_north
            near_sum[layer, block(k), :] = total
            near[2 + layer, block(k), :] = wide[N_FAR + layer, block(at), :]
            near[layer, block(k), :] = wide[2 + layer, block(at), :]
        return carry

    lax.fori_loop(0, half // STEP + 2, frame, 0, unroll=2)

    def other(k, carry):
        for layer in range(2):
            total = around(layer, k + 1 + (1 - group) * (half // STEP))[2]
            far_sum[layer, block(k), :] = total[:, :n_cols]
        return carry

    lax.fori_loop(0, half // STEP, other, 0, unroll=2)


def above_of(field, j, r):
    n_rows = field.shape[1]
    if r + STEP < n_rows:
        return field[j, r + 1 : r + 1 + STEP, :]
    return pltpu.roll(field[j, r : r + STEP, :], STEP - 1, 0)


def below_of(field, j, r):
    if r:
        return field[j, r - 1 : r - 1 + STEP, :]
    return pltpu.roll(field[j, r : r + STEP, :], 1, 0)


def eastward(value):
    return pltpu.roll(value, value.shape[1] - 1, 1)


def westward(value):
    return pltpu.roll(value, 1, 1)


def fold(total):
    width = total.shape[1]
    while width > LANES:
        width //= 2
        total = total[:, :width] + total[:, width:]
    return jnp.sum(total, axis=0, keepdims=True)


def images(field, r, near, far, cross):
    owns, outs = [], []
    for j in range(4):
        east, north = near if j < 2 else far
        e = j % 2
        rows = pl.ds(r, STEP)
        own, edge = field[j, rows, :], east[e, rows, :]
        across = edge * eastward(own) + westward(edge * own)
        along = north[e, rows, :] * above_of(field, j, r)
        owns.append(own)
        outs.append(across + (along + below_of(north, e, r) * below_of(field, j, r)))
    link = cross[pl.ds(r, STEP), :]
    outs[0] = outs[0] + link * owns[2]
    outs[2] = outs[2] + link * owns[0]
    return owns, outs


def solved(inverse, r, outs):
    news = []
    for q in range(2):
        ii, oo, io = [inverse[3 * q + e, pl.ds(r, STEP), :] for e in range(3)]
        one, two = outs[2 * q], outs[2 * q + 1]
        news += [ii * one + io * two, io * one + oo * two]
    return news


def dot(left, right, n_cols):
    pairs = [a * b for a, b in zip(left, right)]
    return ((pairs[0] + pairs[1]) + (pairs[2] + pairs[3]))[:, :n_cols]


def edge_kernel(gz, near, near_e, near_n, near_sum, big_plane, big_via, small, far_e, far_n, cross, inverse, step_1, n_own, inv_own, send, part, *scratch):
    fields, step_0, flat, tall = scratch
    group = gz[0]
    half, n_cols = big_via.shape[1:]
    n_rows = half + 2 * STEP
    n_blocks = n_rows // STEP
    tall_rows = tall.shape[0]
    flat[...] = jnp.zeros(flat.shape, jnp.float32)
    for f in range(N_FAR):
        at, row = 2 * DEEP * f, 2 * DEEP * N_FAR + DEEP * f
        flat[at : at + DEEP, :] = small[row : row + DEEP, :tall_rows]
        flat[at + DEEP : at + 2 * DEEP, :] = small[row : row + DEEP, tall_rows:]
    tall[...] = flat[...].T
    for k in range(n_blocks):
        rows = pl.ds(k * STEP, STEP)
        strip = tall[block(k + group * (half // STEP)), :]
        for f in range(N_FAR):
            if 0 < k < n_blocks - 1:
                core = (big_plane if f < 2 else big_via)[f % 2, (k - 1) * STEP : k * STEP, :]
            else:
                core = pltpu.roll(small[2 * DEEP * f : 2 * DEEP * f + STEP, :], DEEP, 0)
            fields[f, rows, :n_cols] = core
            fields[f, rows, n_cols:] = side(strip, f, 1.0)
    total = jnp.zeros((STEP, n_cols), jnp.float32)
    for k in range(n_blocks):
        r = k * STEP
        rows = pl.ds(r, STEP)
        sums = [near_sum[0, rows, :], near_sum[1, rows, :]]
        for layer in range(2):
            value = fields[layer, rows, :]
            to_east = harmonic(value, eastward(value))
            to_north = harmonic(value, above_of(fields, layer, r))
            far_e[layer, rows, :] = to_east
            far_n[layer, rows, :] = to_north
            carried = pltpu.roll(to_north, 1, 0)
            if k:
                sub = lax.broadcasted_iota(jnp.int32, value.shape, 0)
                under = pltpu.roll(far_n[layer, r - STEP : r, :], 1, 0)
                carried = jnp.where(sub == 0, under, carried)
            sums.append((to_east + westward(to_east)) + (to_north + carried))
        link = harmonic(near[0, rows, :], fields[2, rows, :])
        cross[rows, :] = link
        drawn, pads = near[2, rows, :], near[3, rows, :]
        inner = pl.ds(r - STEP, STEP)
        for q, up in ((0, near[1, rows, :]), (1, fields[3, rows, :])):
            diag_i = sums[2 * q] + up + link
            diag_o = sums[2 * q + 1] + up + jnp.where(group == 1 - q, pads, 0.0)
            scale = 1.0 / (diag_i * diag_o - up * up)
            found = (diag_o * scale, diag_i * scale, up * scale)
            for e in range(3):
                inverse[3 * q + e, rows, :] = found[e]
                if q == 0 and 0 < k < n_blocks - 1:
                    inv_own[e, inner, :] = found[e][:, :n_cols]
            here = jnp.where(group == q, drawn, 0.0)
            one, two = found[2] * here, found[1] * here
            step_0[2 * q, rows, :], step_0[2 * q + 1, rows, :] = one, two
            if 0 < k < n_blocks - 1:
                total = total + (two * here)[:, :n_cols]
    part[...] = jnp.zeros(part.shape, jnp.float32)
    part[0:1, :] = fold(total)
    sums = [jnp.zeros((STEP, n_cols), jnp.float32)] * 2
    for k in range(n_blocks):
        r = k * STEP
        owns, outs = images(step_0, r, (near_e, near_n), (far_e, far_n), cross)
        news = solved(inverse, r, outs)
        for j in range(4):
            step_1[j, pl.ds(r, STEP), :] = news[j]
        if 0 < k < n_blocks - 1:
            inner = pl.ds(r - STEP, STEP)
            for layer in range(2):
                n_own[layer, inner, :] = outs[layer][:, :n_cols]
                send[layer, inner, :] = outs[2 + layer][:, :n_cols]
            sums[0] = sums[0] + dot(owns, outs, n_cols)
            sums[1] = sums[1] + dot(news, outs, n_cols)
    part[1:2, :] = fold(sums[0])
    part[2:3, :] = fold(sums[1])


def steps_kernel(step_1, near_e, near_n, far_e, far_n, cross, inverse, before, n_own, send, spread, step_2):
    n_rows = step_1.shape[1]
    n_cols = n_own.shape[2]
    n_blocks = n_rows // STEP
    near, far = (near_e, near_n), (far_e, far_n)
    sums = [jnp.zeros((STEP, n_cols), jnp.float32)] * 3

    def keep(first, r, outs):
        inner = pl.ds(r - STEP, STEP)
        for layer in range(2):
            n_own[first + layer, inner, :] = outs[layer][:, :n_cols]
            send[first + layer, inner, :] = outs[2 + layer][:, :n_cols]

    for k in range(n_blocks):
        r = k * STEP
        owns, outs = images(step_1, r, near, far, cross)
        news = solved(inverse, r, outs)
        for j in range(4):
            step_2[j, pl.ds(r, STEP), :] = news[j]
        if 0 < k < n_blocks - 1:
            keep(0, r, outs)
            sums[0] = sums[0] + dot(owns, outs, n_cols)
            sums[1] = sums[1] + dot(news, outs, n_cols)
    for k in range(1, n_blocks - 1):
        r = k * STEP
        owns, outs = images(step_2, r, near, far, cross)
        keep(2, r, outs)
        sums[2] = sums[2] + dot(owns, outs, n_cols)
    row = lax.broadcasted_iota(jnp.int32, before.shape, 0)
    part = before[...]
    for j in range(3):
        part = jnp.where(row == 3 + j, fold(sums[j]), part)
    for k in range(spread.shape[0]):
        spread[k] = part


def inverse_kernel(gz, plane, via, sums, given, inverse):
    group = gz[0]
    half = inverse.shape[1]

    def fill(k, carry):
        rows, at = block(k), block(k + (1 - group) * (half // STEP))
        up = via[1, at, :]
        diag_i = sums[0, rows, :] + up + harmonic(via[0, at, :], given[rows, :])
        diag_o = sums[1, rows, :] + up + jnp.where(group == 1, plane[2, at, :], 0.0)
        scale = 1.0 / (diag_i * diag_o - up * up)
        inverse[0, rows, :] = diag_o * scale
        inverse[1, rows, :] = diag_i * scale
        inverse[2, rows, :] = up * scale
        return carry

    lax.fori_loop(0, half // STEP, fill, 0, unroll=2)


def tree(parts):
    values = [parts[k] for k in range(parts.shape[0])]
    while len(values) > 1:
        values = [a + b for a, b in zip(values[::2], values[1::2])]
    return values[0]


def relay_kernel(parts, spread):
    total = tree(parts)
    for k in range(spread.shape[0]):
        spread[k] = total


def solve_kernel(parts, coefs, flag):
    sums = jnp.sum(tree(parts), axis=1, keepdims=True)
    g = [jnp.broadcast_to(sums[k : k + 1, :], (1, LANES)) for k in range(6)]
    step = [g[k] - g[k + 1] for k in range(5)]
    scale = [lax.rsqrt(g[0]), lax.rsqrt(g[2]), lax.rsqrt(g[4])]

    def entry(i, j):
        return step[i + j] * scale[i] * scale[j]

    d0 = entry(0, 0)
    l10, l20 = entry(1, 0) / d0, entry(2, 0) / d0
    d1 = entry(1, 1) - l10 * entry(1, 0)
    e21 = entry(2, 1) - l20 * entry(1, 0)
    l21 = e21 / d1
    d2 = entry(2, 2) - l20 * entry(2, 0) - l21 * e21
    y0 = g[0] * scale[0]
    y1 = g[1] * scale[1] - l10 * y0
    y2 = g[2] * scale[2] - l20 * y0 - l21 * y1
    x2 = y2 / d2
    x1 = y1 / d1 - l21 * x2
    x0 = y0 / d0 - l10 * x1 - l20 * x2
    c0, c1, c2 = x0 * scale[0], x1 * scale[1], x2 * scale[2]
    for k, value in enumerate((c0, c1, c2, 1.0 - c0, c0 - c1, c1 - c2)):
        coefs[k : k + 1, :] = value
    coefs[6:8, :] = jnp.zeros((2, LANES), jnp.float32)
    good = (d0 > GUARD) & (d1 > GUARD) & (d2 > GUARD)
    flag[...] = jnp.where(good, 1, 0)


def combine_kernel(gz, coefs, current, inv_near, inv_far, n_0, n_0_far, n_12, n_12_far, volts, left):
    group = gz[0]
    half, n_cols = n_0.shape[1:]
    c = [jnp.broadcast_to(coefs[k : k + 1, 0:1], (STEP, n_cols)) for k in range(6)]

    def fill(near, inv, first, second):
        start = (group if near else 1 - group) * (half // STEP)

        def body(k, carry):
            rows, at = block(k), block(k + start)
            drawn = jnp.where(group == 0, current[at, :], 0.0)
            n0i, n0o = first[0, rows, :], first[1, rows, :]
            n1i, n1o, n2i, n2o = [second[j, rows, :] for j in range(4)]
            ii, oo, io = [inv[e, rows, :] for e in range(3)]
            one = c[1] * n0i + c[2] * n1i
            two = c[0] * drawn + (c[1] * n0o + c[2] * n1o)
            volts[1 - group, at, :] = ii * one + io * two
            volts[group, at, :] = io * one + oo * two
            left[1 - group, at, :] = c[4] * n0i + c[5] * n1i + c[2] * n2i
            left[group, at, :] = c[3] * drawn + c[4] * n0o + c[5] * n1o + c[2] * n2o
            return carry

        lax.fori_loop(0, half // STEP, body, 0, unroll=2)

    fill(True, inv_near, n_0, n_12)
    fill(False, inv_far, n_0_far, n_12_far)


def call(kernel, outs, scratch, n_smem, *args):
    return pallas(kernel, outs, scratch, n_smem, args)


def pallas(kernel, outs, scratch, n_smem, args):
    return pl.pallas_call(
        kernel,
        in_specs=[SMEM] * n_smem + [VMEM] * (len(args) - n_smem),
        out_specs=[VMEM] * len(outs),
        out_shape=outs,
        scratch_shapes=scratch,
        compiler_params=pltpu.CompilerParams(vmem_limit_bytes=GRANT),
    )(*args)


def shards(load_current, sink_mask, pad_mask, plane_class, via_class, plane_table, via_table):
    _, n_rows, n_cols = plane_class.shape
    half, frame = n_rows // 2, n_rows // 2 + 2 * STEP
    tall = -(-(n_rows + 2 * STEP) // LANES) * LANES
    broad = n_cols + LANES

    def array(*shape):
        return jax.ShapeDtypeStruct(shape, jnp.float32)

    def ring(axis):
        size = lax.axis_size(axis)
        return [(i, (i + 1) % size) for i in range(size)]

    def back(pairs):
        return [(b, a) for a, b in pairs]

    turn = [pltpu.VMEM((LANES, tall), jnp.float32), pltpu.VMEM((tall, LANES), jnp.float32)]
    gz = lax.axis_index("gz").reshape(1).astype(jnp.int32)
    swap = [(0, 1), (1, 0)]
    rest = ("gy_0", "gy_1", "gz")
    n_gx, n_rest = lax.axis_size(GX), lax.axis_size(rest)

    via, pair, via_send = call(
        via_kernel,
        [array(2, n_rows, n_cols), array(2, half, n_cols), array(half, n_cols)],
        [], 2, gz, via_table, via_class,
    )
    big_via = lax.ppermute(pair, "gz", swap)
    plane, drawn, pair, top, bottom = call(
        plane_kernel,
        [array(3, n_rows, n_cols), array(n_rows, n_cols), array(2, half, n_cols)]
        + [array(DEEP * N_OWN, n_cols)] * 2,
        [], 2, gz, plane_table, plane_class, load_current, sink_mask, pad_mask, via,
    )
    south = lax.ppermute(bottom, GY, ring(GY))
    north = lax.ppermute(top, GY, back(ring(GY)))
    big_plane = lax.ppermute(pair, "gz", swap)
    first, last = call(
        columns_kernel, [array(DEEP * N_OWN, tall)] * 2, turn[1:], 0,
        plane, via, drawn, south, north,
    )
    west = lax.ppermute(last, GX, ring(GX))
    east = lax.ppermute(first, GX, back(ring(GX)))
    (small_send,) = call(
        corner_kernel, [array(N_FAR * 3 * DEEP, n_cols)], [], 1,
        gz, plane, via, south, north, west, east,
    )
    small = lax.ppermute(small_send, "gz", swap)
    via_far = lax.ppermute(via_send, "gz", swap)
    near, near_e, near_n, near_sum, far_sum = call(
        own_kernel,
        [array(4, frame, broad)] + [array(2, frame, broad)] * 3 + [array(2, half, n_cols)],
        [pltpu.VMEM((N_OWN, n_rows + 2 * STEP, broad), jnp.float32)] + turn,
        1, gz, plane, via, drawn, south, north, west, east,
    )
    far_e, far_n, cross, inverse, step_1, n_0, inv_near, send, part = call(
        edge_kernel,
        [array(2, frame, broad)] * 2
        + [array(frame, broad), array(6, frame, broad), array(4, frame, broad),
           array(2, half, n_cols), array(3, half, n_cols), array(2, half, n_cols), array(STEP, LANES)],
        [pltpu.VMEM((N_FAR, frame, broad), jnp.float32), pltpu.VMEM((4, frame, broad), jnp.float32)]
        + turn,
        1, gz, near, near_e, near_n, near_sum, big_plane, big_via, small,
    )
    n_0_far = lax.ppermute(send, "gz", swap)
    (inv_far,) = call(
        inverse_kernel, [array(3, half, n_cols)], [], 1,
        gz, plane, via, far_sum, via_far,
    )
    n_12, send, spread = call(
        steps_kernel,
        [array(4, half, n_cols), array(4, half, n_cols), array(n_gx, STEP, LANES)],
        [pltpu.VMEM((4, frame, broad), jnp.float32)],
        0, step_1, near_e, near_n, far_e, far_n, cross, inverse, part,
    )
    n_12_far = lax.ppermute(send, "gz", swap)
    parts = lax.all_to_all(spread, GX, 0, 0, tiled=True)
    (spread,) = call(relay_kernel, [array(n_rest, STEP, LANES)], [], 0, parts)
    parts = lax.all_to_all(spread, rest, 0, 0, tiled=True)
    coefs, flag = call(
        solve_kernel,
        [array(STEP, LANES), jax.ShapeDtypeStruct((1, LANES), jnp.int32)], [], 0, parts,
    )
    quick = call(
        combine_kernel, [array(2, n_rows, n_cols)] * 2, [], 1,
        gz, coefs, drawn, inv_near, inv_far, n_0, n_0_far, n_12, n_12_far,
    )

    def careful():
        return recurrence(
            load_current, sink_mask, pad_mask, plane_class, via_class, plane_table, via_table
        )

    return lax.cond(flag[0, 0] == 1, lambda: tuple(quick), careful)


def solution(mesh):
    split = Mesh(
        mesh.devices.reshape(8, 2, 2, 4, mesh.shape["gz"]), ("gx_0", "gx_1", "gy_0", "gy_1", "gz")
    )
    placed = (
        P(GY, GX),
        P(GY, GX),
        P(GY, GX),
        P("gz", GY, GX),
        P("gz", GY, GX),
        P("gz", None),
        P("gz", None),
    )
    return jax.shard_map(
        shards,
        mesh=split,
        in_specs=placed,
        out_specs=(P("gz", GY, GX), P("gz", GY, GX)),
        check_vma=False,
    )
```

```python
import jax
import jax.numpy as jnp
from jax import lax
from jax.experimental import pallas as pl
from jax.experimental.pallas import tpu as pltpu
from jax.sharding import Mesh
from jax.sharding import PartitionSpec as P

ITERS = 3
GX = ("gx_0", "gx_1")
GY = ("gy_0", "gy_1")
GX_GY_GZ = ("gx_0", "gx_1", "gy_0", "gy_1", "gz")


PAD_CONDUCTANCE = 20.0


def padded(array, sides, width):
    edges = {}
    for axis, dim in sides:
        peers, length = (lax.axis_size(axis), array.shape[dim])
        up = [(i, (i + 1) % peers) for i in range(peers)]
        last = lax.slice_in_dim(array, length - width, length, axis=dim)
        leading = lax.slice_in_dim(array, 0, width, axis=dim)
        edges[dim] = (
            lax.ppermute(last, axis, up),
            lax.ppermute(leading, axis, [(b, a) for a, b in up]),
        )
    done = []
    for _, dim in sides:
        low, high = edges[dim]
        around = [(width, width) if d in done else (0, 0) for d in range(array.ndim)]
        array = jnp.concatenate([jnp.pad(low, around), array, jnp.pad(high, around)], axis=dim)
        done.append(dim)
    return array


def padded_2(block, sides, width):
    for axis, dim in sides:
        count = lax.axis_size(axis)
        forward = [(i, i + 1) for i in range(count - 1)]
        backward = [(target, source) for source, target in forward]
        low = lax.ppermute(
            lax.slice_in_dim(block, block.shape[dim] - width, None, axis=dim), axis, forward
        )
        high = lax.ppermute(lax.slice_in_dim(block, 0, width, axis=dim), axis, backward)
        block = jnp.concatenate([low, block, high], axis=dim)
    return block


def by_axis(array, axes):
    for axis in axes:
        array = lax.psum(array, axis)
    return array


def lookup(classes, table):
    summed = jnp.zeros(classes.shape, jnp.float32)
    for level in range(table.shape[1]):
        summed = summed + jnp.where(
            classes == level, table[:, level][:, None, None], jnp.float32(0.0)
        )
    return summed


def harmonic(first, second):
    return 2.0 * first * second / (first + second)


def factor(diagonal, up_edge):
    inverses = []
    factors = []
    for level in range(diagonal.shape[0]):
        pivots = diagonal[level]
        if level > 0:
            pivots = pivots + up_edge[level - 1] * factors[level - 1]
        inverse = 1.0 / pivots
        inverses.append(inverse)
        factors.append(-up_edge[level] * inverse)
    return (jnp.stack(inverses), jnp.stack(factors))


def solve_block(inverses, factors, up_edge, source_term):
    forward = []
    for level in range(source_term.shape[0]):
        entries = source_term[level]
        if level > 0:
            entries = entries + up_edge[level - 1] * forward[level - 1]
        forward.append(entries * inverses[level])
    result = [forward[-1]]
    level = 0
    result.insert(0, forward[level] - factors[level] * result[0])
    return jnp.stack(result)


def plane_extend(field):
    return padded(field, ((GX, 2), (GY, 1)), 1)


def layer_extend(field):
    return padded_2(field, (("gz", 0),), 1)


def merged_sums(residual, precond, image_field):
    return (
        by_axis(jnp.sum(residual * precond), GX_GY_GZ),
        by_axis(jnp.sum(image_field * precond), GX_GY_GZ),
    )


def recurrence(load_current, sink_mask, pad_mask, plane_class, via_class, plane_table, via_table):
    n_layers, n_rows, n_cols = plane_class.shape
    g_plane = lookup(plane_class, plane_table)
    g_via = lookup(via_class, via_table)
    plane_ext = plane_extend(g_plane)
    middle = plane_ext[:, 1:-1, :]
    across = harmonic(middle[:, :, :-1], middle[:, :, 1:])
    east_edge = across[:, :, 1:]
    west_edge = across[:, :, :-1]
    column = plane_ext[:, :, 1:-1]
    along_rows = harmonic(column[:, :-1], column[:, 1:])
    north_edge = along_rows[:, 1:]
    south_edge = along_rows[:, :-1]
    via_ext = layer_extend(g_via)
    vertical = harmonic(via_ext[:-1], via_ext[1:])
    up_edge = vertical[1:]
    down_edge = vertical[:-1]
    group_index = lax.axis_index("gz")
    is_top = group_index == lax.axis_size("gz") - 1
    is_bottom = group_index == 0
    pad_plane = jnp.where(is_top, PAD_CONDUCTANCE * pad_mask.astype(jnp.float32), jnp.float32(0.0))
    pad_layer = jnp.concatenate(
        [jnp.zeros((n_layers - 1, n_rows, n_cols), jnp.float32), pad_plane[None]], 0
    )
    diagonal = east_edge + west_edge + north_edge + south_edge + up_edge + down_edge + pad_layer
    inverses, factors = factor(diagonal, up_edge)

    def precondition(residual):
        return solve_block(inverses, factors, up_edge, residual)

    def operate(field):
        inner = plane_extend(field)
        layer_ext = layer_extend(field)
        above_field = layer_ext[2:]
        below_field = layer_ext[:-2]
        return (
            diagonal * field
            - east_edge * inner[:, 1:-1, 2:]
            - west_edge * inner[:, 1:-1, :-2]
            - north_edge * inner[:, 2:, 1:-1]
            - south_edge * inner[:, :-2, 1:-1]
            - up_edge * above_field
            - down_edge * below_field
        )

    source = jnp.where(is_bottom, sink_mask.astype(jnp.float32) * load_current, jnp.float32(0.0))
    right_side = jnp.concatenate(
        [source[None], jnp.zeros((n_layers - 1, n_rows, n_cols), jnp.float32)], 0
    )
    voltage = jnp.zeros((n_layers, n_rows, n_cols), jnp.float32)
    residual = right_side
    precond = precondition(residual)
    image_field = operate(precond)
    weight_now, curvature = merged_sums(residual, precond, image_field)
    step_size = weight_now / curvature
    direction = precond
    image_dir = image_field
    for iteration in range(ITERS):
        voltage = voltage + step_size * direction
        residual = residual - step_size * image_dir
        if iteration + 1 < ITERS:
            precond = precondition(residual)
            image_field = operate(precond)
            weight_next, curvature = merged_sums(residual, precond, image_field)
            momentum = weight_next / weight_now
            step_size = weight_next / (curvature - momentum * weight_next / step_size)
            direction = precond + momentum * direction
            image_dir = image_field + momentum * image_dir
            weight_now = weight_next
    return (voltage, residual)


STEP = 8
LANES = 128
DEEP = 4
GUARD = 0.02
GRANT = 16 * 1024 * 1024
N_OWN = 6
N_FAR = 4
VMEM = pl.BlockSpec(memory_space=pltpu.VMEM)
SMEM = pl.BlockSpec(memory_space=pltpu.SMEM)
OUTSIDE = pl.BlockSpec(memory_space=pl.ANY)


def block(k):
    return pl.ds(pl.multiple_of(k * STEP, STEP), STEP)


def mean(first, second):
    return 1.0 / (first + second)


def half_reciprocals(table, layer, n_cols):
    row = 0.5 / table[pl.ds(layer, 1), :]
    return [jnp.broadcast_to(row[:, e : e + 1], (STEP, n_cols)) for e in range(row.shape[1])]


def look_up(entries, classes):
    low = (classes & 1) != 0
    mid = (classes & 2) != 0
    pairs = [jnp.where(low, entries[2 * k + 1], entries[2 * k]) for k in range(4)]
    return jnp.where(
        classes > 3, jnp.where(mid, pairs[3], pairs[2]), jnp.where(mid, pairs[1], pairs[0])
    )


def via_kernel(gz, table, classes, via, pair, lone):
    group = gz[0]
    n_rows, n_cols = via.shape[1:]
    half = n_rows // 2 // STEP
    of_i, of_o = [half_reciprocals(table, layer, n_cols) for layer in (1 - group, group)]

    def fill(k, carry):
        rows = block(k)
        one = look_up(of_i, classes[1 - group, rows, :])
        two = look_up(of_o, classes[group, rows, :])
        via[0, rows, :] = one
        via[1, rows, :] = mean(one, two)
        return carry

    lax.fori_loop(0, n_rows // STEP, fill, 0, unroll=4)

    def copy(k, carry):
        for f in range(2):
            pair[f, block(k), :] = via[f, block(k + (1 - group) * half), :]
        lone[block(k), :] = via[0, block(k + group * half), :]
        return carry

    lax.fori_loop(0, half, copy, 0, unroll=4)


def plane_kernel(gz, table, classes, load, sink, pad, via, plane, drawn, pair, top, bottom):
    group = gz[0]
    n_rows, n_cols = plane.shape[1:]
    half = n_rows // 2 // STEP
    of_i, of_o = [half_reciprocals(table, layer, n_cols) for layer in (1 - group, group)]

    def fill(k, carry):
        rows = block(k)
        plane[0, rows, :] = look_up(of_i, classes[1 - group, rows, :])
        plane[1, rows, :] = look_up(of_o, classes[group, rows, :])
        plane[2, rows, :] = PAD_CONDUCTANCE * pad[rows, :].astype(jnp.float32)
        drawn[rows, :] = sink[rows, :].astype(jnp.float32) * load[rows, :]
        return carry

    lax.fori_loop(0, n_rows // STEP, fill, 0, unroll=4)

    def copy(k, carry):
        for f in range(2):
            pair[f, block(k), :] = plane[f, block(k + (1 - group) * half), :]
        return carry

    lax.fori_loop(0, half, copy, 0, unroll=4)
    for f in range(N_OWN):
        at = pl.ds(DEEP * f, DEEP)
        top[at, :] = field_rows(plane, via, drawn, f, pl.ds(0, DEEP))
        bottom[at, :] = field_rows(plane, via, drawn, f, pl.ds(n_rows - DEEP, DEEP))


def field_rows(plane, via, drawn, f, rows):
    if f == 4:
        return drawn[rows, :]
    if f in (2, 3):
        return via[f - 2, rows, :]
    return plane[2 if f == 5 else f, rows, :]


def tile_of(stack, f, upper):
    rows = stack[f // 2 * STEP : f // 2 * STEP + STEP, :]
    return rows if (f % 2 == 1) == upper else pltpu.roll(rows, DEEP, 0)


def columns_kernel(plane, via, drawn, south, north, first, last, stage):
    n_rows, n_cols = drawn.shape
    lane = lax.broadcasted_iota(jnp.int32, (STEP, LANES), 1)
    place = lane // DEEP

    def put(rows, pick):
        out = jnp.zeros((STEP, LANES), jnp.float32)
        for f in range(N_OWN):
            value = pick(f)
            head, tail = value[:, :LANES], value[:, n_cols - LANES :]
            if f:
                head = pltpu.roll(head, DEEP * f, 1)
            tail = pltpu.roll(tail, DEEP * (N_OWN + f + 1), 1)
            out = jnp.where(place == f, head, jnp.where(place == N_OWN + f, tail, out))
        stage[rows, :] = out

    def inner(k, carry):
        put(block(k + 1), lambda f: field_rows(plane, via, drawn, f, block(k)))
        return carry

    put(pl.ds(0, STEP), lambda f: tile_of(south, f, True))
    lax.fori_loop(0, n_rows // STEP, inner, 0, unroll=2)
    put(pl.ds(n_rows + STEP, STEP), lambda f: tile_of(north, f, False))
    rest = n_rows + 2 * STEP
    stage[rest:, :] = jnp.zeros((stage.shape[0] - rest, LANES), jnp.float32)
    turned = stage[...].T
    size = DEEP * N_OWN
    first[...] = turned[:size, :]
    last[...] = turned[size : 2 * size, :]


def side(strip, slot, blank):
    lane = lax.broadcasted_iota(jnp.int32, strip.shape, 1)
    turned = pltpu.roll(strip, (LANES - DEEP - 2 * DEEP * slot) % LANES, 1)
    return jnp.where((lane < DEEP) | (lane >= LANES - DEEP), turned, blank)


def corner_kernel(gz, plane, via, south, north, west, east, small):
    group = gz[0]
    half, tall_rows = plane.shape[1] // 2, west.shape[1]
    for f in range(N_FAR):
        at, mine = 2 * DEEP * f, pl.ds(DEEP * f, DEEP)
        inner = field_rows(plane, via, None, f, pl.ds(half - DEEP, DEEP))
        small[at : at + DEEP, :] = jnp.where(group == 0, inner, south[mine, :])
        inner = field_rows(plane, via, None, f, pl.ds(half, DEEP))
        small[at + DEEP : at + 2 * DEEP, :] = jnp.where(group == 0, north[mine, :], inner)
    at, size = 2 * DEEP * N_FAR, DEEP * N_FAR
    small[at : at + size, :tall_rows] = west[:size, :]
    small[at : at + size, tall_rows:] = east[:size, :]


def eastward(value):
    return pltpu.roll(value, value.shape[1] - 1, 1)


def westward(value):
    return pltpu.roll(value, 1, 1)


def rows_up(value):
    return pltpu.roll(value, STEP - 1, 0)


def rows_down(value):
    return pltpu.roll(value, 1, 0)


def joined(edge, inner, outer):
    sub = lax.broadcasted_iota(jnp.int32, inner.shape, 0)
    return jnp.where(sub == edge, outer, inner)


def own_kernel(gz, plane, via, drawn, south, north, west, east, near, edge_e, edge_n, near_sum, far_sum, wide, flat, tall):
    group = gz[0]
    n_rows, n_cols = drawn.shape
    half, last = n_rows // 2 // STEP, n_rows // STEP + 1
    flat[...] = jnp.zeros(flat.shape, jnp.float32)
    for f in range(N_OWN):
        at = 2 * DEEP * f
        flat[at : at + DEEP, :] = west[DEEP * f : DEEP * f + DEEP, :]
        flat[at + DEEP : at + 2 * DEEP, :] = east[DEEP * f : DEEP * f + DEEP, :]
    tall[...] = flat[...].T

    def put(rows, pick):
        strip = tall[rows, :]
        for f in range(2):
            wide[f, rows, :n_cols] = pick(f)
            wide[f, rows, n_cols:] = side(strip, f, 1.0)

    def inner(k, carry):
        put(block(k + 1), lambda f: plane[f, block(k), :])
        return carry

    put(pl.ds(0, STEP), lambda f: tile_of(south, f, True))
    lax.fori_loop(0, n_rows // STEP, inner, 0, unroll=4)
    put(pl.ds(n_rows + STEP, STEP), lambda f: tile_of(north, f, False))

    def around(layer, k):
        value = wide[layer, block(k), :]
        over = wide[layer, block(jnp.minimum(k + 1, last)), :]
        under = wide[layer, block(jnp.maximum(k - 1, 0)), :]
        above = joined(STEP - 1, rows_up(value), rows_up(over))
        below = joined(0, rows_down(value), rows_down(under))
        to_east, to_north = mean(value, eastward(value)), mean(value, above)
        return to_east, to_north, (to_east + westward(to_east)) + (to_north + mean(value, below))

    def frame(k, carry):
        at = k + group * half
        for layer in range(2):
            to_east, to_north, total = around(layer, at)
            edge_e[layer, block(k), :] = to_east
            edge_n[layer, block(k), :] = to_north
            near_sum[layer, block(k), :] = total
        strip = tall[block(at), :]
        inside = block(jnp.clip(at - 1, 0, last - 2))
        for place, f in enumerate((2, 3, 4, 5)):
            core = field_rows(plane, via, drawn, f, inside)
            core = jnp.where(at == 0, tile_of(south, f, True), core)
            core = jnp.where(at == last, tile_of(north, f, False), core)
            near[place, block(k), :n_cols] = core
            near[place, block(k), n_cols:] = side(strip, f, 1.0 if f < N_FAR else 0.0)
        return carry

    lax.fori_loop(0, half + 2, frame, 0, unroll=2)

    def other(k, carry):
        for layer in range(2):
            total = around(layer, k + 1 + (1 - group) * half)[2]
            far_sum[layer, block(k), :] = total[:, :n_cols]
        return carry

    lax.fori_loop(0, half, other, 0, unroll=2)


def fold(total):
    width = total.shape[1]
    while width > LANES:
        width //= 2
        total = total[:, :width] + total[:, width:]
    return jnp.sum(total, axis=0, keepdims=True)


def image_pass(field, edges, cross, blocks, done):
    last = field.shape[1] // STEP - 1

    def at(k):
        return pl.ds(k * STEP, STEP)

    for q in range(2):
        east, north = edges[q]
        ups, downs = {}, {}

        def up(layer, k):
            if (layer, k) not in ups:
                ups[layer, k] = rows_up(field[2 * q + layer, at(k), :])
            return ups[layer, k]

        def down(layer, k):
            if (layer, k) not in downs:
                flux = north[layer, at(k), :] * field[2 * q + layer, at(k), :]
                downs[layer, k] = rows_down(flux)
            return downs[layer, k]

        for k in blocks:
            owns, outs = [], []
            for layer in range(2):
                own, edge = field[2 * q + layer, at(k), :], east[layer, at(k), :]
                above = joined(STEP - 1, up(layer, k), up(layer, min(k + 1, last)))
                below = joined(0, down(layer, k), down(layer, max(k - 1, 0)))
                across = edge * eastward(own) + westward(edge * own)
                owns.append(own)
                outs.append(across + (north[layer, at(k), :] * above + below))
            outs[0] = outs[0] + cross[at(k), :] * field[2 - 2 * q, at(k), :]
            done(q, k, owns, outs)


def solved(inverse, q, k, outs):
    ii, oo, io = [inverse[3 * q + e, pl.ds(k * STEP, STEP), :] for e in range(3)]
    return [ii * outs[0] + io * outs[1], io * outs[0] + oo * outs[1]]


def dot(left, right, n_cols):
    return (left[0] * right[0] + left[1] * right[1])[:, :n_cols]


def image_step(field, edges, cross, inverse, stepped, keep, n_cols):
    n_blocks = field.shape[1] // STEP
    sums = [jnp.zeros((STEP, n_cols), jnp.float32)] * 2

    def done(q, k, owns, outs):
        news = solved(inverse, q, k, outs)
        for layer in range(2):
            stepped[2 * q + layer, pl.ds(k * STEP, STEP), :] = news[layer]
        if 0 < k < n_blocks - 1:
            for layer in range(2):
                keep[q][layer, pl.ds((k - 1) * STEP, STEP), :] = outs[layer][:, :n_cols]
            sums[0] = sums[0] + dot(owns, outs, n_cols)
            sums[1] = sums[1] + dot(news, outs, n_cols)

    image_pass(field, edges, cross, range(n_blocks), done)
    return sums


def edge_kernel(gz, near, near_e, near_n, near_sum, big_plane, big_via, small, far_e, far_n, cross, inverse, step_1, n_own, inv_own, send, part, *scratch):
    fields, step_0, flat, tall = scratch
    group = gz[0]
    half, n_cols = big_via.shape[1:]
    n_blocks = half // STEP + 2
    tall_rows = tall.shape[0]
    flat[...] = jnp.zeros(flat.shape, jnp.float32)
    for f in range(N_FAR):
        at, row = 2 * DEEP * f, 2 * DEEP * N_FAR + DEEP * f
        flat[at : at + DEEP, :] = small[row : row + DEEP, :tall_rows]
        flat[at + DEEP : at + 2 * DEEP, :] = small[row : row + DEEP, tall_rows:]
    tall[...] = flat[...].T
    for k in range(n_blocks):
        rows = pl.ds(k * STEP, STEP)
        strip = tall[block(k + group * (half // STEP)), :]
        for f in range(N_FAR):
            if 0 < k < n_blocks - 1:
                core = (big_plane if f < 2 else big_via)[f % 2, (k - 1) * STEP : k * STEP, :]
            else:
                core = pltpu.roll(small[2 * DEEP * f : 2 * DEEP * f + STEP, :], DEEP, 0)
            fields[f, rows, :n_cols] = core
            fields[f, rows, n_cols:] = side(strip, f, 1.0)
    total = jnp.zeros((STEP, n_cols), jnp.float32)
    ups, downs = {}, {}

    def up(layer, k):
        if (layer, k) not in ups:
            ups[layer, k] = rows_up(fields[layer, k * STEP : k * STEP + STEP, :])
        return ups[layer, k]

    for k in range(n_blocks):
        rows = pl.ds(k * STEP, STEP)
        sums = [near_sum[0, rows, :], near_sum[1, rows, :]]
        for layer in range(2):
            value = fields[layer, rows, :]
            above = joined(STEP - 1, up(layer, k), up(layer, min(k + 1, n_blocks - 1)))
            to_east, to_north = mean(value, eastward(value)), mean(value, above)
            far_e[layer, rows, :] = to_east
            far_n[layer, rows, :] = to_north
            downs[layer, k] = rows_down(to_north)
            carried = joined(0, downs[layer, k], downs[layer, max(k - 1, 0)])
            sums.append((to_east + westward(to_east)) + (to_north + carried))
        link = mean(near[0, rows, :], fields[2, rows, :])
        cross[rows, :] = link
        drawn, pads = near[2, rows, :], near[3, rows, :]
        inner = pl.ds((k - 1) * STEP, STEP)
        for q, up_edge in ((0, near[1, rows, :]), (1, fields[3, rows, :])):
            diag_i = sums[2 * q] + up_edge + link
            diag_o = sums[2 * q + 1] + up_edge + jnp.where(group == 1 - q, pads, 0.0)
            scale = 1.0 / (diag_i * diag_o - up_edge * up_edge)
            found = (diag_o * scale, diag_i * scale, up_edge * scale)
            for e in range(3):
                inverse[3 * q + e, rows, :] = found[e]
                if q == 0 and 0 < k < n_blocks - 1:
                    inv_own[e, inner, :] = found[e][:, :n_cols]
            here = jnp.where(group == q, drawn, 0.0)
            one, two = found[2] * here, found[1] * here
            step_0[2 * q, rows, :], step_0[2 * q + 1, rows, :] = one, two
            if 0 < k < n_blocks - 1:
                total = total + (two * here)[:, :n_cols]
    part[...] = jnp.zeros(part.shape, jnp.float32)
    part[0:1, :] = fold(total)
    sums = image_step(
        step_0, ((near_e, near_n), (far_e, far_n)), cross, inverse, step_1, (n_own, send), n_cols
    )
    part[1:2, :] = fold(sums[0])
    part[2:3, :] = fold(sums[1])


def steps_kernel(step_1, near_e, near_n, far_e, far_n, cross, inverse, before, n_own, send, spread, step_2):
    n_cols = n_own.shape[2]
    edges = ((near_e, near_n), (far_e, far_n))
    first, second = pl.ds(0, 2), pl.ds(2, 2)
    sums = image_step(
        step_1, edges, cross, inverse, step_2, (n_own.at[first], send.at[first]), n_cols
    )
    keep = (n_own.at[second], send.at[second])
    sums.append(jnp.zeros((STEP, n_cols), jnp.float32))

    def done(q, k, owns, outs):
        for layer in range(2):
            keep[q][layer, pl.ds((k - 1) * STEP, STEP), :] = outs[layer][:, :n_cols]
        sums[2] = sums[2] + dot(owns, outs, n_cols)

    image_pass(step_2, edges, cross, range(1, step_1.shape[1] // STEP - 1), done)
    row = lax.broadcasted_iota(jnp.int32, before.shape, 0)
    part = before[...]
    for j in range(3):
        part = jnp.where(row == 3 + j, fold(sums[j]), part)
    for k in range(spread.shape[0]):
        spread[k] = part


def inverse_kernel(gz, plane, via, sums, given, inverse):
    group = gz[0]
    half = inverse.shape[1]

    def fill(k, carry):
        rows, at = block(k), block(k + (1 - group) * (half // STEP))
        up = via[1, at, :]
        diag_i = sums[0, rows, :] + up + mean(via[0, at, :], given[rows, :])
        diag_o = sums[1, rows, :] + up + jnp.where(group == 1, plane[2, at, :], 0.0)
        scale = 1.0 / (diag_i * diag_o - up * up)
        inverse[0, rows, :] = diag_o * scale
        inverse[1, rows, :] = diag_i * scale
        inverse[2, rows, :] = up * scale
        return carry

    lax.fori_loop(0, half // STEP, fill, 0, unroll=2)


def tree(parts):
    values = [parts[k] for k in range(parts.shape[0])]
    while len(values) > 1:
        values = [a + b for a, b in zip(values[::2], values[1::2])]
    return values[0]


def relay_kernel(parts, spread):
    total = tree(parts)
    for k in range(spread.shape[0]):
        spread[k] = total


def solve(parts):
    sums = jnp.sum(tree(parts), axis=1, keepdims=True)
    g = [jnp.broadcast_to(sums[k : k + 1, :], (1, LANES)) for k in range(6)]
    step = [g[k] - g[k + 1] for k in range(5)]
    scale = [lax.rsqrt(g[0]), lax.rsqrt(g[2]), lax.rsqrt(g[4])]

    def entry(i, j):
        return step[i + j] * scale[i] * scale[j]

    d0 = entry(0, 0)
    l10, l20 = entry(1, 0) / d0, entry(2, 0) / d0
    d1 = entry(1, 1) - l10 * entry(1, 0)
    e21 = entry(2, 1) - l20 * entry(1, 0)
    l21 = e21 / d1
    d2 = entry(2, 2) - l20 * entry(2, 0) - l21 * e21
    y0 = g[0] * scale[0]
    y1 = g[1] * scale[1] - l10 * y0
    y2 = g[2] * scale[2] - l20 * y0 - l21 * y1
    x2 = y2 / d2
    x1 = y1 / d1 - l21 * x2
    x0 = y0 / d0 - l10 * x1 - l20 * x2
    c0, c1, c2 = x0 * scale[0], x1 * scale[1], x2 * scale[2]
    good = (d0 > GUARD) & (d1 > GUARD) & (d2 > GUARD)
    return (c0, c1, c2, 1.0 - c0, c0 - c1, c1 - c2), good


def combine_kernel(gz, parts, current, inv_near, inv_far, n_0, n_0_far, n_12, n_12_far, volts, left, flag, volts_here, left_here, sems):
    group = gz[0]
    half, n_cols = n_0.shape[1:]
    values, good = solve(parts)
    flag[...] = jnp.where(good, 1, 0)
    c = [jnp.broadcast_to(value[:, 0:1], (STEP, n_cols)) for value in values]

    def fill(part, inv, first, second):
        def body(k, carry):
            rows, at = block(k), block(k + part * (half // STEP))
            drawn = jnp.where(group == 0, current[at, :], 0.0)
            n0i, n0o = first[0, rows, :], first[1, rows, :]
            n1i, n1o, n2i, n2o = [second[j, rows, :] for j in range(4)]
            ii, oo, io = [inv[e, rows, :] for e in range(3)]
            one = c[1] * n0i + c[2] * n1i
            two = c[0] * drawn + (c[1] * n0o + c[2] * n1o)
            volts_here[1 - group, at, :] = ii * one + io * two
            volts_here[group, at, :] = io * one + oo * two
            left_here[1 - group, at, :] = c[4] * n0i + c[5] * n1i + c[2] * n2i
            left_here[group, at, :] = c[3] * drawn + c[4] * n0o + c[5] * n1o + c[2] * n2o
            return carry

        lax.fori_loop(0, half // STEP, body, 0, unroll=2)

    copies = []
    for part in range(2):

        @pl.when(group == part)
        def _(part=part):
            fill(part, inv_near, n_0, n_12)

        @pl.when(group != part)
        def _(part=part):
            fill(part, inv_far, n_0_far, n_12_far)

        for j, (source, target) in enumerate(((volts_here, volts), (left_here, left))):
            rows = pl.ds(part * half, half)
            copy = pltpu.make_async_copy(
                source.at[:, rows, :], target.at[:, rows, :], sems.at[2 * part + j]
            )
            copy.start()
            copies.append(copy)
    for copy in copies:
        copy.wait()


def call(kernel, outs, scratch, n_smem, *args, outside=0):
    return pl.pallas_call(
        kernel,
        in_specs=[SMEM] * n_smem + [VMEM] * (len(args) - n_smem),
        out_specs=[OUTSIDE] * outside + [VMEM] * (len(outs) - outside),
        out_shape=outs,
        scratch_shapes=scratch,
        compiler_params=pltpu.CompilerParams(vmem_limit_bytes=GRANT),
    )(*args)


def shards(load_current, sink_mask, pad_mask, plane_class, via_class, plane_table, via_table):
    _, n_rows, n_cols = plane_class.shape
    half, frame = n_rows // 2, n_rows // 2 + 2 * STEP
    tall = -(-(n_rows + 2 * STEP) // LANES) * LANES
    broad = n_cols + LANES

    def array(*shape):
        return jax.ShapeDtypeStruct(shape, jnp.float32)

    def ring(axis):
        size = lax.axis_size(axis)
        return [(i, (i + 1) % size) for i in range(size)]

    def back(pairs):
        return [(b, a) for a, b in pairs]

    turn = [pltpu.VMEM((LANES, tall), jnp.float32), pltpu.VMEM((tall, LANES), jnp.float32)]
    gz = lax.axis_index("gz").reshape(1).astype(jnp.int32)
    swap = [(0, 1), (1, 0)]
    rest = ("gy_0", "gy_1", "gz")
    n_gx, n_rest = lax.axis_size(GX), lax.axis_size(rest)

    via, pair, via_send = call(
        via_kernel,
        [array(2, n_rows, n_cols), array(2, half, n_cols), array(half, n_cols)],
        [], 1, gz, via_table, via_class,
    )
    big_via = lax.ppermute(pair, "gz", swap)
    plane, drawn, pair, top, bottom = call(
        plane_kernel,
        [array(3, n_rows, n_cols), array(n_rows, n_cols), array(2, half, n_cols)]
        + [array(DEEP * N_OWN, n_cols)] * 2,
        [], 1, gz, plane_table, plane_class, load_current, sink_mask, pad_mask, via,
    )
    south = lax.ppermute(bottom, GY, ring(GY))
    north = lax.ppermute(top, GY, back(ring(GY)))
    big_plane = lax.ppermute(pair, "gz", swap)
    first, last = call(
        columns_kernel, [array(DEEP * N_OWN, tall)] * 2, turn[1:], 0,
        plane, via, drawn, south, north,
    )
    west = lax.ppermute(last, GX, ring(GX))
    east = lax.ppermute(first, GX, back(ring(GX)))
    (small_send,) = call(
        corner_kernel, [array(N_FAR * 3 * DEEP, n_cols)], [], 1,
        gz, plane, via, south, north, west, east,
    )
    small = lax.ppermute(small_send, "gz", swap)
    via_far = lax.ppermute(via_send, "gz", swap)
    near, near_e, near_n, near_sum, far_sum = call(
        own_kernel,
        [array(4, frame, broad)] + [array(2, frame, broad)] * 3 + [array(2, half, n_cols)],
        [pltpu.VMEM((N_OWN, n_rows + 2 * STEP, broad), jnp.float32)] + turn,
        1, gz, plane, via, drawn, south, north, west, east,
    )
    far_e, far_n, cross, inverse, step_1, n_0, inv_near, send, part = call(
        edge_kernel,
        [array(2, frame, broad)] * 2
        + [array(frame, broad), array(6, frame, broad), array(4, frame, broad),
           array(2, half, n_cols), array(3, half, n_cols), array(2, half, n_cols), array(STEP, LANES)],
        [pltpu.VMEM((N_FAR, frame, broad), jnp.float32), pltpu.VMEM((4, frame, broad), jnp.float32)]
        + turn,
        1, gz, near, near_e, near_n, near_sum, big_plane, big_via, small,
    )
    n_0_far = lax.ppermute(send, "gz", swap)
    (inv_far,) = call(
        inverse_kernel, [array(3, half, n_cols)], [], 1,
        gz, plane, via, far_sum, via_far,
    )
    n_12, send, spread = call(
        steps_kernel,
        [array(4, half, n_cols), array(4, half, n_cols), array(n_gx, STEP, LANES)],
        [pltpu.VMEM((4, frame, broad), jnp.float32)],
        0, step_1, near_e, near_n, far_e, far_n, cross, inverse, part,
    )
    n_12_far = lax.ppermute(send, "gz", swap)
    parts = lax.all_to_all(spread, GX, 0, 0, tiled=True)
    (spread,) = call(relay_kernel, [array(n_rest, STEP, LANES)], [], 0, parts)
    parts = lax.all_to_all(spread, rest, 0, 0, tiled=True)
    volts, left, flag = call(
        combine_kernel,
        [array(2, n_rows, n_cols)] * 2 + [jax.ShapeDtypeStruct((1, LANES), jnp.int32)],
        [pltpu.VMEM((2, n_rows, n_cols), jnp.float32)] * 2 + [pltpu.SemaphoreType.DMA((4,))],
        1, gz, parts, drawn, inv_near, inv_far, n_0, n_0_far, n_12, n_12_far, outside=2,
    )

    def careful():
        return recurrence(
            load_current, sink_mask, pad_mask, plane_class, via_class, plane_table, via_table
        )

    return lax.cond(flag[0, 0] == 1, lambda: (volts, left), careful)


def solution(mesh):
    split = Mesh(
        mesh.devices.reshape(8, 2, 2, 4, mesh.shape["gz"]), ("gx_0", "gx_1", "gy_0", "gy_1", "gz")
    )
    placed = (
        P(GY, GX),
        P(GY, GX),
        P(GY, GX),
        P("gz", GY, GX),
        P("gz", GY, GX),
        P("gz", None),
        P("gz", None),
    )
    return jax.shard_map(
        shards,
        mesh=split,
        in_specs=placed,
        out_specs=(P("gz", GY, GX), P("gz", GY, GX)),
        check_vma=False,
    )
```

```python
import jax
import jax.numpy as jnp
from jax import lax
from jax.experimental import pallas as pl
from jax.experimental.pallas import tpu as pltpu
from jax.sharding import Mesh
from jax.sharding import PartitionSpec as P

ITERS = 3
GX = ("gx_0", "gx_1")
GY = ("gy_0", "gy_1")
GX_GY_GZ = ("gx_0", "gx_1", "gy_0", "gy_1", "gz")


PAD_CONDUCTANCE = 20.0


def padded(array, sides, width):
    edges = {}
    for axis, dim in sides:
        peers, length = (lax.axis_size(axis), array.shape[dim])
        up = [(i, (i + 1) % peers) for i in range(peers)]
        last = lax.slice_in_dim(array, length - width, length, axis=dim)
        leading = lax.slice_in_dim(array, 0, width, axis=dim)
        edges[dim] = (
            lax.ppermute(last, axis, up),
            lax.ppermute(leading, axis, [(b, a) for a, b in up]),
        )
    done = []
    for _, dim in sides:
        low, high = edges[dim]
        around = [(width, width) if d in done else (0, 0) for d in range(array.ndim)]
        array = jnp.concatenate([jnp.pad(low, around), array, jnp.pad(high, around)], axis=dim)
        done.append(dim)
    return array


def padded_2(block, sides, width):
    for axis, dim in sides:
        count = lax.axis_size(axis)
        forward = [(i, i + 1) for i in range(count - 1)]
        backward = [(target, source) for source, target in forward]
        low = lax.ppermute(
            lax.slice_in_dim(block, block.shape[dim] - width, None, axis=dim), axis, forward
        )
        high = lax.ppermute(lax.slice_in_dim(block, 0, width, axis=dim), axis, backward)
        block = jnp.concatenate([low, block, high], axis=dim)
    return block


def by_axis(array, axes):
    for axis in axes:
        array = lax.psum(array, axis)
    return array


def lookup(classes, table):
    summed = jnp.zeros(classes.shape, jnp.float32)
    for level in range(table.shape[1]):
        summed = summed + jnp.where(
            classes == level, table[:, level][:, None, None], jnp.float32(0.0)
        )
    return summed


def harmonic(first, second):
    return 2.0 * first * second / (first + second)


def factor(diagonal, up_edge):
    inverses = []
    factors = []
    for level in range(diagonal.shape[0]):
        pivots = diagonal[level]
        if level > 0:
            pivots = pivots + up_edge[level - 1] * factors[level - 1]
        inverse = 1.0 / pivots
        inverses.append(inverse)
        factors.append(-up_edge[level] * inverse)
    return (jnp.stack(inverses), jnp.stack(factors))


def solve_block(inverses, factors, up_edge, source_term):
    forward = []
    for level in range(source_term.shape[0]):
        entries = source_term[level]
        if level > 0:
            entries = entries + up_edge[level - 1] * forward[level - 1]
        forward.append(entries * inverses[level])
    result = [forward[-1]]
    level = 0
    result.insert(0, forward[level] - factors[level] * result[0])
    return jnp.stack(result)


def plane_extend(field):
    return padded(field, ((GX, 2), (GY, 1)), 1)


def layer_extend(field):
    return padded_2(field, (("gz", 0),), 1)


def merged_sums(residual, precond, image_field):
    return (
        by_axis(jnp.sum(residual * precond), GX_GY_GZ),
        by_axis(jnp.sum(image_field * precond), GX_GY_GZ),
    )


def recurrence(load_current, sink_mask, pad_mask, plane_class, via_class, plane_table, via_table):
    n_layers, n_rows, n_cols = plane_class.shape
    g_plane = lookup(plane_class, plane_table)
    g_via = lookup(via_class, via_table)
    plane_ext = plane_extend(g_plane)
    middle = plane_ext[:, 1:-1, :]
    across = harmonic(middle[:, :, :-1], middle[:, :, 1:])
    east_edge = across[:, :, 1:]
    west_edge = across[:, :, :-1]
    column = plane_ext[:, :, 1:-1]
    along_rows = harmonic(column[:, :-1], column[:, 1:])
    north_edge = along_rows[:, 1:]
    south_edge = along_rows[:, :-1]
    via_ext = layer_extend(g_via)
    vertical = harmonic(via_ext[:-1], via_ext[1:])
    up_edge = vertical[1:]
    down_edge = vertical[:-1]
    group_index = lax.axis_index("gz")
    is_top = group_index == lax.axis_size("gz") - 1
    is_bottom = group_index == 0
    pad_plane = jnp.where(is_top, PAD_CONDUCTANCE * pad_mask.astype(jnp.float32), jnp.float32(0.0))
    pad_layer = jnp.concatenate(
        [jnp.zeros((n_layers - 1, n_rows, n_cols), jnp.float32), pad_plane[None]], 0
    )
    diagonal = east_edge + west_edge + north_edge + south_edge + up_edge + down_edge + pad_layer
    inverses, factors = factor(diagonal, up_edge)

    def precondition(residual):
        return solve_block(inverses, factors, up_edge, residual)

    def operate(field):
        inner = plane_extend(field)
        layer_ext = layer_extend(field)
        above_field = layer_ext[2:]
        below_field = layer_ext[:-2]
        return (
            diagonal * field
            - east_edge * inner[:, 1:-1, 2:]
            - west_edge * inner[:, 1:-1, :-2]
            - north_edge * inner[:, 2:, 1:-1]
            - south_edge * inner[:, :-2, 1:-1]
            - up_edge * above_field
            - down_edge * below_field
        )

    source = jnp.where(is_bottom, sink_mask.astype(jnp.float32) * load_current, jnp.float32(0.0))
    right_side = jnp.concatenate(
        [source[None], jnp.zeros((n_layers - 1, n_rows, n_cols), jnp.float32)], 0
    )
    voltage = jnp.zeros((n_layers, n_rows, n_cols), jnp.float32)
    residual = right_side
    precond = precondition(residual)
    image_field = operate(precond)
    weight_now, curvature = merged_sums(residual, precond, image_field)
    step_size = weight_now / curvature
    direction = precond
    image_dir = image_field
    for iteration in range(ITERS):
        voltage = voltage + step_size * direction
        residual = residual - step_size * image_dir
        if iteration + 1 < ITERS:
            precond = precondition(residual)
            image_field = operate(precond)
            weight_next, curvature = merged_sums(residual, precond, image_field)
            momentum = weight_next / weight_now
            step_size = weight_next / (curvature - momentum * weight_next / step_size)
            direction = precond + momentum * direction
            image_dir = image_field + momentum * image_dir
            weight_now = weight_next
    return (voltage, residual)


STEP = 8
LANES = 128
DEEP = 4
GUARD = 0.02
GRANT = 16 * 1024 * 1024
N_OWN = 6
N_FAR = 4
VMEM = pl.BlockSpec(memory_space=pltpu.VMEM)
SMEM = pl.BlockSpec(memory_space=pltpu.SMEM)
OUTSIDE = pl.BlockSpec(memory_space=pl.ANY)


def block(k):
    return pl.ds(pl.multiple_of(k * STEP, STEP), STEP)


def mean(first, second):
    return 1.0 / (first + second)


def half_reciprocals(table, layer, n_cols):
    row = 0.5 / table[pl.ds(layer, 1), :]
    return [jnp.broadcast_to(row[:, e : e + 1], (STEP, n_cols)) for e in range(row.shape[1])]


def look_up(entries, classes):
    low = (classes & 1) != 0
    mid = (classes & 2) != 0
    pairs = [jnp.where(low, entries[2 * k + 1], entries[2 * k]) for k in range(4)]
    return jnp.where(
        classes > 3, jnp.where(mid, pairs[3], pairs[2]), jnp.where(mid, pairs[1], pairs[0])
    )


def via_kernel(gz, table, classes, via, first, lone):
    group = gz[0]
    n_rows, n_cols = via.shape[1:]
    half = n_rows // 2 // STEP
    of_i, of_o = [half_reciprocals(table, layer, n_cols) for layer in (1 - group, group)]

    def fill(k, carry):
        rows = block(k)
        one = look_up(of_i, classes[1 - group, rows, :])
        two = look_up(of_o, classes[group, rows, :])
        via[0, rows, :] = one
        via[1, rows, :] = mean(one, two)
        return carry

    lax.fori_loop(0, n_rows // STEP, fill, 0, unroll=4)

    def copy(k, carry):
        first[block(k), :] = via[0, block(k + (1 - group) * half), :]
        lone[block(k), :] = via[0, block(k + group * half), :]
        return carry

    lax.fori_loop(0, half, copy, 0, unroll=4)


def plane_kernel(gz, table, classes, load, sink, pad, via, plane, drawn, three, top, bottom):
    group = gz[0]
    n_rows, n_cols = plane.shape[1:]
    half = n_rows // 2 // STEP
    of_i, of_o = [half_reciprocals(table, layer, n_cols) for layer in (1 - group, group)]

    def fill(k, carry):
        rows = block(k)
        plane[0, rows, :] = look_up(of_i, classes[1 - group, rows, :])
        plane[1, rows, :] = look_up(of_o, classes[group, rows, :])
        plane[2, rows, :] = PAD_CONDUCTANCE * pad[rows, :].astype(jnp.float32)
        drawn[rows, :] = sink[rows, :].astype(jnp.float32) * load[rows, :]
        return carry

    lax.fori_loop(0, n_rows // STEP, fill, 0, unroll=4)

    def copy(k, carry):
        rows = block(k + (1 - group) * half)
        for f in range(2):
            three[f, block(k), :] = plane[f, rows, :]
        three[2, block(k), :] = via[1, rows, :]
        return carry

    lax.fori_loop(0, half, copy, 0, unroll=4)
    for f in range(N_OWN):
        at = pl.ds(DEEP * f, DEEP)
        top[at, :] = field_rows(plane, via, drawn, f, pl.ds(0, DEEP))
        bottom[at, :] = field_rows(plane, via, drawn, f, pl.ds(n_rows - DEEP, DEEP))


def field_rows(plane, via, drawn, f, rows):
    if f == 4:
        return drawn[rows, :]
    if f in (2, 3):
        return via[f - 2, rows, :]
    return plane[2 if f == 5 else f, rows, :]


def tile_of(stack, f, upper):
    rows = stack[f // 2 * STEP : f // 2 * STEP + STEP, :]
    return rows if (f % 2 == 1) == upper else pltpu.roll(rows, DEEP, 0)


def columns_kernel(plane, via, drawn, south, north, first, last, stage):
    n_rows, n_cols = drawn.shape
    lane = lax.broadcasted_iota(jnp.int32, (STEP, LANES), 1)
    place = lane // DEEP

    def put(rows, pick):
        out = jnp.zeros((STEP, LANES), jnp.float32)
        for f in range(N_OWN):
            value = pick(f)
            head, tail = value[:, :LANES], value[:, n_cols - LANES :]
            if f:
                head = pltpu.roll(head, DEEP * f, 1)
            tail = pltpu.roll(tail, DEEP * (N_OWN + f + 1), 1)
            out = jnp.where(place == f, head, jnp.where(place == N_OWN + f, tail, out))
        stage[rows, :] = out

    def inner(k, carry):
        put(block(k + 1), lambda f: field_rows(plane, via, drawn, f, block(k)))
        return carry

    put(pl.ds(0, STEP), lambda f: tile_of(south, f, True))
    lax.fori_loop(0, n_rows // STEP, inner, 0, unroll=2)
    put(pl.ds(n_rows + STEP, STEP), lambda f: tile_of(north, f, False))
    rest = n_rows + 2 * STEP
    stage[rest:, :] = jnp.zeros((stage.shape[0] - rest, LANES), jnp.float32)
    turned = stage[...].T
    size = DEEP * N_OWN
    first[...] = turned[:size, :]
    last[...] = turned[size : 2 * size, :]


def side(strip, slot, blank):
    lane = lax.broadcasted_iota(jnp.int32, strip.shape, 1)
    turned = pltpu.roll(strip, (LANES - DEEP - 2 * DEEP * slot) % LANES, 1)
    return jnp.where((lane < DEEP) | (lane >= LANES - DEEP), turned, blank)


def corner_kernel(gz, plane, via, south, north, west, east, small):
    group = gz[0]
    half, tall_rows = plane.shape[1] // 2, west.shape[1]
    for f in range(N_FAR):
        at, mine = 2 * DEEP * f, pl.ds(DEEP * f, DEEP)
        inner = field_rows(plane, via, None, f, pl.ds(half - DEEP, DEEP))
        small[at : at + DEEP, :] = jnp.where(group == 0, inner, south[mine, :])
        inner = field_rows(plane, via, None, f, pl.ds(half, DEEP))
        small[at + DEEP : at + 2 * DEEP, :] = jnp.where(group == 0, north[mine, :], inner)
    at, size = 2 * DEEP * N_FAR, DEEP * N_FAR
    small[at : at + size, :tall_rows] = west[:size, :]
    small[at : at + size, tall_rows:] = east[:size, :]


def eastward(value):
    return pltpu.roll(value, value.shape[1] - 1, 1)


def westward(value):
    return pltpu.roll(value, 1, 1)


def rows_up(value):
    return pltpu.roll(value, STEP - 1, 0)


def rows_down(value):
    return pltpu.roll(value, 1, 0)


def joined(edge, inner, outer):
    sub = lax.broadcasted_iota(jnp.int32, inner.shape, 0)
    return jnp.where(sub == edge, outer, inner)


def edge_loop(wide, start, count, done):
    last = wide.shape[1] // STEP - 1

    def body(k, carried):
        kept = []
        for layer in range(2):
            value = wide[layer, block(start + k), :]
            over = wide[layer, block(jnp.minimum(start + k + 1, last)), :]
            above = joined(STEP - 1, rows_up(value), rows_up(over))
            to_east, to_north = mean(value, eastward(value)), mean(value, above)
            down = rows_down(to_north)
            south = joined(0, down, carried[layer])
            kept.append(down)
            done(layer, k, to_east, to_north, (to_east + westward(to_east)) + (to_north + south))
        return tuple(kept)

    none = jnp.zeros((STEP, wide.shape[2]), jnp.float32)
    lax.fori_loop(0, count, body, (none, none), unroll=2)


def own_kernel(gz, plane, via, drawn, south, north, west, east, near, edge_e, edge_n, near_sum, far_sum, wide, flat, tall):
    group = gz[0]
    n_rows, n_cols = drawn.shape
    half = n_rows // 2 // STEP
    flat[...] = jnp.zeros(flat.shape, jnp.float32)
    for f in range(N_OWN):
        at = 2 * DEEP * f
        flat[at : at + DEEP, :] = west[DEEP * f : DEEP * f + DEEP, :]
        flat[at + DEEP : at + 2 * DEEP, :] = east[DEEP * f : DEEP * f + DEEP, :]
    tall[...] = flat[...].T

    def put(target, index, rows, value, strip, f):
        target[index, rows, :n_cols] = value
        target[index, rows, n_cols:] = side(strip, f, 1.0 if f < N_FAR else 0.0)

    def inner(k, carry):
        rows = block(k + 1)
        strip = tall[rows, :]
        for f in range(2):
            put(wide, f, rows, plane[f, block(k), :], strip, f)
        return carry

    ends = (pl.ds(0, STEP), south, True), (pl.ds(n_rows + STEP, STEP), north, False)
    for rows, stack, upper in ends:
        for f in range(2):
            put(wide, f, rows, tile_of(stack, f, upper), tall[rows, :], f)
    lax.fori_loop(0, n_rows // STEP, inner, 0, unroll=2)

    def rest(k, carry):
        at = block(k + group * half)
        strip = tall[block(k + 1 + group * half), :]
        for f in range(2, N_OWN):
            put(near, f - 2, block(k + 1), field_rows(plane, via, drawn, f, at), strip, f)
        return carry

    lax.fori_loop(0, half, rest, 0, unroll=2)
    for f in range(2, N_OWN):
        value = field_rows(plane, via, drawn, f, pl.ds((half - 1) * STEP, STEP))
        value = jnp.where(group == 0, tile_of(south, f, True), value)
        put(near, f - 2, pl.ds(0, STEP), value, tall[block(group * half), :], f)
        value = field_rows(plane, via, drawn, f, pl.ds(half * STEP, STEP))
        value = jnp.where(group == 1, tile_of(north, f, False), value)
        strip = tall[block(half + 1 + group * half), :]
        put(near, f - 2, pl.ds((half + 1) * STEP, STEP), value, strip, f)

    def done(layer, k, to_east, to_north, total):
        edge_e[layer, block(k), :] = to_east
        edge_n[layer, block(k), :] = to_north
        near_sum[layer, block(k), :] = total

    edge_loop(wide, group * half, half + 2, done)

    def other(layer, k, to_east, to_north, total):
        far_sum[layer, block(jnp.maximum(k - 1, 0)), :] = total[:, :n_cols]

    edge_loop(wide, (1 - group) * half, half + 1, other)


def fold(total):
    width = total.shape[1]
    while width > LANES:
        width //= 2
        total = total[:, :width] + total[:, width:]
    return jnp.sum(total, axis=0, keepdims=True)


PAIRS = ((0, 0, 2), (1, 2, 0))


def image_pass(field, edges, cross, blocks, done, pairs=PAIRS):
    last = field.shape[1] // STEP - 1

    def at(k):
        return pl.ds(k * STEP, STEP)

    for q, base, facing in pairs:
        east, north = edges[q]
        ups, downs = {}, {}

        def up(layer, k):
            if (layer, k) not in ups:
                ups[layer, k] = rows_up(field[base + layer, at(k), :])
            return ups[layer, k]

        def down(layer, k):
            if (layer, k) not in downs:
                flux = north[layer, at(k), :] * field[base + layer, at(k), :]
                downs[layer, k] = rows_down(flux)
            return downs[layer, k]

        for k in blocks:
            owns, outs = [], []
            for layer in range(2):
                own, edge = field[base + layer, at(k), :], east[layer, at(k), :]
                above = joined(STEP - 1, up(layer, k), up(layer, min(k + 1, last)))
                below = joined(0, down(layer, k), down(layer, max(k - 1, 0)))
                across = edge * eastward(own) + westward(edge * own)
                owns.append(own)
                outs.append(across + (north[layer, at(k), :] * above + below))
            if facing is not None:
                outs[0] = outs[0] + cross[at(k), :] * field[facing, at(k), :]
            done(q, k, owns, outs)


def solved(inverse, q, k, outs):
    ii, oo, io = [inverse[3 * q + e, pl.ds(k * STEP, STEP), :] for e in range(3)]
    return [ii * outs[0] + io * outs[1], io * outs[0] + oo * outs[1]]


def dot(left, right, n_cols):
    return (left[0] * right[0] + left[1] * right[1])[:, :n_cols]


def image_step(field, edges, cross, inverse, stepped, keep, n_cols):
    n_blocks = field.shape[1] // STEP
    sums = [jnp.zeros((STEP, n_cols), jnp.float32)] * 2

    def done(q, k, owns, outs):
        news = solved(inverse, q, k, outs)
        for layer in range(2):
            stepped[2 * q + layer, pl.ds(k * STEP, STEP), :] = news[layer]
        if 0 < k < n_blocks - 1:
            for layer in range(2):
                keep[q][layer, pl.ds((k - 1) * STEP, STEP), :] = outs[layer][:, :n_cols]
            sums[0] = sums[0] + dot(owns, outs, n_cols)
            sums[1] = sums[1] + dot(news, outs, n_cols)

    image_pass(field, edges, cross, range(n_blocks), done)
    return sums


def edge_kernel(gz, near, near_e, near_n, near_sum, three, first, small, far_e, far_n, cross, inverse, step_1, n_own, inv_own, send, part, *scratch):
    fields, step_0, flat, tall = scratch
    group = gz[0]
    half, n_cols = first.shape
    n_blocks = half // STEP + 2
    tall_rows = tall.shape[0]
    flat[...] = jnp.zeros(flat.shape, jnp.float32)
    for f in range(N_FAR):
        at, row = 2 * DEEP * f, 2 * DEEP * N_FAR + DEEP * f
        flat[at : at + DEEP, :] = small[row : row + DEEP, :tall_rows]
        flat[at + DEEP : at + 2 * DEEP, :] = small[row : row + DEEP, tall_rows:]
    tall[...] = flat[...].T
    for k in range(n_blocks):
        rows = pl.ds(k * STEP, STEP)
        strip = tall[block(k + group * (half // STEP)), :]
        for f in range(N_FAR):
            if 0 < k < n_blocks - 1:
                core = (first if f == 2 else three.at[min(f, 2)])[(k - 1) * STEP : k * STEP, :]
            else:
                core = pltpu.roll(small[2 * DEEP * f : 2 * DEEP * f + STEP, :], DEEP, 0)
            fields[f, rows, :n_cols] = core
            fields[f, rows, n_cols:] = side(strip, f, 1.0)
    total = jnp.zeros((STEP, n_cols), jnp.float32)
    ups, downs = {}, {}

    def up(layer, k):
        if (layer, k) not in ups:
            ups[layer, k] = rows_up(fields[layer, k * STEP : k * STEP + STEP, :])
        return ups[layer, k]

    for k in range(n_blocks):
        rows = pl.ds(k * STEP, STEP)
        sums = [near_sum[0, rows, :], near_sum[1, rows, :]]
        for layer in range(2):
            value = fields[layer, rows, :]
            above = joined(STEP - 1, up(layer, k), up(layer, min(k + 1, n_blocks - 1)))
            to_east, to_north = mean(value, eastward(value)), mean(value, above)
            far_e[layer, rows, :] = to_east
            far_n[layer, rows, :] = to_north
            downs[layer, k] = rows_down(to_north)
            carried = joined(0, downs[layer, k], downs[layer, max(k - 1, 0)])
            sums.append((to_east + westward(to_east)) + (to_north + carried))
        link = mean(near[0, rows, :], fields[2, rows, :])
        cross[rows, :] = link
        drawn, pads = near[2, rows, :], near[3, rows, :]
        inner = pl.ds((k - 1) * STEP, STEP)
        both = []
        for q, up_edge in ((0, near[1, rows, :]), (1, fields[3, rows, :])):
            diag_i = sums[2 * q] + up_edge + link
            diag_o = sums[2 * q + 1] + up_edge + jnp.where(group == 1 - q, pads, 0.0)
            scale = 1.0 / (diag_i * diag_o - up_edge * up_edge)
            found = (diag_o * scale, diag_i * scale, up_edge * scale)
            for e in range(3):
                inverse[3 * q + e, rows, :] = found[e]
                if q == 0 and 0 < k < n_blocks - 1:
                    inv_own[e, inner, :] = found[e][:, :n_cols]
            both.append(found)
        one = jnp.where(group == 0, both[0][2], both[1][2]) * drawn
        two = jnp.where(group == 0, both[0][1], both[1][1]) * drawn
        step_0[0, rows, :], step_0[1, rows, :] = one, two
        if 0 < k < n_blocks - 1:
            total = total + (two * drawn)[:, :n_cols]
    part[...] = jnp.zeros(part.shape, jnp.float32)
    part[0:1, :] = fold(total)
    edges, keep = ((near_e, near_n), (far_e, far_n)), (n_own, send)
    for q in range(2):

        @pl.when(group == q)
        def _(q=q):
            first_step(q, step_0, edges, cross, inverse, step_1, keep, part)


def first_step(q, step_0, edges, cross, inverse, step_1, keep, part):
    n_cols = keep[0].shape[2]
    n_blocks, p = step_0.shape[1] // STEP, 1 - q
    sums = [jnp.zeros((STEP, n_cols), jnp.float32)] * 2

    def done(_, k, owns, outs):
        rows = pl.ds(k * STEP, STEP)
        news = solved(inverse, q, k, outs)
        over = cross[rows, :] * owns[0]
        facing = inverse[3 * p, rows, :] * over
        for layer in range(2):
            step_1[2 * q + layer, rows, :] = news[layer]
        step_1[2 * p, rows, :] = facing
        step_1[2 * p + 1, rows, :] = inverse[3 * p + 2, rows, :] * over
        if 0 < k < n_blocks - 1:
            inner = pl.ds((k - 1) * STEP, STEP)
            for layer in range(2):
                keep[q][layer, inner, :] = outs[layer][:, :n_cols]
            keep[p][0, inner, :] = over[:, :n_cols]
            keep[p][1, inner, :] = jnp.zeros((STEP, n_cols), jnp.float32)
            sums[0] = sums[0] + dot(owns, outs, n_cols)
            sums[1] = sums[1] + (dot(news, outs, n_cols) + (facing * over)[:, :n_cols])

    image_pass(step_0, edges, cross, range(n_blocks), done, ((q, 0, None),))
    part[1:2, :] = fold(sums[0])
    part[2:3, :] = fold(sums[1])


def steps_kernel(step_1, near_e, near_n, far_e, far_n, cross, inverse, before, n_own, send, spread, step_2):
    n_cols = n_own.shape[2]
    edges = ((near_e, near_n), (far_e, far_n))
    first, second = pl.ds(0, 2), pl.ds(2, 2)
    sums = image_step(
        step_1, edges, cross, inverse, step_2, (n_own.at[first], send.at[first]), n_cols
    )
    keep = (n_own.at[second], send.at[second])
    sums.append(jnp.zeros((STEP, n_cols), jnp.float32))

    def done(q, k, owns, outs):
        for layer in range(2):
            keep[q][layer, pl.ds((k - 1) * STEP, STEP), :] = outs[layer][:, :n_cols]
        sums[2] = sums[2] + dot(owns, outs, n_cols)

    image_pass(step_2, edges, cross, range(1, step_1.shape[1] // STEP - 1), done)
    row = lax.broadcasted_iota(jnp.int32, before.shape, 0)
    part = before[...]
    for j in range(3):
        part = jnp.where(row == 3 + j, fold(sums[j]), part)
    for k in range(spread.shape[0]):
        spread[k] = part


def inverse_kernel(gz, plane, via, sums, given, inverse):
    group = gz[0]
    half = inverse.shape[1]

    def fill(k, carry):
        rows, at = block(k), block(k + (1 - group) * (half // STEP))
        up = via[1, at, :]
        diag_i = sums[0, rows, :] + up + mean(via[0, at, :], given[rows, :])
        diag_o = sums[1, rows, :] + up + jnp.where(group == 1, plane[2, at, :], 0.0)
        scale = 1.0 / (diag_i * diag_o - up * up)
        inverse[0, rows, :] = diag_o * scale
        inverse[1, rows, :] = diag_i * scale
        inverse[2, rows, :] = up * scale
        return carry

    lax.fori_loop(0, half // STEP, fill, 0, unroll=2)


def tree(parts):
    values = [parts[k] for k in range(parts.shape[0])]
    while len(values) > 1:
        values = [a + b for a, b in zip(values[::2], values[1::2])]
    return values[0]


def relay_kernel(parts, spread):
    total = tree(parts)
    for k in range(spread.shape[0]):
        spread[k] = total


def solve(parts):
    sums = jnp.sum(tree(parts), axis=1, keepdims=True)
    g = [jnp.broadcast_to(sums[k : k + 1, :], (1, LANES)) for k in range(6)]
    step = [g[k] - g[k + 1] for k in range(5)]
    scale = [lax.rsqrt(g[0]), lax.rsqrt(g[2]), lax.rsqrt(g[4])]

    def entry(i, j):
        return step[i + j] * scale[i] * scale[j]

    d0 = entry(0, 0)
    l10, l20 = entry(1, 0) / d0, entry(2, 0) / d0
    d1 = entry(1, 1) - l10 * entry(1, 0)
    e21 = entry(2, 1) - l20 * entry(1, 0)
    l21 = e21 / d1
    d2 = entry(2, 2) - l20 * entry(2, 0) - l21 * e21
    y0 = g[0] * scale[0]
    y1 = g[1] * scale[1] - l10 * y0
    y2 = g[2] * scale[2] - l20 * y0 - l21 * y1
    x2 = y2 / d2
    x1 = y1 / d1 - l21 * x2
    x0 = y0 / d0 - l10 * x1 - l20 * x2
    c0, c1, c2 = x0 * scale[0], x1 * scale[1], x2 * scale[2]
    good = (d0 > GUARD) & (d1 > GUARD) & (d2 > GUARD)
    return (c0, c1, c2, 1.0 - c0, c0 - c1, c1 - c2), good


def combine_kernel(gz, parts, current, inv_near, inv_far, n_0, n_0_far, n_12, n_12_far, volts, left, flag, volts_here, left_here, sems):
    group = gz[0]
    half, n_cols = n_0.shape[1:]
    values, good = solve(parts)
    flag[...] = jnp.where(good, 1, 0)
    c = [jnp.broadcast_to(value[:, 0:1], (STEP, n_cols)) for value in values]

    def fill(part, inv, first, second):
        def body(k, carry):
            rows, at = block(k), block(k + part * (half // STEP))
            drawn = jnp.where(group == 0, current[at, :], 0.0)
            n0i, n0o = first[0, rows, :], first[1, rows, :]
            n1i, n1o, n2i, n2o = [second[j, rows, :] for j in range(4)]
            ii, oo, io = [inv[e, rows, :] for e in range(3)]
            one = c[1] * n0i + c[2] * n1i
            two = c[0] * drawn + (c[1] * n0o + c[2] * n1o)
            volts_here[1 - group, at, :] = ii * one + io * two
            volts_here[group, at, :] = io * one + oo * two
            left_here[1 - group, at, :] = c[4] * n0i + c[5] * n1i + c[2] * n2i
            left_here[group, at, :] = c[3] * drawn + c[4] * n0o + c[5] * n1o + c[2] * n2o
            return carry

        lax.fori_loop(0, half // STEP, body, 0, unroll=2)

    copies = []
    for part in range(2):

        @pl.when(group == part)
        def _(part=part):
            fill(part, inv_near, n_0, n_12)

        @pl.when(group != part)
        def _(part=part):
            fill(part, inv_far, n_0_far, n_12_far)

        for j, (source, target) in enumerate(((volts_here, volts), (left_here, left))):
            rows = pl.ds(part * half, half)
            copy = pltpu.make_async_copy(
                source.at[:, rows, :], target.at[:, rows, :], sems.at[2 * part + j]
            )
            copy.start()
            copies.append(copy)
    for copy in copies:
        copy.wait()


def call(kernel, outs, scratch, n_smem, *args, outside=0):
    return pl.pallas_call(
        kernel,
        in_specs=[SMEM] * n_smem + [VMEM] * (len(args) - n_smem),
        out_specs=[OUTSIDE] * outside + [VMEM] * (len(outs) - outside),
        out_shape=outs,
        scratch_shapes=scratch,
        compiler_params=pltpu.CompilerParams(vmem_limit_bytes=GRANT),
    )(*args)


def shards(load_current, sink_mask, pad_mask, plane_class, via_class, plane_table, via_table):
    _, n_rows, n_cols = plane_class.shape
    half, frame = n_rows // 2, n_rows // 2 + 2 * STEP
    tall = -(-(n_rows + 2 * STEP) // LANES) * LANES
    broad = n_cols + LANES

    def array(*shape):
        return jax.ShapeDtypeStruct(shape, jnp.float32)

    def ring(axis):
        size = lax.axis_size(axis)
        return [(i, (i + 1) % size) for i in range(size)]

    def back(pairs):
        return [(b, a) for a, b in pairs]

    turn = [pltpu.VMEM((LANES, tall), jnp.float32), pltpu.VMEM((tall, LANES), jnp.float32)]
    gz = lax.axis_index("gz").reshape(1).astype(jnp.int32)
    swap = [(0, 1), (1, 0)]
    rest = ("gy_0", "gy_1", "gz")
    n_gx, n_rest = lax.axis_size(GX), lax.axis_size(rest)

    via, one, via_send = call(
        via_kernel,
        [array(2, n_rows, n_cols), array(half, n_cols), array(half, n_cols)],
        [], 1, gz, via_table, via_class,
    )
    big_via = lax.ppermute(one, "gz", swap)
    plane, drawn, three, top, bottom = call(
        plane_kernel,
        [array(3, n_rows, n_cols), array(n_rows, n_cols), array(3, half, n_cols)]
        + [array(DEEP * N_OWN, n_cols)] * 2,
        [], 1, gz, plane_table, plane_class, load_current, sink_mask, pad_mask, via,
    )
    south = lax.ppermute(bottom, GY, ring(GY))
    north = lax.ppermute(top, GY, back(ring(GY)))
    big_plane = lax.ppermute(three, "gz", swap)
    first, last = call(
        columns_kernel, [array(DEEP * N_OWN, tall)] * 2, turn[1:], 0,
        plane, via, drawn, south, north,
    )
    west = lax.ppermute(last, GX, ring(GX))
    east = lax.ppermute(first, GX, back(ring(GX)))
    (small_send,) = call(
        corner_kernel, [array(N_FAR * 3 * DEEP, n_cols)], [], 1,
        gz, plane, via, south, north, west, east,
    )
    small = lax.ppermute(small_send, "gz", swap)
    via_far = lax.ppermute(via_send, "gz", swap)
    near, near_e, near_n, near_sum, far_sum = call(
        own_kernel,
        [array(4, frame, broad)] + [array(2, frame, broad)] * 3 + [array(2, half, n_cols)],
        [pltpu.VMEM((2, n_rows + 2 * STEP, broad), jnp.float32)] + turn,
        1, gz, plane, via, drawn, south, north, west, east,
    )
    far_e, far_n, cross, inverse, step_1, n_0, inv_near, send, part = call(
        edge_kernel,
        [array(2, frame, broad)] * 2
        + [array(frame, broad), array(6, frame, broad), array(4, frame, broad),
           array(2, half, n_cols), array(3, half, n_cols), array(2, half, n_cols), array(STEP, LANES)],
        [pltpu.VMEM((N_FAR, frame, broad), jnp.float32), pltpu.VMEM((2, frame, broad), jnp.float32)]
        + turn,
        1, gz, near, near_e, near_n, near_sum, big_plane, big_via, small,
    )
    n_0_far = lax.ppermute(send, "gz", swap)
    (inv_far,) = call(
        inverse_kernel, [array(3, half, n_cols)], [], 1,
        gz, plane, via, far_sum, via_far,
    )
    n_12, send, spread = call(
        steps_kernel,
        [array(4, half, n_cols), array(4, half, n_cols), array(n_gx, STEP, LANES)],
        [pltpu.VMEM((4, frame, broad), jnp.float32)],
        0, step_1, near_e, near_n, far_e, far_n, cross, inverse, part,
    )
    n_12_far = lax.ppermute(send, "gz", swap)
    parts = lax.all_to_all(spread, GX, 0, 0, tiled=True)
    (spread,) = call(relay_kernel, [array(n_rest, STEP, LANES)], [], 0, parts)
    parts = lax.all_to_all(spread, rest, 0, 0, tiled=True)
    volts, left, flag = call(
        combine_kernel,
        [array(2, n_rows, n_cols)] * 2 + [jax.ShapeDtypeStruct((1, LANES), jnp.int32)],
        [pltpu.VMEM((2, n_rows, n_cols), jnp.float32)] * 2 + [pltpu.SemaphoreType.DMA((4,))],
        1, gz, parts, drawn, inv_near, inv_far, n_0, n_0_far, n_12, n_12_far, outside=2,
    )

    def careful():
        return recurrence(
            load_current, sink_mask, pad_mask, plane_class, via_class, plane_table, via_table
        )

    return lax.cond(flag[0, 0] == 1, lambda: (volts, left), careful)


def solution(mesh):
    split = Mesh(
        mesh.devices.reshape(8, 2, 2, 4, mesh.shape["gz"]), ("gx_0", "gx_1", "gy_0", "gy_1", "gz")
    )
    placed = (
        P(GY, GX),
        P(GY, GX),
        P(GY, GX),
        P("gz", GY, GX),
        P("gz", GY, GX),
        P("gz", None),
        P("gz", None),
    )
    return jax.shard_map(
        shards,
        mesh=split,
        in_specs=placed,
        out_specs=(P("gz", GY, GX), P("gz", GY, GX)),
        check_vma=False,
    )
```

```python
import jax
import jax.numpy as jnp
from jax import lax
from jax.experimental import pallas as pl
from jax.experimental.pallas import tpu as pltpu
from jax.sharding import Mesh
from jax.sharding import PartitionSpec as P

ITERS = 3
GX = ("gx_0", "gx_1")
GY = ("gy_0", "gy_1")
GX_GY_GZ = ("gx_0", "gx_1", "gy_0", "gy_1", "gz")


PAD_CONDUCTANCE = 20.0


def padded(array, sides, width):
    edges = {}
    for axis, dim in sides:
        peers, length = (lax.axis_size(axis), array.shape[dim])
        up = [(i, (i + 1) % peers) for i in range(peers)]
        last = lax.slice_in_dim(array, length - width, length, axis=dim)
        leading = lax.slice_in_dim(array, 0, width, axis=dim)
        edges[dim] = (
            lax.ppermute(last, axis, up),
            lax.ppermute(leading, axis, [(b, a) for a, b in up]),
        )
    done = []
    for _, dim in sides:
        low, high = edges[dim]
        around = [(width, width) if d in done else (0, 0) for d in range(array.ndim)]
        array = jnp.concatenate([jnp.pad(low, around), array, jnp.pad(high, around)], axis=dim)
        done.append(dim)
    return array


def padded_2(block, sides, width):
    for axis, dim in sides:
        count = lax.axis_size(axis)
        forward = [(i, i + 1) for i in range(count - 1)]
        backward = [(target, source) for source, target in forward]
        low = lax.ppermute(
            lax.slice_in_dim(block, block.shape[dim] - width, None, axis=dim), axis, forward
        )
        high = lax.ppermute(lax.slice_in_dim(block, 0, width, axis=dim), axis, backward)
        block = jnp.concatenate([low, block, high], axis=dim)
    return block


def by_axis(array, axes):
    for axis in axes:
        array = lax.psum(array, axis)
    return array


def lookup(classes, table):
    summed = jnp.zeros(classes.shape, jnp.float32)
    for level in range(table.shape[1]):
        summed = summed + jnp.where(
            classes == level, table[:, level][:, None, None], jnp.float32(0.0)
        )
    return summed


def harmonic(first, second):
    return 2.0 * first * second / (first + second)


def factor(diagonal, up_edge):
    inverses = []
    factors = []
    for level in range(diagonal.shape[0]):
        pivots = diagonal[level]
        if level > 0:
            pivots = pivots + up_edge[level - 1] * factors[level - 1]
        inverse = 1.0 / pivots
        inverses.append(inverse)
        factors.append(-up_edge[level] * inverse)
    return (jnp.stack(inverses), jnp.stack(factors))


def solve_block(inverses, factors, up_edge, source_term):
    forward = []
    for level in range(source_term.shape[0]):
        entries = source_term[level]
        if level > 0:
            entries = entries + up_edge[level - 1] * forward[level - 1]
        forward.append(entries * inverses[level])
    result = [forward[-1]]
    level = 0
    result.insert(0, forward[level] - factors[level] * result[0])
    return jnp.stack(result)


def plane_extend(field):
    return padded(field, ((GX, 2), (GY, 1)), 1)


def layer_extend(field):
    return padded_2(field, (("gz", 0),), 1)


def merged_sums(residual, precond, image_field):
    return (
        by_axis(jnp.sum(residual * precond), GX_GY_GZ),
        by_axis(jnp.sum(image_field * precond), GX_GY_GZ),
    )


def recurrence(load_current, sink_mask, pad_mask, plane_class, via_class, plane_table, via_table):
    n_layers, n_rows, n_cols = plane_class.shape
    g_plane = lookup(plane_class, plane_table)
    g_via = lookup(via_class, via_table)
    plane_ext = plane_extend(g_plane)
    middle = plane_ext[:, 1:-1, :]
    across = harmonic(middle[:, :, :-1], middle[:, :, 1:])
    east_edge = across[:, :, 1:]
    west_edge = across[:, :, :-1]
    column = plane_ext[:, :, 1:-1]
    along_rows = harmonic(column[:, :-1], column[:, 1:])
    north_edge = along_rows[:, 1:]
    south_edge = along_rows[:, :-1]
    via_ext = layer_extend(g_via)
    vertical = harmonic(via_ext[:-1], via_ext[1:])
    up_edge = vertical[1:]
    down_edge = vertical[:-1]
    group_index = lax.axis_index("gz")
    is_top = group_index == lax.axis_size("gz") - 1
    is_bottom = group_index == 0
    pad_plane = jnp.where(is_top, PAD_CONDUCTANCE * pad_mask.astype(jnp.float32), jnp.float32(0.0))
    pad_layer = jnp.concatenate(
        [jnp.zeros((n_layers - 1, n_rows, n_cols), jnp.float32), pad_plane[None]], 0
    )
    diagonal = east_edge + west_edge + north_edge + south_edge + up_edge + down_edge + pad_layer
    inverses, factors = factor(diagonal, up_edge)

    def precondition(residual):
        return solve_block(inverses, factors, up_edge, residual)

    def operate(field):
        inner = plane_extend(field)
        layer_ext = layer_extend(field)
        above_field = layer_ext[2:]
        below_field = layer_ext[:-2]
        return (
            diagonal * field
            - east_edge * inner[:, 1:-1, 2:]
            - west_edge * inner[:, 1:-1, :-2]
            - north_edge * inner[:, 2:, 1:-1]
            - south_edge * inner[:, :-2, 1:-1]
            - up_edge * above_field
            - down_edge * below_field
        )

    source = jnp.where(is_bottom, sink_mask.astype(jnp.float32) * load_current, jnp.float32(0.0))
    right_side = jnp.concatenate(
        [source[None], jnp.zeros((n_layers - 1, n_rows, n_cols), jnp.float32)], 0
    )
    voltage = jnp.zeros((n_layers, n_rows, n_cols), jnp.float32)
    residual = right_side
    precond = precondition(residual)
    image_field = operate(precond)
    weight_now, curvature = merged_sums(residual, precond, image_field)
    step_size = weight_now / curvature
    direction = precond
    image_dir = image_field
    for iteration in range(ITERS):
        voltage = voltage + step_size * direction
        residual = residual - step_size * image_dir
        if iteration + 1 < ITERS:
            precond = precondition(residual)
            image_field = operate(precond)
            weight_next, curvature = merged_sums(residual, precond, image_field)
            momentum = weight_next / weight_now
            step_size = weight_next / (curvature - momentum * weight_next / step_size)
            direction = precond + momentum * direction
            image_dir = image_field + momentum * image_dir
            weight_now = weight_next
    return (voltage, residual)


STEP = 8
LANES = 128
DEEP = 4
GUARD = 0.02
GRANT = 16 * 1024 * 1024
N_OWN = 6
N_FAR = 4
VMEM = pl.BlockSpec(memory_space=pltpu.VMEM)
SMEM = pl.BlockSpec(memory_space=pltpu.SMEM)
OUTSIDE = pl.BlockSpec(memory_space=pl.ANY)


def block(k):
    return pl.ds(pl.multiple_of(k * STEP, STEP), STEP)


def mean(first, second):
    return 1.0 / (first + second)


def half_reciprocals(table, layer, n_cols):
    row = 0.5 / table[pl.ds(layer, 1), :]
    return [jnp.broadcast_to(row[:, e : e + 1], (STEP, n_cols)) for e in range(row.shape[1])]


def look_up(entries, classes):
    low = (classes & 1) != 0
    mid = (classes & 2) != 0
    pairs = [jnp.where(low, entries[2 * k + 1], entries[2 * k]) for k in range(4)]
    return jnp.where(
        classes > 3, jnp.where(mid, pairs[3], pairs[2]), jnp.where(mid, pairs[1], pairs[0])
    )


def via_kernel(gz, table, classes, via, first, lone):
    group = gz[0]
    n_rows, n_cols = via.shape[1:]
    half = n_rows // 2 // STEP
    of_i, of_o = [half_reciprocals(table, layer, n_cols) for layer in (1 - group, group)]

    def fill(k, carry):
        rows = block(k)
        one = look_up(of_i, classes[1 - group, rows, :])
        two = look_up(of_o, classes[group, rows, :])
        via[0, rows, :] = one
        via[1, rows, :] = mean(one, two)
        return carry

    lax.fori_loop(0, n_rows // STEP, fill, 0, unroll=8)

    def copy(k, carry):
        first[block(k), :] = via[0, block(k + (1 - group) * half), :]
        lone[block(k), :] = via[0, block(k + group * half), :]
        return carry

    lax.fori_loop(0, half, copy, 0, unroll=12)


def plane_kernel(gz, table, classes, load, sink, pad, via, plane, drawn, three, top, bottom):
    group = gz[0]
    n_rows, n_cols = plane.shape[1:]
    half = n_rows // 2 // STEP
    of_i, of_o = [half_reciprocals(table, layer, n_cols) for layer in (1 - group, group)]

    def fill(k, carry):
        rows = block(k)
        plane[0, rows, :] = look_up(of_i, classes[1 - group, rows, :])
        plane[1, rows, :] = look_up(of_o, classes[group, rows, :])
        plane[2, rows, :] = PAD_CONDUCTANCE * pad[rows, :].astype(jnp.float32)
        drawn[rows, :] = sink[rows, :].astype(jnp.float32) * load[rows, :]
        return carry

    lax.fori_loop(0, n_rows // STEP, fill, 0, unroll=8)

    def copy(k, carry):
        rows = block(k + (1 - group) * half)
        for f in range(2):
            three[f, block(k), :] = plane[f, rows, :]
        three[2, block(k), :] = via[1, rows, :]
        return carry

    lax.fori_loop(0, half, copy, 0, unroll=12)
    for f in range(N_OWN):
        at = pl.ds(DEEP * f, DEEP)
        top[at, :] = field_rows(plane, via, drawn, f, pl.ds(0, DEEP))
        bottom[at, :] = field_rows(plane, via, drawn, f, pl.ds(n_rows - DEEP, DEEP))


def field_rows(plane, via, drawn, f, rows):
    if f == 4:
        return drawn[rows, :]
    if f in (2, 3):
        return via[f - 2, rows, :]
    return plane[2 if f == 5 else f, rows, :]


def tile_of(stack, f, upper):
    rows = stack[f // 2 * STEP : f // 2 * STEP + STEP, :]
    return rows if (f % 2 == 1) == upper else pltpu.roll(rows, DEEP, 0)


def columns_kernel(plane, via, drawn, south, north, first, last, stage):
    n_rows, n_cols = drawn.shape
    lane = lax.broadcasted_iota(jnp.int32, (STEP, LANES), 1)
    place = lane // DEEP

    def put(rows, pick):
        out = jnp.zeros((STEP, LANES), jnp.float32)
        for f in range(N_OWN):
            value = pick(f)
            head, tail = value[:, :LANES], value[:, n_cols - LANES :]
            if f:
                head = pltpu.roll(head, DEEP * f, 1)
            tail = pltpu.roll(tail, DEEP * (N_OWN + f + 1), 1)
            out = jnp.where(place == f, head, jnp.where(place == N_OWN + f, tail, out))
        stage[rows, :] = out

    def inner(k, carry):
        put(block(k + 1), lambda f: field_rows(plane, via, drawn, f, block(k)))
        return carry

    put(pl.ds(0, STEP), lambda f: tile_of(south, f, True))
    lax.fori_loop(0, n_rows // STEP, inner, 0, unroll=8)
    put(pl.ds(n_rows + STEP, STEP), lambda f: tile_of(north, f, False))
    rest = n_rows + 2 * STEP
    stage[rest:, :] = jnp.zeros((stage.shape[0] - rest, LANES), jnp.float32)
    turned = stage[...].T
    size = DEEP * N_OWN
    first[...] = turned[:size, :]
    last[...] = turned[size : 2 * size, :]


def side(strip, slot, blank):
    lane = lax.broadcasted_iota(jnp.int32, strip.shape, 1)
    turned = pltpu.roll(strip, (LANES - DEEP - 2 * DEEP * slot) % LANES, 1)
    return jnp.where((lane < DEEP) | (lane >= LANES - DEEP), turned, blank)


def corner_kernel(gz, plane, via, south, north, west, east, small):
    group = gz[0]
    half, tall_rows = plane.shape[1] // 2, west.shape[1]
    for f in range(N_FAR):
        at, mine = 2 * DEEP * f, pl.ds(DEEP * f, DEEP)
        inner = field_rows(plane, via, None, f, pl.ds(half - DEEP, DEEP))
        small[at : at + DEEP, :] = jnp.where(group == 0, inner, south[mine, :])
        inner = field_rows(plane, via, None, f, pl.ds(half, DEEP))
        small[at + DEEP : at + 2 * DEEP, :] = jnp.where(group == 0, north[mine, :], inner)
    at, size = 2 * DEEP * N_FAR, DEEP * N_FAR
    small[at : at + size, :tall_rows] = west[:size, :]
    small[at : at + size, tall_rows:] = east[:size, :]


def eastward(value):
    return pltpu.roll(value, value.shape[1] - 1, 1)


def westward(value):
    return pltpu.roll(value, 1, 1)


def rows_up(value):
    return pltpu.roll(value, STEP - 1, 0)


def rows_down(value):
    return pltpu.roll(value, 1, 0)


def joined(edge, inner, outer):
    sub = lax.broadcasted_iota(jnp.int32, inner.shape, 0)
    return jnp.where(sub == edge, outer, inner)


def own_kernel(gz, plane, via, drawn, south, north, west, east, near, edge_e, edge_n, near_sum, far_sum, wide, flat, tall):
    group = gz[0]
    n_rows, n_cols = drawn.shape
    half, last = n_rows // 2 // STEP, n_rows // STEP + 1
    flat[...] = jnp.zeros(flat.shape, jnp.float32)
    for f in range(N_OWN):
        at = 2 * DEEP * f
        flat[at : at + DEEP, :] = west[DEEP * f : DEEP * f + DEEP, :]
        flat[at + DEEP : at + 2 * DEEP, :] = east[DEEP * f : DEEP * f + DEEP, :]
    tall[...] = flat[...].T

    def put(rows, pick):
        strip = tall[rows, :]
        for f in range(2):
            wide[f, rows, :n_cols] = pick(f)
            wide[f, rows, n_cols:] = side(strip, f, 1.0)

    def inner(k, carry):
        put(block(k + 1), lambda f: plane[f, block(k), :])
        return carry

    put(pl.ds(0, STEP), lambda f: tile_of(south, f, True))
    lax.fori_loop(0, n_rows // STEP, inner, 0, unroll=8)
    put(pl.ds(n_rows + STEP, STEP), lambda f: tile_of(north, f, False))

    def around(layer, k):
        value = wide[layer, block(k), :]
        over = wide[layer, block(jnp.minimum(k + 1, last)), :]
        under = wide[layer, block(jnp.maximum(k - 1, 0)), :]
        above = joined(STEP - 1, rows_up(value), rows_up(over))
        below = joined(0, rows_down(value), rows_down(under))
        to_east, to_north = mean(value, eastward(value)), mean(value, above)
        return to_east, to_north, (to_east + westward(to_east)) + (to_north + mean(value, below))

    def frame(k, carry):
        at = k + group * half
        for layer in range(2):
            to_east, to_north, total = around(layer, at)
            edge_e[layer, block(k), :] = to_east
            edge_n[layer, block(k), :] = to_north
            near_sum[layer, block(k), :] = total
        strip = tall[block(at), :]
        inside = block(jnp.clip(at - 1, 0, last - 2))
        for place, f in enumerate((2, 3, 4, 5)):
            core = field_rows(plane, via, drawn, f, inside)
            core = jnp.where(at == 0, tile_of(south, f, True), core)
            core = jnp.where(at == last, tile_of(north, f, False), core)
            near[place, block(k), :n_cols] = core
            near[place, block(k), n_cols:] = side(strip, f, 1.0 if f < N_FAR else 0.0)
        return carry

    lax.fori_loop(0, half + 2, frame, 0, unroll=7)

    def other(k, carry):
        for layer in range(2):
            total = around(layer, k + 1 + (1 - group) * half)[2]
            far_sum[layer, block(k), :] = total[:, :n_cols]
        return carry

    lax.fori_loop(0, half, other, 0, unroll=6)


def fold(total):
    width = total.shape[1]
    while width > LANES:
        width //= 2
        total = total[:, :width] + total[:, width:]
    return jnp.sum(total, axis=0, keepdims=True)


PAIRS = ((0, 0, 2), (1, 2, 0))


def image_pass(field, edges, cross, blocks, done, pairs=PAIRS):
    last = field.shape[1] // STEP - 1

    def at(k):
        return pl.ds(k * STEP, STEP)

    for q, base, facing in pairs:
        east, north = edges[q]
        ups, downs = {}, {}

        def up(layer, k):
            if (layer, k) not in ups:
                ups[layer, k] = rows_up(field[base + layer, at(k), :])
            return ups[layer, k]

        def down(layer, k):
            if (layer, k) not in downs:
                flux = north[layer, at(k), :] * field[base + layer, at(k), :]
                downs[layer, k] = rows_down(flux)
            return downs[layer, k]

        for k in blocks:
            owns, outs = [], []
            for layer in range(2):
                own, edge = field[base + layer, at(k), :], east[layer, at(k), :]
                above = joined(STEP - 1, up(layer, k), up(layer, min(k + 1, last)))
                below = joined(0, down(layer, k), down(layer, max(k - 1, 0)))
                across = edge * eastward(own) + westward(edge * own)
                owns.append(own)
                outs.append(across + (north[layer, at(k), :] * above + below))
            if facing is not None:
                outs[0] = outs[0] + cross[at(k), :] * field[facing, at(k), :]
            done(q, k, owns, outs)


def solved(inverse, q, k, outs):
    ii, oo, io = [inverse[3 * q + e, pl.ds(k * STEP, STEP), :] for e in range(3)]
    return [ii * outs[0] + io * outs[1], io * outs[0] + oo * outs[1]]


def dot(left, right, n_cols):
    return (left[0] * right[0] + left[1] * right[1])[:, :n_cols]


def image_step(field, edges, cross, inverse, stepped, keep, n_cols):
    n_blocks = field.shape[1] // STEP
    sums = [jnp.zeros((STEP, n_cols), jnp.float32)] * 2

    def done(q, k, owns, outs):
        news = solved(inverse, q, k, outs)
        for layer in range(2):
            stepped[2 * q + layer, pl.ds(k * STEP, STEP), :] = news[layer]
        if 0 < k < n_blocks - 1:
            for layer in range(2):
                keep[q][layer, pl.ds((k - 1) * STEP, STEP), :] = outs[layer][:, :n_cols]
            sums[0] = sums[0] + dot(owns, outs, n_cols)
            sums[1] = sums[1] + dot(news, outs, n_cols)

    image_pass(field, edges, cross, range(n_blocks), done)
    return sums


def edge_kernel(gz, near, near_e, near_n, near_sum, three, first, small, far_e, far_n, cross, inverse, step_1, n_own, inv_own, send, part, *scratch):
    fields, step_0, flat, tall = scratch
    group = gz[0]
    half, n_cols = first.shape
    n_blocks = half // STEP + 2
    tall_rows = tall.shape[0]
    flat[...] = jnp.zeros(flat.shape, jnp.float32)
    for f in range(N_FAR):
        at, row = 2 * DEEP * f, 2 * DEEP * N_FAR + DEEP * f
        flat[at : at + DEEP, :] = small[row : row + DEEP, :tall_rows]
        flat[at + DEEP : at + 2 * DEEP, :] = small[row : row + DEEP, tall_rows:]
    tall[...] = flat[...].T
    for k in range(n_blocks):
        rows = pl.ds(k * STEP, STEP)
        strip = tall[block(k + group * (half // STEP)), :]
        for f in range(N_FAR):
            if 0 < k < n_blocks - 1:
                core = (first if f == 2 else three.at[min(f, 2)])[(k - 1) * STEP : k * STEP, :]
            else:
                core = pltpu.roll(small[2 * DEEP * f : 2 * DEEP * f + STEP, :], DEEP, 0)
            fields[f, rows, :n_cols] = core
            fields[f, rows, n_cols:] = side(strip, f, 1.0)
    total = jnp.zeros((STEP, n_cols), jnp.float32)
    ups, downs = {}, {}

    def up(layer, k):
        if (layer, k) not in ups:
            ups[layer, k] = rows_up(fields[layer, k * STEP : k * STEP + STEP, :])
        return ups[layer, k]

    for k in range(n_blocks):
        rows = pl.ds(k * STEP, STEP)
        sums = [near_sum[0, rows, :], near_sum[1, rows, :]]
        for layer in range(2):
            value = fields[layer, rows, :]
            above = joined(STEP - 1, up(layer, k), up(layer, min(k + 1, n_blocks - 1)))
            to_east, to_north = mean(value, eastward(value)), mean(value, above)
            far_e[layer, rows, :] = to_east
            far_n[layer, rows, :] = to_north
            downs[layer, k] = rows_down(to_north)
            carried = joined(0, downs[layer, k], downs[layer, max(k - 1, 0)])
            sums.append((to_east + westward(to_east)) + (to_north + carried))
        link = mean(near[0, rows, :], fields[2, rows, :])
        cross[rows, :] = link
        drawn, pads = near[2, rows, :], near[3, rows, :]
        inner = pl.ds((k - 1) * STEP, STEP)
        both = []
        for q, up_edge in ((0, near[1, rows, :]), (1, fields[3, rows, :])):
            diag_i = sums[2 * q] + up_edge + link
            diag_o = sums[2 * q + 1] + up_edge + jnp.where(group == 1 - q, pads, 0.0)
            scale = 1.0 / (diag_i * diag_o - up_edge * up_edge)
            found = (diag_o * scale, diag_i * scale, up_edge * scale)
            for e in range(3):
                inverse[3 * q + e, rows, :] = found[e]
                if q == 0 and 0 < k < n_blocks - 1:
                    inv_own[e, inner, :] = found[e][:, :n_cols]
            both.append(found)
        one = jnp.where(group == 0, both[0][2], both[1][2]) * drawn
        two = jnp.where(group == 0, both[0][1], both[1][1]) * drawn
        step_0[0, rows, :], step_0[1, rows, :] = one, two
        if 0 < k < n_blocks - 1:
            total = total + (two * drawn)[:, :n_cols]
    part[...] = jnp.zeros(part.shape, jnp.float32)
    part[0:1, :] = fold(total)
    edges, keep = ((near_e, near_n), (far_e, far_n)), (n_own, send)
    for q in range(2):

        @pl.when(group == q)
        def _(q=q):
            first_step(q, step_0, edges, cross, inverse, step_1, keep, part)


def first_step(q, step_0, edges, cross, inverse, step_1, keep, part):
    n_cols = keep[0].shape[2]
    n_blocks, p = step_0.shape[1] // STEP, 1 - q
    sums = [jnp.zeros((STEP, n_cols), jnp.float32)] * 2

    def done(_, k, owns, outs):
        rows = pl.ds(k * STEP, STEP)
        news = solved(inverse, q, k, outs)
        over = cross[rows, :] * owns[0]
        facing = inverse[3 * p, rows, :] * over
        for layer in range(2):
            step_1[2 * q + layer, rows, :] = news[layer]
        step_1[2 * p, rows, :] = facing
        step_1[2 * p + 1, rows, :] = inverse[3 * p + 2, rows, :] * over
        if 0 < k < n_blocks - 1:
            inner = pl.ds((k - 1) * STEP, STEP)
            for layer in range(2):
                keep[q][layer, inner, :] = outs[layer][:, :n_cols]
            keep[p][0, inner, :] = over[:, :n_cols]
            keep[p][1, inner, :] = jnp.zeros((STEP, n_cols), jnp.float32)
            sums[0] = sums[0] + dot(owns, outs, n_cols)
            sums[1] = sums[1] + (dot(news, outs, n_cols) + (facing * over)[:, :n_cols])

    image_pass(step_0, edges, cross, range(n_blocks), done, ((q, 0, None),))
    part[1:2, :] = fold(sums[0])
    part[2:3, :] = fold(sums[1])


def steps_kernel(step_1, near_e, near_n, far_e, far_n, cross, inverse, before, n_own, send, spread, step_2):
    n_cols = n_own.shape[2]
    edges = ((near_e, near_n), (far_e, far_n))
    first, second = pl.ds(0, 2), pl.ds(2, 2)
    sums = image_step(
        step_1, edges, cross, inverse, step_2, (n_own.at[first], send.at[first]), n_cols
    )
    keep = (n_own.at[second], send.at[second])
    sums.append(jnp.zeros((STEP, n_cols), jnp.float32))

    def done(q, k, owns, outs):
        for layer in range(2):
            keep[q][layer, pl.ds((k - 1) * STEP, STEP), :] = outs[layer][:, :n_cols]
        sums[2] = sums[2] + dot(owns, outs, n_cols)

    image_pass(step_2, edges, cross, range(1, step_1.shape[1] // STEP - 1), done)
    row = lax.broadcasted_iota(jnp.int32, before.shape, 0)
    part = before[...]
    for j in range(3):
        part = jnp.where(row == 3 + j, fold(sums[j]), part)
    sums = jnp.sum(part, axis=1, keepdims=True)
    lane = lax.broadcasted_iota(jnp.int32, part.shape, 1)
    line = jnp.sum(jnp.where(lane == row, sums, 0.0), axis=0, keepdims=True)
    for k in range(spread.shape[0]):
        spread[k] = line


def inverse_kernel(gz, plane, via, sums, given, inverse):
    group = gz[0]
    half = inverse.shape[1]

    def fill(k, carry):
        rows, at = block(k), block(k + (1 - group) * (half // STEP))
        up = via[1, at, :]
        diag_i = sums[0, rows, :] + up + mean(via[0, at, :], given[rows, :])
        diag_o = sums[1, rows, :] + up + jnp.where(group == 1, plane[2, at, :], 0.0)
        scale = 1.0 / (diag_i * diag_o - up * up)
        inverse[0, rows, :] = diag_o * scale
        inverse[1, rows, :] = diag_i * scale
        inverse[2, rows, :] = up * scale
        return carry

    lax.fori_loop(0, half // STEP, fill, 0, unroll=2)


def tree(parts):
    values = [parts[k] for k in range(parts.shape[0])]
    while len(values) > 1:
        values = [a + b for a, b in zip(values[::2], values[1::2])]
    return values[0]


def relay_kernel(parts, spread):
    total = tree(parts)
    for k in range(spread.shape[0]):
        spread[k] = total


def solve(parts):
    sums = tree(parts)
    g = [jnp.broadcast_to(sums[:, k : k + 1], (1, LANES)) for k in range(6)]
    step = [g[k] - g[k + 1] for k in range(5)]
    scale = [lax.rsqrt(g[0]), lax.rsqrt(g[2]), lax.rsqrt(g[4])]

    def entry(i, j):
        return step[i + j] * scale[i] * scale[j]

    d0 = entry(0, 0)
    l10, l20 = entry(1, 0) / d0, entry(2, 0) / d0
    d1 = entry(1, 1) - l10 * entry(1, 0)
    e21 = entry(2, 1) - l20 * entry(1, 0)
    l21 = e21 / d1
    d2 = entry(2, 2) - l20 * entry(2, 0) - l21 * e21
    y0 = g[0] * scale[0]
    y1 = g[1] * scale[1] - l10 * y0
    y2 = g[2] * scale[2] - l20 * y0 - l21 * y1
    x2 = y2 / d2
    x1 = y1 / d1 - l21 * x2
    x0 = y0 / d0 - l10 * x1 - l20 * x2
    c0, c1, c2 = x0 * scale[0], x1 * scale[1], x2 * scale[2]
    good = (d0 > GUARD) & (d1 > GUARD) & (d2 > GUARD)
    return (c0, c1, c2, 1.0 - c0, c0 - c1, c1 - c2), good


def combine_kernel(gz, far_0, parts, current, inv_near, inv_far, n_0, n_12, n_12_far, volts, left, flag, volts_here, left_here, n_0_far, sems):
    group = gz[0]
    half, n_cols = n_0.shape[1:]
    bring = pltpu.make_async_copy(far_0, n_0_far, sems.at[4])
    bring.start()
    values, good = solve(parts)
    flag[...] = jnp.where(good, 1, 0)
    c = [jnp.broadcast_to(value[:, 0:1], (STEP, n_cols)) for value in values]

    def fill(part, inv, first, second):
        def body(k, carry):
            rows, at = block(k), block(k + part * (half // STEP))
            drawn = jnp.where(group == 0, current[at, :], 0.0)
            n0i, n0o = first[0, rows, :], first[1, rows, :]
            n1i, n1o, n2i, n2o = [second[j, rows, :] for j in range(4)]
            ii, oo, io = [inv[e, rows, :] for e in range(3)]
            one = c[1] * n0i + c[2] * n1i
            two = c[0] * drawn + (c[1] * n0o + c[2] * n1o)
            volts_here[1 - group, at, :] = ii * one + io * two
            volts_here[group, at, :] = io * one + oo * two
            left_here[1 - group, at, :] = c[4] * n0i + c[5] * n1i + c[2] * n2i
            left_here[group, at, :] = c[3] * drawn + c[4] * n0o + c[5] * n1o + c[2] * n2o
            return carry

        lax.fori_loop(0, half // STEP, body, 0, unroll=6)

    copies = []

    def put_out(part, first_sem):
        rows = pl.ds(pl.multiple_of(part * half, STEP), half)
        for j, (source, target) in enumerate(((volts_here, volts), (left_here, left))):
            copy = pltpu.make_async_copy(
                source.at[:, rows, :], target.at[:, rows, :], sems.at[first_sem + j]
            )
            copy.start()
            copies.append(copy)

    fill(group, inv_near, n_0, n_12)
    put_out(group, 0)
    bring.wait()
    fill(1 - group, inv_far, n_0_far, n_12_far)
    put_out(1 - group, 2)
    for copy in copies:
        copy.wait()


def call(kernel, outs, scratch, n_smem, *args, outside=0, far=0):
    return pl.pallas_call(
        kernel,
        in_specs=[SMEM] * n_smem + [OUTSIDE] * far + [VMEM] * (len(args) - n_smem - far),
        out_specs=[OUTSIDE] * outside + [VMEM] * (len(outs) - outside),
        out_shape=outs,
        scratch_shapes=scratch,
        compiler_params=pltpu.CompilerParams(vmem_limit_bytes=GRANT),
    )(*args)


def shards(load_current, sink_mask, pad_mask, plane_class, via_class, plane_table, via_table):
    _, n_rows, n_cols = plane_class.shape
    half, frame = n_rows // 2, n_rows // 2 + 2 * STEP
    tall = -(-(n_rows + 2 * STEP) // LANES) * LANES
    broad = n_cols + LANES

    def array(*shape):
        return jax.ShapeDtypeStruct(shape, jnp.float32)

    def ring(axis):
        size = lax.axis_size(axis)
        return [(i, (i + 1) % size) for i in range(size)]

    def back(pairs):
        return [(b, a) for a, b in pairs]

    turn = [pltpu.VMEM((LANES, tall), jnp.float32), pltpu.VMEM((tall, LANES), jnp.float32)]
    gz = lax.axis_index("gz").reshape(1).astype(jnp.int32)
    swap = [(0, 1), (1, 0)]
    rest = ("gy_0", "gy_1", "gz")
    n_gx, n_rest = lax.axis_size(GX), lax.axis_size(rest)

    via, one, via_send = call(
        via_kernel,
        [array(2, n_rows, n_cols), array(half, n_cols), array(half, n_cols)],
        [], 1, gz, via_table, via_class,
    )
    big_via = lax.ppermute(one, "gz", swap)
    plane, drawn, three, top, bottom = call(
        plane_kernel,
        [array(3, n_rows, n_cols), array(n_rows, n_cols), array(3, half, n_cols)]
        + [array(DEEP * N_OWN, n_cols)] * 2,
        [], 1, gz, plane_table, plane_class, load_current, sink_mask, pad_mask, via,
    )
    south = lax.ppermute(bottom, GY, ring(GY))
    north = lax.ppermute(top, GY, back(ring(GY)))
    big_plane = lax.ppermute(three, "gz", swap)
    first, last = call(
        columns_kernel, [array(DEEP * N_OWN, tall)] * 2, turn[1:], 0,
        plane, via, drawn, south, north,
    )
    west = lax.ppermute(last, GX, ring(GX))
    east = lax.ppermute(first, GX, back(ring(GX)))
    (small_send,) = call(
        corner_kernel, [array(N_FAR * 3 * DEEP, n_cols)], [], 1,
        gz, plane, via, south, north, west, east,
    )
    small = lax.ppermute(small_send, "gz", swap)
    via_far = lax.ppermute(via_send, "gz", swap)
    near, near_e, near_n, near_sum, far_sum = call(
        own_kernel,
        [array(4, frame, broad)] + [array(2, frame, broad)] * 3 + [array(2, half, n_cols)],
        [pltpu.VMEM((2, n_rows + 2 * STEP, broad), jnp.float32)] + turn,
        1, gz, plane, via, drawn, south, north, west, east,
    )
    far_e, far_n, cross, inverse, step_1, n_0, inv_near, send, part = call(
        edge_kernel,
        [array(2, frame, broad)] * 2
        + [array(frame, broad), array(6, frame, broad), array(4, frame, broad),
           array(2, half, n_cols), array(3, half, n_cols), array(2, half, n_cols), array(STEP, LANES)],
        [pltpu.VMEM((N_FAR, frame, broad), jnp.float32), pltpu.VMEM((2, frame, broad), jnp.float32)]
        + turn,
        1, gz, near, near_e, near_n, near_sum, big_plane, big_via, small,
    )
    n_0_far = lax.ppermute(send, "gz", swap)
    (inv_far,) = call(
        inverse_kernel, [array(3, half, n_cols)], [], 1,
        gz, plane, via, far_sum, via_far,
    )
    n_12, send, spread = call(
        steps_kernel,
        [array(4, half, n_cols), array(4, half, n_cols), array(n_gx, 1, LANES)],
        [pltpu.VMEM((4, frame, broad), jnp.float32)],
        0, step_1, near_e, near_n, far_e, far_n, cross, inverse, part,
    )
    n_12_far = lax.ppermute(send, "gz", swap)
    parts = lax.all_to_all(spread, GX, 0, 0, tiled=True)
    (spread,) = call(relay_kernel, [array(n_rest, 1, LANES)], [], 0, parts)
    parts = lax.all_to_all(spread, rest, 0, 0, tiled=True)
    volts, left, flag = call(
        combine_kernel,
        [array(2, n_rows, n_cols)] * 2 + [jax.ShapeDtypeStruct((1, LANES), jnp.int32)],
        [pltpu.VMEM((2, n_rows, n_cols), jnp.float32)] * 2
        + [pltpu.VMEM((2, half, n_cols), jnp.float32), pltpu.SemaphoreType.DMA((5,))],
        1, gz, n_0_far, parts, drawn, inv_near, inv_far, n_0, n_12, n_12_far, outside=2, far=1,
    )

    def careful():
        return recurrence(
            load_current, sink_mask, pad_mask, plane_class, via_class, plane_table, via_table
        )

    return lax.cond(flag[0, 0] == 1, lambda: (volts, left), careful)


def solution(mesh):
    split = Mesh(
        mesh.devices.reshape(8, 2, 2, 4, mesh.shape["gz"]), ("gx_0", "gx_1", "gy_0", "gy_1", "gz")
    )
    placed = (
        P(GY, GX),
        P(GY, GX),
        P(GY, GX),
        P("gz", GY, GX),
        P("gz", GY, GX),
        P("gz", None),
        P("gz", None),
    )
    return jax.shard_map(
        shards,
        mesh=split,
        in_specs=placed,
        out_specs=(P("gz", GY, GX), P("gz", GY, GX)),
        check_vma=False,
    )
```

```python
import jax
import jax.numpy as jnp
from jax import lax
from jax.experimental import pallas as pl
from jax.experimental.pallas import tpu as pltpu
from jax.sharding import Mesh
from jax.sharding import PartitionSpec as P

ITERS = 3
GX = ("gx_0", "gx_1")
GY = ("gy_0", "gy_1")
GX_GY_GZ = ("gx_0", "gx_1", "gy_0", "gy_1", "gz")


PAD_CONDUCTANCE = 20.0


def padded(array, sides, width):
    edges = {}
    for axis, dim in sides:
        peers, length = (lax.axis_size(axis), array.shape[dim])
        up = [(i, (i + 1) % peers) for i in range(peers)]
        last = lax.slice_in_dim(array, length - width, length, axis=dim)
        leading = lax.slice_in_dim(array, 0, width, axis=dim)
        edges[dim] = (
            lax.ppermute(last, axis, up),
            lax.ppermute(leading, axis, [(b, a) for a, b in up]),
        )
    done = []
    for _, dim in sides:
        low, high = edges[dim]
        around = [(width, width) if d in done else (0, 0) for d in range(array.ndim)]
        array = jnp.concatenate([jnp.pad(low, around), array, jnp.pad(high, around)], axis=dim)
        done.append(dim)
    return array


def padded_2(block, sides, width):
    for axis, dim in sides:
        count = lax.axis_size(axis)
        forward = [(i, i + 1) for i in range(count - 1)]
        backward = [(target, source) for source, target in forward]
        low = lax.ppermute(
            lax.slice_in_dim(block, block.shape[dim] - width, None, axis=dim), axis, forward
        )
        high = lax.ppermute(lax.slice_in_dim(block, 0, width, axis=dim), axis, backward)
        block = jnp.concatenate([low, block, high], axis=dim)
    return block


def by_axis(array, axes):
    for axis in axes:
        array = lax.psum(array, axis)
    return array


def lookup(classes, table):
    summed = jnp.zeros(classes.shape, jnp.float32)
    for level in range(table.shape[1]):
        summed = summed + jnp.where(
            classes == level, table[:, level][:, None, None], jnp.float32(0.0)
        )
    return summed


def harmonic(first, second):
    return 2.0 * first * second / (first + second)


def factor(diagonal, up_edge):
    inverses = []
    factors = []
    for level in range(diagonal.shape[0]):
        pivots = diagonal[level]
        if level > 0:
            pivots = pivots + up_edge[level - 1] * factors[level - 1]
        inverse = 1.0 / pivots
        inverses.append(inverse)
        factors.append(-up_edge[level] * inverse)
    return (jnp.stack(inverses), jnp.stack(factors))


def solve_block(inverses, factors, up_edge, source_term):
    forward = []
    for level in range(source_term.shape[0]):
        entries = source_term[level]
        if level > 0:
            entries = entries + up_edge[level - 1] * forward[level - 1]
        forward.append(entries * inverses[level])
    result = [forward[-1]]
    level = 0
    result.insert(0, forward[level] - factors[level] * result[0])
    return jnp.stack(result)


def plane_extend(field):
    return padded(field, ((GX, 2), (GY, 1)), 1)


def layer_extend(field):
    return padded_2(field, (("gz", 0),), 1)


def merged_sums(residual, precond, image_field):
    return (
        by_axis(jnp.sum(residual * precond), GX_GY_GZ),
        by_axis(jnp.sum(image_field * precond), GX_GY_GZ),
    )


def recurrence(load_current, sink_mask, pad_mask, plane_class, via_class, plane_table, via_table):
    n_layers, n_rows, n_cols = plane_class.shape
    g_plane = lookup(plane_class, plane_table)
    g_via = lookup(via_class, via_table)
    plane_ext = plane_extend(g_plane)
    middle = plane_ext[:, 1:-1, :]
    across = harmonic(middle[:, :, :-1], middle[:, :, 1:])
    east_edge = across[:, :, 1:]
    west_edge = across[:, :, :-1]
    column = plane_ext[:, :, 1:-1]
    along_rows = harmonic(column[:, :-1], column[:, 1:])
    north_edge = along_rows[:, 1:]
    south_edge = along_rows[:, :-1]
    via_ext = layer_extend(g_via)
    vertical = harmonic(via_ext[:-1], via_ext[1:])
    up_edge = vertical[1:]
    down_edge = vertical[:-1]
    group_index = lax.axis_index("gz")
    is_top = group_index == lax.axis_size("gz") - 1
    is_bottom = group_index == 0
    pad_plane = jnp.where(is_top, PAD_CONDUCTANCE * pad_mask.astype(jnp.float32), jnp.float32(0.0))
    pad_layer = jnp.concatenate(
        [jnp.zeros((n_layers - 1, n_rows, n_cols), jnp.float32), pad_plane[None]], 0
    )
    diagonal = east_edge + west_edge + north_edge + south_edge + up_edge + down_edge + pad_layer
    inverses, factors = factor(diagonal, up_edge)

    def precondition(residual):
        return solve_block(inverses, factors, up_edge, residual)

    def operate(field):
        inner = plane_extend(field)
        layer_ext = layer_extend(field)
        above_field = layer_ext[2:]
        below_field = layer_ext[:-2]
        return (
            diagonal * field
            - east_edge * inner[:, 1:-1, 2:]
            - west_edge * inner[:, 1:-1, :-2]
            - north_edge * inner[:, 2:, 1:-1]
            - south_edge * inner[:, :-2, 1:-1]
            - up_edge * above_field
            - down_edge * below_field
        )

    source = jnp.where(is_bottom, sink_mask.astype(jnp.float32) * load_current, jnp.float32(0.0))
    right_side = jnp.concatenate(
        [source[None], jnp.zeros((n_layers - 1, n_rows, n_cols), jnp.float32)], 0
    )
    voltage = jnp.zeros((n_layers, n_rows, n_cols), jnp.float32)
    residual = right_side
    precond = precondition(residual)
    image_field = operate(precond)
    weight_now, curvature = merged_sums(residual, precond, image_field)
    step_size = weight_now / curvature
    direction = precond
    image_dir = image_field
    for iteration in range(ITERS):
        voltage = voltage + step_size * direction
        residual = residual - step_size * image_dir
        if iteration + 1 < ITERS:
            precond = precondition(residual)
            image_field = operate(precond)
            weight_next, curvature = merged_sums(residual, precond, image_field)
            momentum = weight_next / weight_now
            step_size = weight_next / (curvature - momentum * weight_next / step_size)
            direction = precond + momentum * direction
            image_dir = image_field + momentum * image_dir
            weight_now = weight_next
    return (voltage, residual)


STEP = 8
LANES = 128
DEEP = 4
GUARD = 0.02
GRANT = 16 * 1024 * 1024
N_OWN = 6
N_FAR = 4
VMEM = pl.BlockSpec(memory_space=pltpu.VMEM)
SMEM = pl.BlockSpec(memory_space=pltpu.SMEM)
OUTSIDE = pl.BlockSpec(memory_space=pl.ANY)


def block(k):
    return pl.ds(pl.multiple_of(k * STEP, STEP), STEP)


def mean(first, second):
    return 1.0 / (first + second)


def half_reciprocals(table, layer, n_cols):
    row = 0.5 / table[pl.ds(layer, 1), :]
    return [jnp.broadcast_to(row[:, e : e + 1], (STEP, n_cols)) for e in range(row.shape[1])]


def look_up(entries, classes):
    low = (classes & 1) != 0
    mid = (classes & 2) != 0
    pairs = [jnp.where(low, entries[2 * k + 1], entries[2 * k]) for k in range(4)]
    return jnp.where(
        classes > 3, jnp.where(mid, pairs[3], pairs[2]), jnp.where(mid, pairs[1], pairs[0])
    )


def via_kernel(gz, table, classes, via, first, lone):
    group = gz[0]
    n_rows, n_cols = via.shape[1:]
    half = n_rows // 2 // STEP
    of_i, of_o = [half_reciprocals(table, layer, n_cols) for layer in (1 - group, group)]

    def fill(k, carry):
        rows = block(k)
        one = look_up(of_i, classes[1 - group, rows, :])
        two = look_up(of_o, classes[group, rows, :])
        via[0, rows, :] = one
        via[1, rows, :] = mean(one, two)
        return carry

    lax.fori_loop(0, n_rows // STEP, fill, 0, unroll=8)

    head = first.shape[0] // STEP - half
    for k in range(half):
        first[k * STEP : k * STEP + STEP, :] = via[0, block(k + (1 - group) * half), :]
        lone[k * STEP : k * STEP + STEP, :] = via[0, block(k + group * half), :]
    for k in range(head):
        rows = pl.ds((half + k) * STEP, STEP)
        first[rows, :] = via[1, block(k + (1 - group) * half), :]


def plane_kernel(gz, table, classes, load, sink, pad, via, plane, drawn, three, top, bottom):
    group = gz[0]
    n_rows, n_cols = plane.shape[1:]
    half = n_rows // 2 // STEP
    of_i, of_o = [half_reciprocals(table, layer, n_cols) for layer in (1 - group, group)]

    def fill(k, carry):
        rows = block(k)
        plane[0, rows, :] = look_up(of_i, classes[1 - group, rows, :])
        plane[1, rows, :] = look_up(of_o, classes[group, rows, :])
        plane[2, rows, :] = PAD_CONDUCTANCE * pad[rows, :].astype(jnp.float32)
        drawn[rows, :] = sink[rows, :].astype(jnp.float32) * load[rows, :]
        return carry

    lax.fori_loop(0, n_rows // STEP, fill, 0, unroll=8)

    head = 3 * half - three.shape[0] // STEP
    for k in range(half):
        rows = block(k + (1 - group) * half)
        for f in range(2):
            three[pl.ds((f * half + k) * STEP, STEP), :] = plane[f, rows, :]
        if k >= head:
            three[pl.ds((2 * half + k - head) * STEP, STEP), :] = via[1, rows, :]
    for f in range(N_OWN):
        at = pl.ds(DEEP * f, DEEP)
        top[at, :] = field_rows(plane, via, drawn, f, pl.ds(0, DEEP))
        bottom[at, :] = field_rows(plane, via, drawn, f, pl.ds(n_rows - DEEP, DEEP))


def field_rows(plane, via, drawn, f, rows):
    if f == 4:
        return drawn[rows, :]
    if f in (2, 3):
        return via[f - 2, rows, :]
    return plane[2 if f == 5 else f, rows, :]


def tile_of(stack, f, upper):
    rows = stack[f // 2 * STEP : f // 2 * STEP + STEP, :]
    return rows if (f % 2 == 1) == upper else pltpu.roll(rows, DEEP, 0)


def columns_kernel(plane, via, drawn, south, north, first, last, stage):
    n_rows, n_cols = drawn.shape
    lane = lax.broadcasted_iota(jnp.int32, (STEP, LANES), 1)
    place = lane // DEEP

    def put(rows, pick):
        out = jnp.zeros((STEP, LANES), jnp.float32)
        for f in range(N_OWN):
            value = pick(f)
            head, tail = value[:, :LANES], value[:, n_cols - LANES :]
            if f:
                head = pltpu.roll(head, DEEP * f, 1)
            tail = pltpu.roll(tail, DEEP * (N_OWN + f + 1), 1)
            out = jnp.where(place == f, head, jnp.where(place == N_OWN + f, tail, out))
        stage[rows, :] = out

    def inner(k, carry):
        put(block(k + 1), lambda f: field_rows(plane, via, drawn, f, block(k)))
        return carry

    put(pl.ds(0, STEP), lambda f: tile_of(south, f, True))
    lax.fori_loop(0, n_rows // STEP, inner, 0, unroll=8)
    put(pl.ds(n_rows + STEP, STEP), lambda f: tile_of(north, f, False))
    rest = n_rows + 2 * STEP
    stage[rest:, :] = jnp.zeros((stage.shape[0] - rest, LANES), jnp.float32)
    turned = stage[...].T
    size = DEEP * N_OWN
    first[...] = turned[:size, :]
    last[...] = turned[size : 2 * size, :]


def side(strip, slot, blank):
    lane = lax.broadcasted_iota(jnp.int32, strip.shape, 1)
    turned = pltpu.roll(strip, (LANES - DEEP - 2 * DEEP * slot) % LANES, 1)
    return jnp.where((lane < DEEP) | (lane >= LANES - DEEP), turned, blank)


def corner_kernel(gz, plane, via, south, north, west, east, small):
    group = gz[0]
    half, tall_rows = plane.shape[1] // 2, west.shape[1]
    for f in range(N_FAR):
        at, mine = 2 * DEEP * f, pl.ds(DEEP * f, DEEP)
        inner = field_rows(plane, via, None, f, pl.ds(half - DEEP, DEEP))
        small[at : at + DEEP, :] = jnp.where(group == 0, inner, south[mine, :])
        inner = field_rows(plane, via, None, f, pl.ds(half, DEEP))
        small[at + DEEP : at + 2 * DEEP, :] = jnp.where(group == 0, north[mine, :], inner)
    at, size = 2 * DEEP * N_FAR, DEEP * N_FAR
    small[at : at + size, :tall_rows] = west[:size, :]
    small[at : at + size, tall_rows:] = east[:size, :]


def eastward(value):
    return pltpu.roll(value, value.shape[1] - 1, 1)


def westward(value):
    return pltpu.roll(value, 1, 1)


def rows_up(value):
    return pltpu.roll(value, STEP - 1, 0)


def rows_down(value):
    return pltpu.roll(value, 1, 0)


def joined(edge, inner, outer):
    sub = lax.broadcasted_iota(jnp.int32, inner.shape, 0)
    return jnp.where(sub == edge, outer, inner)


def own_kernel(gz, plane, via, drawn, south, north, west, east, near, edge_e, edge_n, near_sum, far_sum, wide, flat, tall):
    group = gz[0]
    n_rows, n_cols = drawn.shape
    half, last = n_rows // 2 // STEP, n_rows // STEP + 1
    flat[...] = jnp.zeros(flat.shape, jnp.float32)
    for f in range(N_OWN):
        at = 2 * DEEP * f
        flat[at : at + DEEP, :] = west[DEEP * f : DEEP * f + DEEP, :]
        flat[at + DEEP : at + 2 * DEEP, :] = east[DEEP * f : DEEP * f + DEEP, :]
    tall[...] = flat[...].T

    def put(rows, pick):
        strip = tall[rows, :]
        for f in range(2):
            wide[f, rows, :n_cols] = pick(f)
            wide[f, rows, n_cols:] = side(strip, f, 1.0)

    def inner(k, carry):
        put(block(k + 1), lambda f: plane[f, block(k), :])
        return carry

    put(pl.ds(0, STEP), lambda f: tile_of(south, f, True))
    lax.fori_loop(0, n_rows // STEP, inner, 0, unroll=8)
    put(pl.ds(n_rows + STEP, STEP), lambda f: tile_of(north, f, False))

    def around(layer, k):
        value = wide[layer, block(k), :]
        over = wide[layer, block(jnp.minimum(k + 1, last)), :]
        under = wide[layer, block(jnp.maximum(k - 1, 0)), :]
        above = joined(STEP - 1, rows_up(value), rows_up(over))
        below = joined(0, rows_down(value), rows_down(under))
        to_east, to_north = mean(value, eastward(value)), mean(value, above)
        return to_east, to_north, (to_east + westward(to_east)) + (to_north + mean(value, below))

    def frame(k, carry):
        at = k + group * half
        for layer in range(2):
            to_east, to_north, total = around(layer, at)
            edge_e[layer, block(k), :] = to_east
            edge_n[layer, block(k), :] = to_north
            near_sum[layer, block(k), :] = total
        strip = tall[block(at), :]
        inside = block(jnp.clip(at - 1, 0, last - 2))
        for place, f in enumerate((2, 3, 4, 5)):
            core = field_rows(plane, via, drawn, f, inside)
            core = jnp.where(at == 0, tile_of(south, f, True), core)
            core = jnp.where(at == last, tile_of(north, f, False), core)
            near[place, block(k), :n_cols] = core
            near[place, block(k), n_cols:] = side(strip, f, 1.0 if f < N_FAR else 0.0)
        return carry

    lax.fori_loop(0, half + 2, frame, 0, unroll=7)

    def other(k, carry):
        for layer in range(2):
            total = around(layer, k + 1 + (1 - group) * half)[2]
            far_sum[layer, block(k), :] = total[:, :n_cols]
        return carry

    lax.fori_loop(0, half, other, 0, unroll=6)


def fold(total):
    width = total.shape[1]
    while width > LANES:
        width //= 2
        total = total[:, :width] + total[:, width:]
    return jnp.sum(total, axis=0, keepdims=True)


PAIRS = ((0, 0, 2), (1, 2, 0))


def image_pass(field, edges, cross, blocks, done, pairs=PAIRS):
    last = field.shape[1] // STEP - 1

    def at(k):
        return pl.ds(k * STEP, STEP)

    for q, base, facing in pairs:
        east, north = edges[q]
        ups, downs = {}, {}

        def up(layer, k):
            if (layer, k) not in ups:
                ups[layer, k] = rows_up(field[base + layer, at(k), :])
            return ups[layer, k]

        def down(layer, k):
            if (layer, k) not in downs:
                flux = north[layer, at(k), :] * field[base + layer, at(k), :]
                downs[layer, k] = rows_down(flux)
            return downs[layer, k]

        for k in blocks:
            owns, outs = [], []
            for layer in range(2):
                own, edge = field[base + layer, at(k), :], east[layer, at(k), :]
                above = joined(STEP - 1, up(layer, k), up(layer, min(k + 1, last)))
                below = joined(0, down(layer, k), down(layer, max(k - 1, 0)))
                across = edge * eastward(own) + westward(edge * own)
                owns.append(own)
                outs.append(across + (north[layer, at(k), :] * above + below))
            if facing is not None:
                outs[0] = outs[0] + cross[at(k), :] * field[facing, at(k), :]
            done(q, k, owns, outs)


def solved(inverse, q, k, outs):
    ii, oo, io = [inverse[3 * q + e, pl.ds(k * STEP, STEP), :] for e in range(3)]
    return [ii * outs[0] + io * outs[1], io * outs[0] + oo * outs[1]]


def dot(left, right, n_cols):
    return (left[0] * right[0] + left[1] * right[1])[:, :n_cols]


def image_step(field, edges, cross, inverse, stepped, keep, n_cols):
    n_blocks = field.shape[1] // STEP
    sums = [jnp.zeros((STEP, n_cols), jnp.float32)] * 2

    def done(q, k, owns, outs):
        news = solved(inverse, q, k, outs)
        for layer in range(2):
            stepped[2 * q + layer, pl.ds(k * STEP, STEP), :] = news[layer]
        if 0 < k < n_blocks - 1:
            for layer in range(2):
                keep[q][layer, pl.ds((k - 1) * STEP, STEP), :] = outs[layer][:, :n_cols]
            sums[0] = sums[0] + dot(owns, outs, n_cols)
            sums[1] = sums[1] + dot(news, outs, n_cols)

    image_pass(field, edges, cross, range(n_blocks), done)
    return sums


def edge_kernel(gz, near, near_e, near_n, near_sum, three, first, small, far_e, far_n, cross, inverse, step_1, n_own, inv_own, send, part, *scratch):
    fields, step_0, flat, tall = scratch
    group = gz[0]
    n_cols = first.shape[1]
    half = (first.shape[0] + three.shape[0]) // N_FAR
    head = first.shape[0] - half
    n_blocks = half // STEP + 2
    tall_rows = tall.shape[0]
    flat[...] = jnp.zeros(flat.shape, jnp.float32)
    for f in range(N_FAR):
        at, row = 2 * DEEP * f, 2 * DEEP * N_FAR + DEEP * f
        flat[at : at + DEEP, :] = small[row : row + DEEP, :tall_rows]
        flat[at + DEEP : at + 2 * DEEP, :] = small[row : row + DEEP, tall_rows:]
    tall[...] = flat[...].T
    for k in range(n_blocks):
        rows = pl.ds(k * STEP, STEP)
        strip = tall[block(k + group * (half // STEP)), :]
        for f in range(N_FAR):
            if 0 < k < n_blocks - 1:
                r = (k - 1) * STEP
                stack, r = {
                    0: (three, r),
                    1: (three, half + r),
                    2: (first, r),
                    3: (first, half + r) if r < head else (three, 2 * half + r - head),
                }[f]
                core = stack[r : r + STEP, :]
            else:
                core = pltpu.roll(small[2 * DEEP * f : 2 * DEEP * f + STEP, :], DEEP, 0)
            fields[f, rows, :n_cols] = core
            fields[f, rows, n_cols:] = side(strip, f, 1.0)
    total = jnp.zeros((STEP, n_cols), jnp.float32)
    ups, downs = {}, {}

    def up(layer, k):
        if (layer, k) not in ups:
            ups[layer, k] = rows_up(fields[layer, k * STEP : k * STEP + STEP, :])
        return ups[layer, k]

    for k in range(n_blocks):
        rows = pl.ds(k * STEP, STEP)
        sums = [near_sum[0, rows, :], near_sum[1, rows, :]]
        for layer in range(2):
            value = fields[layer, rows, :]
            above = joined(STEP - 1, up(layer, k), up(layer, min(k + 1, n_blocks - 1)))
            to_east, to_north = mean(value, eastward(value)), mean(value, above)
            far_e[layer, rows, :] = to_east
            far_n[layer, rows, :] = to_north
            downs[layer, k] = rows_down(to_north)
            carried = joined(0, downs[layer, k], downs[layer, max(k - 1, 0)])
            sums.append((to_east + westward(to_east)) + (to_north + carried))
        link = mean(near[0, rows, :], fields[2, rows, :])
        cross[rows, :] = link
        drawn, pads = near[2, rows, :], near[3, rows, :]
        inner = pl.ds((k - 1) * STEP, STEP)
        both = []
        for q, up_edge in ((0, near[1, rows, :]), (1, fields[3, rows, :])):
            diag_i = sums[2 * q] + up_edge + link
            diag_o = sums[2 * q + 1] + up_edge + jnp.where(group == 1 - q, pads, 0.0)
            scale = 1.0 / (diag_i * diag_o - up_edge * up_edge)
            found = (diag_o * scale, diag_i * scale, up_edge * scale)
            for e in range(3):
                inverse[3 * q + e, rows, :] = found[e]
                if q == 0 and 0 < k < n_blocks - 1:
                    inv_own[e, inner, :] = found[e][:, :n_cols]
            both.append(found)
        one = jnp.where(group == 0, both[0][2], both[1][2]) * drawn
        two = jnp.where(group == 0, both[0][1], both[1][1]) * drawn
        step_0[0, rows, :], step_0[1, rows, :] = one, two
        if 0 < k < n_blocks - 1:
            total = total + (two * drawn)[:, :n_cols]
    part[...] = jnp.zeros(part.shape, jnp.float32)
    part[0:1, :] = fold(total)
    edges, keep = ((near_e, near_n), (far_e, far_n)), (n_own, send)
    for q in range(2):

        @pl.when(group == q)
        def _(q=q):
            first_step(q, step_0, edges, cross, inverse, step_1, keep, part)


def first_step(q, step_0, edges, cross, inverse, step_1, keep, part):
    n_cols = keep[0].shape[2]
    n_blocks, p = step_0.shape[1] // STEP, 1 - q
    sums = [jnp.zeros((STEP, n_cols), jnp.float32)] * 2

    def done(_, k, owns, outs):
        rows = pl.ds(k * STEP, STEP)
        news = solved(inverse, q, k, outs)
        over = cross[rows, :] * owns[0]
        facing = inverse[3 * p, rows, :] * over
        for layer in range(2):
            step_1[2 * q + layer, rows, :] = news[layer]
        step_1[2 * p, rows, :] = facing
        step_1[2 * p + 1, rows, :] = inverse[3 * p + 2, rows, :] * over
        if 0 < k < n_blocks - 1:
            inner = pl.ds((k - 1) * STEP, STEP)
            for layer in range(2):
                keep[q][layer, inner, :] = outs[layer][:, :n_cols]
            keep[p][0, inner, :] = over[:, :n_cols]
            keep[p][1, inner, :] = jnp.zeros((STEP, n_cols), jnp.float32)
            sums[0] = sums[0] + dot(owns, outs, n_cols)
            sums[1] = sums[1] + (dot(news, outs, n_cols) + (facing * over)[:, :n_cols])

    image_pass(step_0, edges, cross, range(n_blocks), done, ((q, 0, None),))
    part[1:2, :] = fold(sums[0])
    part[2:3, :] = fold(sums[1])


def steps_kernel(step_1, near_e, near_n, far_e, far_n, cross, inverse, before, n_own, send, spread, step_2):
    n_cols = n_own.shape[2]
    edges = ((near_e, near_n), (far_e, far_n))
    first, second = pl.ds(0, 2), pl.ds(2, 2)
    sums = image_step(
        step_1, edges, cross, inverse, step_2, (n_own.at[first], send.at[first]), n_cols
    )
    keep = (n_own.at[second], send.at[second])
    sums.append(jnp.zeros((STEP, n_cols), jnp.float32))

    def done(q, k, owns, outs):
        for layer in range(2):
            keep[q][layer, pl.ds((k - 1) * STEP, STEP), :] = outs[layer][:, :n_cols]
        sums[2] = sums[2] + dot(owns, outs, n_cols)

    image_pass(step_2, edges, cross, range(1, step_1.shape[1] // STEP - 1), done)
    row = lax.broadcasted_iota(jnp.int32, before.shape, 0)
    part = before[...]
    for j in range(3):
        part = jnp.where(row == 3 + j, fold(sums[j]), part)
    sums = jnp.sum(part, axis=1, keepdims=True)
    lane = lax.broadcasted_iota(jnp.int32, part.shape, 1)
    line = jnp.sum(jnp.where(lane == row, sums, 0.0), axis=0, keepdims=True)
    for k in range(spread.shape[0]):
        spread[k] = line


def inverse_kernel(gz, plane, via, sums, given, inverse):
    group = gz[0]
    half = inverse.shape[1]

    def fill(k, carry):
        rows, at = block(k), block(k + (1 - group) * (half // STEP))
        up = via[1, at, :]
        diag_i = sums[0, rows, :] + up + mean(via[0, at, :], given[rows, :])
        diag_o = sums[1, rows, :] + up + jnp.where(group == 1, plane[2, at, :], 0.0)
        scale = 1.0 / (diag_i * diag_o - up * up)
        inverse[0, rows, :] = diag_o * scale
        inverse[1, rows, :] = diag_i * scale
        inverse[2, rows, :] = up * scale
        return carry

    lax.fori_loop(0, half // STEP, fill, 0, unroll=2)


def tree(parts):
    values = [parts[k] for k in range(parts.shape[0])]
    while len(values) > 1:
        values = [a + b for a, b in zip(values[::2], values[1::2])]
    return values[0]


def relay_kernel(parts, spread):
    total = tree(parts)
    for k in range(spread.shape[0]):
        spread[k] = total


def solve(parts):
    sums = tree(parts)
    g = [jnp.broadcast_to(sums[:, k : k + 1], (1, LANES)) for k in range(6)]
    step = [g[k] - g[k + 1] for k in range(5)]
    scale = [lax.rsqrt(g[0]), lax.rsqrt(g[2]), lax.rsqrt(g[4])]

    def entry(i, j):
        return step[i + j] * scale[i] * scale[j]

    d0 = entry(0, 0)
    l10, l20 = entry(1, 0) / d0, entry(2, 0) / d0
    d1 = entry(1, 1) - l10 * entry(1, 0)
    e21 = entry(2, 1) - l20 * entry(1, 0)
    l21 = e21 / d1
    d2 = entry(2, 2) - l20 * entry(2, 0) - l21 * e21
    y0 = g[0] * scale[0]
    y1 = g[1] * scale[1] - l10 * y0
    y2 = g[2] * scale[2] - l20 * y0 - l21 * y1
    x2 = y2 / d2
    x1 = y1 / d1 - l21 * x2
    x0 = y0 / d0 - l10 * x1 - l20 * x2
    c0, c1, c2 = x0 * scale[0], x1 * scale[1], x2 * scale[2]
    good = (d0 > GUARD) & (d1 > GUARD) & (d2 > GUARD)
    return (c0, c1, c2, 1.0 - c0, c0 - c1, c1 - c2), good


def combine_kernel(gz, far_0, parts, current, inv_near, inv_far, n_0, n_12, n_12_far, volts, left, flag, volts_here, left_here, n_0_far, sems):
    group = gz[0]
    half, n_cols = n_0.shape[1:]
    bring = pltpu.make_async_copy(far_0, n_0_far, sems.at[4])
    bring.start()
    values, good = solve(parts)
    flag[...] = jnp.where(good, 1, 0)
    c = [jnp.broadcast_to(value[:, 0:1], (STEP, n_cols)) for value in values]

    def fill(part, inv, first, second):
        def body(k, carry):
            rows, at = block(k), block(k + part * (half // STEP))
            drawn = jnp.where(group == 0, current[at, :], 0.0)
            n0i, n0o = first[0, rows, :], first[1, rows, :]
            n1i, n1o, n2i, n2o = [second[j, rows, :] for j in range(4)]
            ii, oo, io = [inv[e, rows, :] for e in range(3)]
            one = c[1] * n0i + c[2] * n1i
            two = c[0] * drawn + (c[1] * n0o + c[2] * n1o)
            volts_here[1 - group, at, :] = ii * one + io * two
            volts_here[group, at, :] = io * one + oo * two
            left_here[1 - group, at, :] = c[4] * n0i + c[5] * n1i + c[2] * n2i
            left_here[group, at, :] = c[3] * drawn + c[4] * n0o + c[5] * n1o + c[2] * n2o
            return carry

        lax.fori_loop(0, half // STEP, body, 0, unroll=6)

    copies = []

    def put_out(part, first_sem):
        rows = pl.ds(pl.multiple_of(part * half, STEP), half)
        for j, (source, target) in enumerate(((volts_here, volts), (left_here, left))):
            copy = pltpu.make_async_copy(
                source.at[:, rows, :], target.at[:, rows, :], sems.at[first_sem + j]
            )
            copy.start()
            copies.append(copy)

    fill(group, inv_near, n_0, n_12)
    put_out(group, 0)
    bring.wait()
    fill(1 - group, inv_far, n_0_far, n_12_far)
    put_out(1 - group, 2)
    for copy in copies:
        copy.wait()


def call(kernel, outs, scratch, n_smem, *args, outside=0, far=0):
    return pl.pallas_call(
        kernel,
        in_specs=[SMEM] * n_smem + [OUTSIDE] * far + [VMEM] * (len(args) - n_smem - far),
        out_specs=[OUTSIDE] * outside + [VMEM] * (len(outs) - outside),
        out_shape=outs,
        scratch_shapes=scratch,
        compiler_params=pltpu.CompilerParams(vmem_limit_bytes=GRANT),
    )(*args)


def shards(load_current, sink_mask, pad_mask, plane_class, via_class, plane_table, via_table):
    _, n_rows, n_cols = plane_class.shape
    half, frame = n_rows // 2, n_rows // 2 + 2 * STEP
    tall = -(-(n_rows + 2 * STEP) // LANES) * LANES
    broad = n_cols + LANES
    head = half * 6 // 12

    def array(*shape):
        return jax.ShapeDtypeStruct(shape, jnp.float32)

    def ring(axis):
        size = lax.axis_size(axis)
        return [(i, (i + 1) % size) for i in range(size)]

    def back(pairs):
        return [(b, a) for a, b in pairs]

    turn = [pltpu.VMEM((LANES, tall), jnp.float32), pltpu.VMEM((tall, LANES), jnp.float32)]
    gz = lax.axis_index("gz").reshape(1).astype(jnp.int32)
    swap = [(0, 1), (1, 0)]
    rest = ("gy_0", "gy_1", "gz")
    n_gx, n_rest = lax.axis_size(GX), lax.axis_size(rest)

    via, one, via_send = call(
        via_kernel,
        [array(2, n_rows, n_cols), array(half + head, n_cols), array(half, n_cols)],
        [], 1, gz, via_table, via_class,
    )
    big_via = lax.ppermute(one, "gz", swap)
    plane, drawn, three, top, bottom = call(
        plane_kernel,
        [array(3, n_rows, n_cols), array(n_rows, n_cols), array(3 * half - head, n_cols)]
        + [array(DEEP * N_OWN, n_cols)] * 2,
        [], 1, gz, plane_table, plane_class, load_current, sink_mask, pad_mask, via,
    )
    south = lax.ppermute(bottom, GY, ring(GY))
    north = lax.ppermute(top, GY, back(ring(GY)))
    big_plane = lax.ppermute(three, "gz", swap)
    first, last = call(
        columns_kernel, [array(DEEP * N_OWN, tall)] * 2, turn[1:], 0,
        plane, via, drawn, south, north,
    )
    west = lax.ppermute(last, GX, ring(GX))
    east = lax.ppermute(first, GX, back(ring(GX)))
    (small_send,) = call(
        corner_kernel, [array(N_FAR * 3 * DEEP, n_cols)], [], 1,
        gz, plane, via, south, north, west, east,
    )
    small = lax.ppermute(small_send, "gz", swap)
    via_far = lax.ppermute(via_send, "gz", swap)
    near, near_e, near_n, near_sum, far_sum = call(
        own_kernel,
        [array(4, frame, broad)] + [array(2, frame, broad)] * 3 + [array(2, half, n_cols)],
        [pltpu.VMEM((2, n_rows + 2 * STEP, broad), jnp.float32)] + turn,
        1, gz, plane, via, drawn, south, north, west, east,
    )
    far_e, far_n, cross, inverse, step_1, n_0, inv_near, send, part = call(
        edge_kernel,
        [array(2, frame, broad)] * 2
        + [array(frame, broad), array(6, frame, broad), array(4, frame, broad),
           array(2, half, n_cols), array(3, half, n_cols), array(2, half, n_cols), array(STEP, LANES)],
        [pltpu.VMEM((N_FAR, frame, broad), jnp.float32), pltpu.VMEM((2, frame, broad), jnp.float32)]
        + turn,
        1, gz, near, near_e, near_n, near_sum, big_plane, big_via, small,
    )
    n_0_far = lax.ppermute(send, "gz", swap)
    (inv_far,) = call(
        inverse_kernel, [array(3, half, n_cols)], [], 1,
        gz, plane, via, far_sum, via_far,
    )
    n_12, send, spread = call(
        steps_kernel,
        [array(4, half, n_cols), array(4, half, n_cols), array(n_gx, 1, LANES)],
        [pltpu.VMEM((4, frame, broad), jnp.float32)],
        0, step_1, near_e, near_n, far_e, far_n, cross, inverse, part,
    )
    n_12_far = lax.ppermute(send, "gz", swap)
    parts = lax.all_to_all(spread, GX, 0, 0, tiled=True)
    (spread,) = call(relay_kernel, [array(n_rest, 1, LANES)], [], 0, parts)
    parts = lax.all_to_all(spread, rest, 0, 0, tiled=True)
    volts, left, flag = call(
        combine_kernel,
        [array(2, n_rows, n_cols)] * 2 + [jax.ShapeDtypeStruct((1, LANES), jnp.int32)],
        [pltpu.VMEM((2, n_rows, n_cols), jnp.float32)] * 2
        + [pltpu.VMEM((2, half, n_cols), jnp.float32), pltpu.SemaphoreType.DMA((5,))],
        1, gz, n_0_far, parts, drawn, inv_near, inv_far, n_0, n_12, n_12_far, outside=2, far=1,
    )

    def careful():
        return recurrence(
            load_current, sink_mask, pad_mask, plane_class, via_class, plane_table, via_table
        )

    return lax.cond(flag[0, 0] == 1, lambda: (volts, left), careful)


def solution(mesh):
    split = Mesh(
        mesh.devices.reshape(8, 2, 2, 4, mesh.shape["gz"]), ("gx_0", "gx_1", "gy_0", "gy_1", "gz")
    )
    placed = (
        P(GY, GX),
        P(GY, GX),
        P(GY, GX),
        P("gz", GY, GX),
        P("gz", GY, GX),
        P("gz", None),
        P("gz", None),
    )
    return jax.shard_map(
        shards,
        mesh=split,
        in_specs=placed,
        out_specs=(P("gz", GY, GX), P("gz", GY, GX)),
        check_vma=False,
    )
```

```python
import jax
import jax.numpy as jnp
from jax import lax
from jax.experimental import pallas as pl
from jax.experimental.pallas import tpu as pltpu
from jax.sharding import Mesh
from jax.sharding import PartitionSpec as P

ITERS = 3
GX = ("gx_0", "gx_1")
GY = ("gy_0", "gy_1")
GX_GY_GZ = ("gx_0", "gx_1", "gy_0", "gy_1", "gz")


PAD_CONDUCTANCE = 20.0


def padded(array, sides, width):
    edges = {}
    for axis, dim in sides:
        peers, length = (lax.axis_size(axis), array.shape[dim])
        up = [(i, (i + 1) % peers) for i in range(peers)]
        last = lax.slice_in_dim(array, length - width, length, axis=dim)
        leading = lax.slice_in_dim(array, 0, width, axis=dim)
        edges[dim] = (
            lax.ppermute(last, axis, up),
            lax.ppermute(leading, axis, [(b, a) for a, b in up]),
        )
    done = []
    for _, dim in sides:
        low, high = edges[dim]
        around = [(width, width) if d in done else (0, 0) for d in range(array.ndim)]
        array = jnp.concatenate([jnp.pad(low, around), array, jnp.pad(high, around)], axis=dim)
        done.append(dim)
    return array


def padded_2(block, sides, width):
    for axis, dim in sides:
        count = lax.axis_size(axis)
        forward = [(i, i + 1) for i in range(count - 1)]
        backward = [(target, source) for source, target in forward]
        low = lax.ppermute(
            lax.slice_in_dim(block, block.shape[dim] - width, None, axis=dim), axis, forward
        )
        high = lax.ppermute(lax.slice_in_dim(block, 0, width, axis=dim), axis, backward)
        block = jnp.concatenate([low, block, high], axis=dim)
    return block


def by_axis(array, axes):
    for axis in axes:
        array = lax.psum(array, axis)
    return array


def lookup(classes, table):
    summed = jnp.zeros(classes.shape, jnp.float32)
    for level in range(table.shape[1]):
        summed = summed + jnp.where(
            classes == level, table[:, level][:, None, None], jnp.float32(0.0)
        )
    return summed


def harmonic(first, second):
    return 2.0 * first * second / (first + second)


def factor(diagonal, up_edge):
    inverses = []
    factors = []
    for level in range(diagonal.shape[0]):
        pivots = diagonal[level]
        if level > 0:
            pivots = pivots + up_edge[level - 1] * factors[level - 1]
        inverse = 1.0 / pivots
        inverses.append(inverse)
        factors.append(-up_edge[level] * inverse)
    return (jnp.stack(inverses), jnp.stack(factors))


def solve_block(inverses, factors, up_edge, source_term):
    forward = []
    for level in range(source_term.shape[0]):
        entries = source_term[level]
        if level > 0:
            entries = entries + up_edge[level - 1] * forward[level - 1]
        forward.append(entries * inverses[level])
    result = [forward[-1]]
    level = 0
    result.insert(0, forward[level] - factors[level] * result[0])
    return jnp.stack(result)


def plane_extend(field):
    return padded(field, ((GX, 2), (GY, 1)), 1)


def layer_extend(field):
    return padded_2(field, (("gz", 0),), 1)


def merged_sums(residual, precond, image_field):
    return (
        by_axis(jnp.sum(residual * precond), GX_GY_GZ),
        by_axis(jnp.sum(image_field * precond), GX_GY_GZ),
    )


def recurrence(load_current, sink_mask, pad_mask, plane_class, via_class, plane_table, via_table):
    n_layers, n_rows, n_cols = plane_class.shape
    g_plane = lookup(plane_class, plane_table)
    g_via = lookup(via_class, via_table)
    plane_ext = plane_extend(g_plane)
    middle = plane_ext[:, 1:-1, :]
    across = harmonic(middle[:, :, :-1], middle[:, :, 1:])
    east_edge = across[:, :, 1:]
    west_edge = across[:, :, :-1]
    column = plane_ext[:, :, 1:-1]
    along_rows = harmonic(column[:, :-1], column[:, 1:])
    north_edge = along_rows[:, 1:]
    south_edge = along_rows[:, :-1]
    via_ext = layer_extend(g_via)
    vertical = harmonic(via_ext[:-1], via_ext[1:])
    up_edge = vertical[1:]
    down_edge = vertical[:-1]
    group_index = lax.axis_index("gz")
    is_top = group_index == lax.axis_size("gz") - 1
    is_bottom = group_index == 0
    pad_plane = jnp.where(is_top, PAD_CONDUCTANCE * pad_mask.astype(jnp.float32), jnp.float32(0.0))
    pad_layer = jnp.concatenate(
        [jnp.zeros((n_layers - 1, n_rows, n_cols), jnp.float32), pad_plane[None]], 0
    )
    diagonal = east_edge + west_edge + north_edge + south_edge + up_edge + down_edge + pad_layer
    inverses, factors = factor(diagonal, up_edge)

    def precondition(residual):
        return solve_block(inverses, factors, up_edge, residual)

    def operate(field):
        inner = plane_extend(field)
        layer_ext = layer_extend(field)
        above_field = layer_ext[2:]
        below_field = layer_ext[:-2]
        return (
            diagonal * field
            - east_edge * inner[:, 1:-1, 2:]
            - west_edge * inner[:, 1:-1, :-2]
            - north_edge * inner[:, 2:, 1:-1]
            - south_edge * inner[:, :-2, 1:-1]
            - up_edge * above_field
            - down_edge * below_field
        )

    source = jnp.where(is_bottom, sink_mask.astype(jnp.float32) * load_current, jnp.float32(0.0))
    right_side = jnp.concatenate(
        [source[None], jnp.zeros((n_layers - 1, n_rows, n_cols), jnp.float32)], 0
    )
    voltage = jnp.zeros((n_layers, n_rows, n_cols), jnp.float32)
    residual = right_side
    precond = precondition(residual)
    image_field = operate(precond)
    weight_now, curvature = merged_sums(residual, precond, image_field)
    step_size = weight_now / curvature
    direction = precond
    image_dir = image_field
    for iteration in range(ITERS):
        voltage = voltage + step_size * direction
        residual = residual - step_size * image_dir
        if iteration + 1 < ITERS:
            precond = precondition(residual)
            image_field = operate(precond)
            weight_next, curvature = merged_sums(residual, precond, image_field)
            momentum = weight_next / weight_now
            step_size = weight_next / (curvature - momentum * weight_next / step_size)
            direction = precond + momentum * direction
            image_dir = image_field + momentum * image_dir
            weight_now = weight_next
    return (voltage, residual)


STEP = 8
LANES = 128
DEEP = 4
GUARD = 0.02
GRANT = 16 * 1024 * 1024
N_OWN = 6
N_FAR = 4
VMEM = pl.BlockSpec(memory_space=pltpu.VMEM)
SMEM = pl.BlockSpec(memory_space=pltpu.SMEM)
OUTSIDE = pl.BlockSpec(memory_space=pl.ANY)


def block(k):
    return pl.ds(pl.multiple_of(k * STEP, STEP), STEP)


def mean(first, second):
    return 1.0 / (first + second)


def half_reciprocals(table, layer, n_cols):
    row = 0.5 / table[pl.ds(layer, 1), :]
    return [jnp.broadcast_to(row[:, e : e + 1], (STEP, n_cols)) for e in range(row.shape[1])]


def look_up(entries, classes):
    low = (classes & 1) != 0
    mid = (classes & 2) != 0
    pairs = [jnp.where(low, entries[2 * k + 1], entries[2 * k]) for k in range(4)]
    return jnp.where(
        classes > 3, jnp.where(mid, pairs[3], pairs[2]), jnp.where(mid, pairs[1], pairs[0])
    )


def via_kernel(gz, table, classes, via, first, lone):
    group = gz[0]
    n_rows, n_cols = via.shape[1:]
    half = n_rows // 2 // STEP
    of_i, of_o = [half_reciprocals(table, layer, n_cols) for layer in (1 - group, group)]

    def fill(k, carry):
        rows = block(k)
        one = look_up(of_i, classes[1 - group, rows, :])
        two = look_up(of_o, classes[group, rows, :])
        via[0, rows, :] = one
        via[1, rows, :] = mean(one, two)
        return carry

    lax.fori_loop(0, n_rows // STEP, fill, 0, unroll=8)

    head = first.shape[0] // STEP - half
    for k in range(half):
        first[k * STEP : k * STEP + STEP, :] = via[0, block(k + (1 - group) * half), :]
        lone[k * STEP : k * STEP + STEP, :] = via[0, block(k + group * half), :]
    for k in range(head):
        rows = pl.ds((half + k) * STEP, STEP)
        first[rows, :] = via[1, block(k + (1 - group) * half), :]


def plane_kernel(gz, table, classes, load, sink, pad, via, plane, drawn, three, top, bottom):
    group = gz[0]
    n_rows, n_cols = plane.shape[1:]
    half = n_rows // 2 // STEP
    of_i, of_o = [half_reciprocals(table, layer, n_cols) for layer in (1 - group, group)]

    def fill(k, carry):
        rows = block(k)
        plane[0, rows, :] = look_up(of_i, classes[1 - group, rows, :])
        plane[1, rows, :] = look_up(of_o, classes[group, rows, :])
        plane[2, rows, :] = PAD_CONDUCTANCE * pad[rows, :].astype(jnp.float32)
        drawn[rows, :] = sink[rows, :].astype(jnp.float32) * load[rows, :]
        return carry

    lax.fori_loop(0, n_rows // STEP, fill, 0, unroll=8)

    head = 3 * half - three.shape[0] // STEP
    for k in range(half):
        rows = block(k + (1 - group) * half)
        for f in range(2):
            three[pl.ds((f * half + k) * STEP, STEP), :] = plane[f, rows, :]
        if k >= head:
            three[pl.ds((2 * half + k - head) * STEP, STEP), :] = via[1, rows, :]
    for f in range(N_OWN):
        at = pl.ds(DEEP * f, DEEP)
        top[at, :] = field_rows(plane, via, drawn, f, pl.ds(0, DEEP))
        bottom[at, :] = field_rows(plane, via, drawn, f, pl.ds(n_rows - DEEP, DEEP))


def field_rows(plane, via, drawn, f, rows):
    if f == 4:
        return drawn[rows, :]
    if f in (2, 3):
        return via[f - 2, rows, :]
    return plane[2 if f == 5 else f, rows, :]


def tile_of(stack, f, upper):
    rows = stack[f // 2 * STEP : f // 2 * STEP + STEP, :]
    return rows if (f % 2 == 1) == upper else pltpu.roll(rows, DEEP, 0)


def columns_kernel(plane, via, drawn, south, north, first, last, stage):
    n_rows, n_cols = drawn.shape
    lane = lax.broadcasted_iota(jnp.int32, (STEP, LANES), 1)
    place = lane // DEEP

    def put(rows, pick):
        out = jnp.zeros((STEP, LANES), jnp.float32)
        for f in range(N_OWN):
            value = pick(f)
            head, tail = value[:, :LANES], value[:, n_cols - LANES :]
            if f:
                head = pltpu.roll(head, DEEP * f, 1)
            tail = pltpu.roll(tail, DEEP * (N_OWN + f + 1), 1)
            out = jnp.where(place == f, head, jnp.where(place == N_OWN + f, tail, out))
        stage[rows, :] = out

    def inner(k, carry):
        put(block(k + 1), lambda f: field_rows(plane, via, drawn, f, block(k)))
        return carry

    put(pl.ds(0, STEP), lambda f: tile_of(south, f, True))
    lax.fori_loop(0, n_rows // STEP, inner, 0, unroll=8)
    put(pl.ds(n_rows + STEP, STEP), lambda f: tile_of(north, f, False))
    rest = n_rows + 2 * STEP
    stage[rest:, :] = jnp.zeros((stage.shape[0] - rest, LANES), jnp.float32)
    turned = stage[...].T
    size = DEEP * N_OWN
    first[...] = turned[:size, :]
    last[...] = turned[size : 2 * size, :]


def side(strip, slot, blank):
    lane = lax.broadcasted_iota(jnp.int32, strip.shape, 1)
    turned = pltpu.roll(strip, (LANES - DEEP - 2 * DEEP * slot) % LANES, 1)
    return jnp.where((lane < DEEP) | (lane >= LANES - DEEP), turned, blank)


def corner_kernel(gz, plane, via, south, north, west, east, small):
    group = gz[0]
    half, tall_rows = plane.shape[1] // 2, west.shape[1]
    for f in range(N_FAR):
        at, mine = 2 * DEEP * f, pl.ds(DEEP * f, DEEP)
        inner = field_rows(plane, via, None, f, pl.ds(half - DEEP, DEEP))
        small[at : at + DEEP, :] = jnp.where(group == 0, inner, south[mine, :])
        inner = field_rows(plane, via, None, f, pl.ds(half, DEEP))
        small[at + DEEP : at + 2 * DEEP, :] = jnp.where(group == 0, north[mine, :], inner)
    at, size = 2 * DEEP * N_FAR, DEEP * N_FAR
    small[at : at + size, :tall_rows] = west[:size, :]
    small[at : at + size, tall_rows:] = east[:size, :]


def eastward(value):
    return pltpu.roll(value, value.shape[1] - 1, 1)


def westward(value):
    return pltpu.roll(value, 1, 1)


def rows_up(value):
    return pltpu.roll(value, STEP - 1, 0)


def rows_down(value):
    return pltpu.roll(value, 1, 0)


def joined(edge, inner, outer):
    sub = lax.broadcasted_iota(jnp.int32, inner.shape, 0)
    return jnp.where(sub == edge, outer, inner)


def own_kernel(gz, plane, via, drawn, south, north, west, east, near, edge_e, edge_n, near_sum, far_sum, wide, flat, tall):
    group = gz[0]
    n_rows, n_cols = drawn.shape
    half, last = n_rows // 2 // STEP, n_rows // STEP + 1
    flat[...] = jnp.zeros(flat.shape, jnp.float32)
    for f in range(N_OWN):
        at = 2 * DEEP * f
        flat[at : at + DEEP, :] = west[DEEP * f : DEEP * f + DEEP, :]
        flat[at + DEEP : at + 2 * DEEP, :] = east[DEEP * f : DEEP * f + DEEP, :]
    tall[...] = flat[...].T

    def put(rows, pick):
        strip = tall[rows, :]
        for f in range(2):
            wide[f, rows, :n_cols] = pick(f)
            wide[f, rows, n_cols:] = side(strip, f, 1.0)

    def inner(k, carry):
        put(block(k + 1), lambda f: plane[f, block(k), :])
        return carry

    put(pl.ds(0, STEP), lambda f: tile_of(south, f, True))
    lax.fori_loop(0, n_rows // STEP, inner, 0, unroll=8)
    put(pl.ds(n_rows + STEP, STEP), lambda f: tile_of(north, f, False))

    def around(layer, k):
        value = wide[layer, block(k), :]
        over = wide[layer, block(jnp.minimum(k + 1, last)), :]
        under = wide[layer, block(jnp.maximum(k - 1, 0)), :]
        above = joined(STEP - 1, rows_up(value), rows_up(over))
        below = joined(0, rows_down(value), rows_down(under))
        to_east, to_north = mean(value, eastward(value)), mean(value, above)
        return to_east, to_north, (to_east + westward(to_east)) + (to_north + mean(value, below))

    def frame(k, carry):
        at = k + group * half
        for layer in range(2):
            to_east, to_north, total = around(layer, at)
            edge_e[layer, block(k), :] = to_east
            edge_n[layer, block(k), :] = to_north
            near_sum[layer, block(k), :] = total
        strip = tall[block(at), :]
        inside = block(jnp.clip(at - 1, 0, last - 2))
        for place, f in enumerate((2, 3, 4, 5)):
            core = field_rows(plane, via, drawn, f, inside)
            core = jnp.where(at == 0, tile_of(south, f, True), core)
            core = jnp.where(at == last, tile_of(north, f, False), core)
            near[place, block(k), :n_cols] = core
            near[place, block(k), n_cols:] = side(strip, f, 1.0 if f < N_FAR else 0.0)
        return carry

    lax.fori_loop(0, half + 2, frame, 0, unroll=7)

    def other(k, carry):
        for layer in range(2):
            total = around(layer, k + 1 + (1 - group) * half)[2]
            far_sum[layer, block(k), :] = total[:, :n_cols]
        return carry

    lax.fori_loop(0, half, other, 0, unroll=6)


def fold(total):
    width = total.shape[1]
    while width > LANES:
        width //= 2
        total = total[:, :width] + total[:, width:]
    return jnp.sum(total, axis=0, keepdims=True)


PAIRS = ((1, 2, 0), (0, 0, 2))


def image_pass(field, edges, cross, blocks, done, pairs=PAIRS):
    last = field.shape[1] // STEP - 1

    def at(k):
        return pl.ds(k * STEP, STEP)

    for q, base, facing in pairs:
        east, north = edges[q]
        ups, downs = {}, {}

        def up(layer, k):
            if (layer, k) not in ups:
                ups[layer, k] = rows_up(field[base + layer, at(k), :])
            return ups[layer, k]

        def down(layer, k):
            if (layer, k) not in downs:
                flux = north[layer, at(k), :] * field[base + layer, at(k), :]
                downs[layer, k] = rows_down(flux)
            return downs[layer, k]

        for k in blocks:
            owns, outs = [], []
            for layer in range(2):
                own, edge = field[base + layer, at(k), :], east[layer, at(k), :]
                above = joined(STEP - 1, up(layer, k), up(layer, min(k + 1, last)))
                below = joined(0, down(layer, k), down(layer, max(k - 1, 0)))
                across = edge * eastward(own) + westward(edge * own)
                owns.append(own)
                outs.append(across + (north[layer, at(k), :] * above + below))
            if facing is not None:
                outs[0] = outs[0] + cross[at(k), :] * field[facing, at(k), :]
            done(q, k, owns, outs)


def solved(inverse, q, k, outs):
    ii, oo, io = [inverse[3 * q + e, pl.ds(k * STEP, STEP), :] for e in range(3)]
    return [ii * outs[0] + io * outs[1], io * outs[0] + oo * outs[1]]


def dot(left, right, n_cols):
    return (left[0] * right[0] + left[1] * right[1])[:, :n_cols]


def image_step(field, edges, cross, inverse, stepped, keep, n_cols):
    n_blocks = field.shape[1] // STEP
    sums = [jnp.zeros((STEP, n_cols), jnp.float32)] * 2

    def done(q, k, owns, outs):
        news = solved(inverse, q, k, outs)
        for layer in range(2):
            stepped[2 * q + layer, pl.ds(k * STEP, STEP), :] = news[layer]
        if 0 < k < n_blocks - 1:
            for layer in range(2):
                keep[q][layer, pl.ds((k - 1) * STEP, STEP), :] = outs[layer][:, :n_cols]
            sums[0] = sums[0] + dot(owns, outs, n_cols)
            sums[1] = sums[1] + dot(news, outs, n_cols)

    image_pass(field, edges, cross, range(n_blocks), done)
    return sums


def edge_kernel(gz, near, near_e, near_n, near_sum, three, first, small, out, far_e, far_n, cross, inverse, step_1, n_own, inv_own, part, *scratch):
    fields, step_0, flat, tall, send, sems = scratch
    group = gz[0]
    n_cols = first.shape[1]
    half = (first.shape[0] + three.shape[0]) // N_FAR
    head = first.shape[0] - half
    n_blocks = half // STEP + 2
    tall_rows = tall.shape[0]
    flat[...] = jnp.zeros(flat.shape, jnp.float32)
    for f in range(N_FAR):
        at, row = 2 * DEEP * f, 2 * DEEP * N_FAR + DEEP * f
        flat[at : at + DEEP, :] = small[row : row + DEEP, :tall_rows]
        flat[at + DEEP : at + 2 * DEEP, :] = small[row : row + DEEP, tall_rows:]
    tall[...] = flat[...].T
    for k in range(n_blocks):
        rows = pl.ds(k * STEP, STEP)
        strip = tall[block(k + group * (half // STEP)), :]
        for f in range(N_FAR):
            if 0 < k < n_blocks - 1:
                r = (k - 1) * STEP
                stack, r = {
                    0: (three, r),
                    1: (three, half + r),
                    2: (first, r),
                    3: (first, half + r) if r < head else (three, 2 * half + r - head),
                }[f]
                core = stack[r : r + STEP, :]
            else:
                core = pltpu.roll(small[2 * DEEP * f : 2 * DEEP * f + STEP, :], DEEP, 0)
            fields[f, rows, :n_cols] = core
            fields[f, rows, n_cols:] = side(strip, f, 1.0)
    total = jnp.zeros((STEP, n_cols), jnp.float32)
    ups, downs = {}, {}

    def up(layer, k):
        if (layer, k) not in ups:
            ups[layer, k] = rows_up(fields[layer, k * STEP : k * STEP + STEP, :])
        return ups[layer, k]

    for k in range(n_blocks):
        rows = pl.ds(k * STEP, STEP)
        sums = [near_sum[0, rows, :], near_sum[1, rows, :]]
        for layer in range(2):
            value = fields[layer, rows, :]
            above = joined(STEP - 1, up(layer, k), up(layer, min(k + 1, n_blocks - 1)))
            to_east, to_north = mean(value, eastward(value)), mean(value, above)
            far_e[layer, rows, :] = to_east
            far_n[layer, rows, :] = to_north
            downs[layer, k] = rows_down(to_north)
            carried = joined(0, downs[layer, k], downs[layer, max(k - 1, 0)])
            sums.append((to_east + westward(to_east)) + (to_north + carried))
        link = mean(near[0, rows, :], fields[2, rows, :])
        cross[rows, :] = link
        drawn, pads = near[2, rows, :], near[3, rows, :]
        inner = pl.ds((k - 1) * STEP, STEP)
        both = []
        for q, up_edge in ((0, near[1, rows, :]), (1, fields[3, rows, :])):
            diag_i = sums[2 * q] + up_edge + link
            diag_o = sums[2 * q + 1] + up_edge + jnp.where(group == 1 - q, pads, 0.0)
            scale = 1.0 / (diag_i * diag_o - up_edge * up_edge)
            found = (diag_o * scale, diag_i * scale, up_edge * scale)
            for e in range(3):
                inverse[3 * q + e, rows, :] = found[e]
                if q == 0 and 0 < k < n_blocks - 1:
                    inv_own[e, inner, :] = found[e][:, :n_cols]
            both.append(found)
        one = jnp.where(group == 0, both[0][2], both[1][2]) * drawn
        two = jnp.where(group == 0, both[0][1], both[1][1]) * drawn
        step_0[0, rows, :], step_0[1, rows, :] = one, two
        if 0 < k < n_blocks - 1:
            total = total + (two * drawn)[:, :n_cols]
    part[...] = jnp.zeros(part.shape, jnp.float32)
    part[0:1, :] = fold(total)
    edges, keep = ((near_e, near_n), (far_e, far_n)), (n_own, send)
    copies = []
    for piece in range(2):
        blocks = range(piece * n_blocks // 2, (piece + 1) * n_blocks // 2)
        for q in range(2):

            @pl.when(group == q)
            def _(q=q, blocks=blocks):
                first_step(q, blocks, step_0, edges, cross, inverse, step_1, keep, part)

        rows = pl.ds(piece * (half // 2), half // 2)
        copy = pltpu.make_async_copy(send.at[:, rows, :], out.at[:, rows, :], sems.at[piece])
        copy.start()
        copies.append(copy)
    for copy in copies:
        copy.wait()


def first_step(q, blocks, step_0, edges, cross, inverse, step_1, keep, part):
    n_cols = keep[0].shape[2]
    n_blocks, p = step_0.shape[1] // STEP, 1 - q
    sums = [jnp.zeros((STEP, n_cols), jnp.float32)] * 2

    def done(_, k, owns, outs):
        rows = pl.ds(k * STEP, STEP)
        news = solved(inverse, q, k, outs)
        over = cross[rows, :] * owns[0]
        facing = inverse[3 * p, rows, :] * over
        for layer in range(2):
            step_1[2 * q + layer, rows, :] = news[layer]
        step_1[2 * p, rows, :] = facing
        step_1[2 * p + 1, rows, :] = inverse[3 * p + 2, rows, :] * over
        if 0 < k < n_blocks - 1:
            inner = pl.ds((k - 1) * STEP, STEP)
            for layer in range(2):
                keep[q][layer, inner, :] = outs[layer][:, :n_cols]
            keep[p][0, inner, :] = over[:, :n_cols]
            keep[p][1, inner, :] = jnp.zeros((STEP, n_cols), jnp.float32)
            sums[0] = sums[0] + dot(owns, outs, n_cols)
            sums[1] = sums[1] + (dot(news, outs, n_cols) + (facing * over)[:, :n_cols])

    image_pass(step_0, edges, cross, blocks, done, ((q, 0, None),))
    part[1:2, :] = part[1:2, :] + fold(sums[0])
    part[2:3, :] = part[2:3, :] + fold(sums[1])


def steps_kernel(step_1, near_e, near_n, far_e, far_n, cross, inverse, before, out, n_own, spread, step_2, send, sems):
    n_cols = n_own.shape[2]
    edges = ((near_e, near_n), (far_e, far_n))
    first, second = pl.ds(0, 2), pl.ds(2, 2)
    copies = [
        pltpu.make_async_copy(send.at[part], out.at[part], sems.at[j])
        for j, part in enumerate((first, second))
    ]
    last = step_1.shape[1] // STEP - 2
    sums = image_step(
        step_1, edges, cross, inverse, step_2, (n_own.at[first], send.at[first]), n_cols
    )
    copies[0].start()
    keep = (n_own.at[second], send.at[second])
    sums.append(jnp.zeros((STEP, n_cols), jnp.float32))

    def done(q, k, owns, outs):
        for layer in range(2):
            keep[q][layer, pl.ds((k - 1) * STEP, STEP), :] = outs[layer][:, :n_cols]
        sums[2] = sums[2] + dot(owns, outs, n_cols)
        if q == 1 and k == last:
            copies[1].start()

    image_pass(step_2, edges, cross, range(1, last + 1), done)
    row = lax.broadcasted_iota(jnp.int32, before.shape, 0)
    part = before[...]
    for j in range(3):
        part = jnp.where(row == 3 + j, fold(sums[j]), part)
    sums = jnp.sum(part, axis=1, keepdims=True)
    lane = lax.broadcasted_iota(jnp.int32, part.shape, 1)
    line = jnp.sum(jnp.where(lane == row, sums, 0.0), axis=0, keepdims=True)
    for k in range(spread.shape[0]):
        spread[k] = line
    for copy in copies:
        copy.wait()


def inverse_kernel(gz, plane, via, sums, given, inverse):
    group = gz[0]
    half = inverse.shape[1]

    def fill(k, carry):
        rows, at = block(k), block(k + (1 - group) * (half // STEP))
        up = via[1, at, :]
        diag_i = sums[0, rows, :] + up + mean(via[0, at, :], given[rows, :])
        diag_o = sums[1, rows, :] + up + jnp.where(group == 1, plane[2, at, :], 0.0)
        scale = 1.0 / (diag_i * diag_o - up * up)
        inverse[0, rows, :] = diag_o * scale
        inverse[1, rows, :] = diag_i * scale
        inverse[2, rows, :] = up * scale
        return carry

    lax.fori_loop(0, half // STEP, fill, 0, unroll=2)


def tree(parts):
    values = [parts[k] for k in range(parts.shape[0])]
    while len(values) > 1:
        values = [a + b for a, b in zip(values[::2], values[1::2])]
    return values[0]


def relay_kernel(parts, spread):
    total = tree(parts)
    for k in range(spread.shape[0]):
        spread[k] = total


def solve(parts):
    sums = tree(parts)
    g = [jnp.broadcast_to(sums[:, k : k + 1], (1, LANES)) for k in range(6)]
    step = [g[k] - g[k + 1] for k in range(5)]
    scale = [lax.rsqrt(g[0]), lax.rsqrt(g[2]), lax.rsqrt(g[4])]

    def entry(i, j):
        return step[i + j] * scale[i] * scale[j]

    d0 = entry(0, 0)
    l10, l20 = entry(1, 0) / d0, entry(2, 0) / d0
    d1 = entry(1, 1) - l10 * entry(1, 0)
    e21 = entry(2, 1) - l20 * entry(1, 0)
    l21 = e21 / d1
    d2 = entry(2, 2) - l20 * entry(2, 0) - l21 * e21
    y0 = g[0] * scale[0]
    y1 = g[1] * scale[1] - l10 * y0
    y2 = g[2] * scale[2] - l20 * y0 - l21 * y1
    x2 = y2 / d2
    x1 = y1 / d1 - l21 * x2
    x0 = y0 / d0 - l10 * x1 - l20 * x2
    c0, c1, c2 = x0 * scale[0], x1 * scale[1], x2 * scale[2]
    good = (d0 > GUARD) & (d1 > GUARD) & (d2 > GUARD)
    return (c0, c1, c2, 1.0 - c0, c0 - c1, c1 - c2), good


def combine_kernel(gz, far_0, parts, current, inv_near, inv_far, n_0, n_12, n_12_far, volts, left, flag, volts_here, left_here, n_0_far, sems):
    group = gz[0]
    half, n_cols = n_0.shape[1:]
    bring = pltpu.make_async_copy(far_0, n_0_far, sems.at[4])
    bring.start()
    values, good = solve(parts)
    flag[...] = jnp.where(good, 1, 0)
    c = [jnp.broadcast_to(value[:, 0:1], (STEP, n_cols)) for value in values]

    def fill(part, inv, first, second):
        def body(k, carry):
            rows, at = block(k), block(k + part * (half // STEP))
            drawn = jnp.where(group == 0, current[at, :], 0.0)
            n0i, n0o = first[0, rows, :], first[1, rows, :]
            n1i, n1o, n2i, n2o = [second[j, rows, :] for j in range(4)]
            ii, oo, io = [inv[e, rows, :] for e in range(3)]
            one = c[1] * n0i + c[2] * n1i
            two = c[0] * drawn + (c[1] * n0o + c[2] * n1o)
            volts_here[1 - group, at, :] = ii * one + io * two
            volts_here[group, at, :] = io * one + oo * two
            left_here[1 - group, at, :] = c[4] * n0i + c[5] * n1i + c[2] * n2i
            left_here[group, at, :] = c[3] * drawn + c[4] * n0o + c[5] * n1o + c[2] * n2o
            return carry

        lax.fori_loop(0, half // STEP, body, 0, unroll=6)

    copies = []

    def put_out(part, first_sem):
        rows = pl.ds(pl.multiple_of(part * half, STEP), half)
        for j, (source, target) in enumerate(((volts_here, volts), (left_here, left))):
            copy = pltpu.make_async_copy(
                source.at[:, rows, :], target.at[:, rows, :], sems.at[first_sem + j]
            )
            copy.start()
            copies.append(copy)

    fill(group, inv_near, n_0, n_12)
    put_out(group, 0)
    bring.wait()
    fill(1 - group, inv_far, n_0_far, n_12_far)
    put_out(1 - group, 2)
    for copy in copies:
        copy.wait()


def call(kernel, outs, scratch, n_smem, *args, outside=0, far=0):
    return pl.pallas_call(
        kernel,
        in_specs=[SMEM] * n_smem + [OUTSIDE] * far + [VMEM] * (len(args) - n_smem - far),
        out_specs=[OUTSIDE] * outside + [VMEM] * (len(outs) - outside),
        out_shape=outs,
        scratch_shapes=scratch,
        compiler_params=pltpu.CompilerParams(vmem_limit_bytes=GRANT),
    )(*args)


def shards(load_current, sink_mask, pad_mask, plane_class, via_class, plane_table, via_table):
    _, n_rows, n_cols = plane_class.shape
    half, frame = n_rows // 2, n_rows // 2 + 2 * STEP
    tall = -(-(n_rows + 2 * STEP) // LANES) * LANES
    broad = n_cols + LANES
    head = half * 4 // 12

    def array(*shape):
        return jax.ShapeDtypeStruct(shape, jnp.float32)

    def ring(axis):
        size = lax.axis_size(axis)
        return [(i, (i + 1) % size) for i in range(size)]

    def back(pairs):
        return [(b, a) for a, b in pairs]

    turn = [pltpu.VMEM((LANES, tall), jnp.float32), pltpu.VMEM((tall, LANES), jnp.float32)]
    gz = lax.axis_index("gz").reshape(1).astype(jnp.int32)
    swap = [(0, 1), (1, 0)]
    rest = ("gy_0", "gy_1", "gz")
    n_gx, n_rest = lax.axis_size(GX), lax.axis_size(rest)

    via, one, via_send = call(
        via_kernel,
        [array(2, n_rows, n_cols), array(half + head, n_cols), array(half, n_cols)],
        [], 1, gz, via_table, via_class,
    )
    big_via = lax.ppermute(one, "gz", swap)
    plane, drawn, three, top, bottom = call(
        plane_kernel,
        [array(3, n_rows, n_cols), array(n_rows, n_cols), array(3 * half - head, n_cols)]
        + [array(DEEP * N_OWN, n_cols)] * 2,
        [], 1, gz, plane_table, plane_class, load_current, sink_mask, pad_mask, via,
    )
    south = lax.ppermute(bottom, GY, ring(GY))
    north = lax.ppermute(top, GY, back(ring(GY)))
    big_plane = lax.ppermute(three, "gz", swap)
    first, last = call(
        columns_kernel, [array(DEEP * N_OWN, tall)] * 2, turn[1:], 0,
        plane, via, drawn, south, north,
    )
    west = lax.ppermute(last, GX, ring(GX))
    east = lax.ppermute(first, GX, back(ring(GX)))
    (small_send,) = call(
        corner_kernel, [array(N_FAR * 3 * DEEP, n_cols)], [], 1,
        gz, plane, via, south, north, west, east,
    )
    small = lax.ppermute(small_send, "gz", swap)
    via_far = lax.ppermute(via_send, "gz", swap)
    near, near_e, near_n, near_sum, far_sum = call(
        own_kernel,
        [array(4, frame, broad)] + [array(2, frame, broad)] * 3 + [array(2, half, n_cols)],
        [pltpu.VMEM((2, n_rows + 2 * STEP, broad), jnp.float32)] + turn,
        1, gz, plane, via, drawn, south, north, west, east,
    )
    send, far_e, far_n, cross, inverse, step_1, n_0, inv_near, part = call(
        edge_kernel,
        [array(2, half, n_cols)] + [array(2, frame, broad)] * 2
        + [array(frame, broad), array(6, frame, broad), array(4, frame, broad),
           array(2, half, n_cols), array(3, half, n_cols), array(STEP, LANES)],
        [pltpu.VMEM((N_FAR, frame, broad), jnp.float32), pltpu.VMEM((2, frame, broad), jnp.float32)]
        + turn + [pltpu.VMEM((2, half, n_cols), jnp.float32), pltpu.SemaphoreType.DMA((2,))],
        1, gz, near, near_e, near_n, near_sum, big_plane, big_via, small, outside=1,
    )
    n_0_far = lax.ppermute(send, "gz", swap)
    (inv_far,) = call(
        inverse_kernel, [array(3, half, n_cols)], [], 1,
        gz, plane, via, far_sum, via_far,
    )
    send, n_12, spread = call(
        steps_kernel,
        [array(4, half, n_cols), array(4, half, n_cols), array(n_gx, 1, LANES)],
        [pltpu.VMEM((4, frame, broad), jnp.float32), pltpu.VMEM((4, half, n_cols), jnp.float32),
         pltpu.SemaphoreType.DMA((2,))],
        0, step_1, near_e, near_n, far_e, far_n, cross, inverse, part, outside=1,
    )
    n_12_far = lax.ppermute(send, "gz", swap)
    parts = lax.all_to_all(spread, GX, 0, 0, tiled=True)
    (spread,) = call(relay_kernel, [array(n_rest, 1, LANES)], [], 0, parts)
    parts = lax.all_to_all(spread, rest, 0, 0, tiled=True)
    volts, left, flag = call(
        combine_kernel,
        [array(2, n_rows, n_cols)] * 2 + [jax.ShapeDtypeStruct((1, LANES), jnp.int32)],
        [pltpu.VMEM((2, n_rows, n_cols), jnp.float32)] * 2
        + [pltpu.VMEM((2, half, n_cols), jnp.float32), pltpu.SemaphoreType.DMA((5,))],
        1, gz, n_0_far, parts, drawn, inv_near, inv_far, n_0, n_12, n_12_far, outside=2, far=1,
    )

    def careful():
        return recurrence(
            load_current, sink_mask, pad_mask, plane_class, via_class, plane_table, via_table
        )

    return lax.cond(flag[0, 0] == 1, lambda: (volts, left), careful)


def solution(mesh):
    split = Mesh(
        mesh.devices.reshape(8, 2, 2, 4, mesh.shape["gz"]), ("gx_0", "gx_1", "gy_0", "gy_1", "gz")
    )
    placed = (
        P(GY, GX),
        P(GY, GX),
        P(GY, GX),
        P("gz", GY, GX),
        P("gz", GY, GX),
        P("gz", None),
        P("gz", None),
    )
    return jax.shard_map(
        shards,
        mesh=split,
        in_specs=placed,
        out_specs=(P("gz", GY, GX), P("gz", GY, GX)),
        check_vma=False,
    )
```
